8 devices in a mesh: rep: 1 (over z), fsdp: 8 (over y, x, core).
Axes of the slice: x: 2, y: 2, z: 1, core: 2. Of those that a mesh axis runs over, the one named last changes fastest.
Arguments:
- tokens: bfloat16 [8192, 1536], P(('rep', 'fsdp'))
- seg_ids: int32 [8192], P(('rep', 'fsdp'))
- w_q: bfloat16 [2, 1536, 1536], P(None, 'fsdp')
- w_k: bfloat16 [2, 1536, 256], P(None, 'fsdp')
- w_v: bfloat16 [2, 1536, 256], P(None, 'fsdp')
- w_o: bfloat16 [2, 1536, 1536], P(None, 'fsdp')
- w_gate: bfloat16 [2, 1536, 8960], P(None, 'fsdp')
- w_up: bfloat16 [2, 1536, 8960], P(None, 'fsdp')
- w_down: bfloat16 [2, 8960, 1536], P(None, 'fsdp')
- g_attn: bfloat16 [2, 1536], replicated
- g_mlp: bfloat16 [2, 1536], replicated
Outputs:
- output: float32 [8192, 1536], P(('rep', 'fsdp'))
All inputs are finite; a program needn't handle non-finite values.
Results may differ from the reference program's by a relative error of at most 0.0138107.
Values are sent between devices in bfloat16 or wider.
A program may use at most 1 GiB of HBM per device.

```python
import jax
import jax.numpy as jnp
from jax import lax

D = 1536
FF = 8960
HEADS = 12
KV_HEADS = 2
HEAD = 128
TOKENS_DEV = 1024
GROUP = 8
LAYERS = 2
PART_TOKENS = GROUP * TOKENS_DEV
MEAN_LEN = max(2, TOKENS_DEV // 4)
Q_GROUP = HEADS // KV_HEADS
EPS = 1e-5
ROPE_BASE = 10000.0


def draw_segments(seg_key):
    tok_idx = jnp.arange(PART_TOKENS, dtype=jnp.int32)
    new_req = (jax.random.randint(seg_key, (PART_TOKENS,), 0, MEAN_LEN) == 0) | (tok_idx % TOKENS_DEV == 0)
    return (jnp.cumsum(new_req.astype(jnp.int32)) - 1).astype(jnp.int32)


def weight_draw(w_key, shape, scale):
    return (jax.random.normal(w_key, shape, jnp.float32) * scale).astype(jnp.bfloat16)


def setup_inputs(seed: int = 0, part: int = 0) -> dict:
    root_key = jax.random.key(seed)
    part_key = jax.random.fold_in(root_key, part)
    tok_key, seg_key = jax.random.split(part_key)
    key_list = jax.random.split(root_key, 9)
    q_width = HEADS * HEAD
    kv_width = KV_HEADS * HEAD
    d_scale = D ** -0.5
    qk_scale = 1.5 * d_scale
    o_scale = q_width ** -0.5
    down_scale = FF ** -0.5
    tokens = jax.random.normal(tok_key, (PART_TOKENS, D), jnp.float32).astype(jnp.bfloat16)
    gain_a = 1.0 + 0.3 * jax.random.normal(key_list[7], (LAYERS, D), jnp.float32)
    gain_m = 1.0 + 0.3 * jax.random.normal(key_list[8], (LAYERS, D), jnp.float32)
    return {
        "tokens": tokens,
        "seg_ids": draw_segments(seg_key),
        "w_q": weight_draw(key_list[0], (LAYERS, D, q_width), qk_scale),
        "w_k": weight_draw(key_list[1], (LAYERS, D, kv_width), qk_scale),
        "w_v": weight_draw(key_list[2], (LAYERS, D, kv_width), d_scale),
        "w_o": weight_draw(key_list[3], (LAYERS, q_width, D), o_scale),
        "w_gate": weight_draw(key_list[4], (LAYERS, D, FF), d_scale),
        "w_up": weight_draw(key_list[5], (LAYERS, D, FF), d_scale),
        "w_down": weight_draw(key_list[6], (LAYERS, FF, D), down_scale),
        "g_attn": gain_a.astype(jnp.bfloat16),
        "g_mlp": gain_m.astype(jnp.bfloat16),
    }


def rms_norm(hidden, gain):
    inv_rms = lax.rsqrt(jnp.mean(hidden * hidden, axis=-1, keepdims=True) + EPS)
    return (hidden * inv_rms * gain.astype(jnp.float32)).astype(jnp.bfloat16)


def rotary(vals, tok_pos):
    half_dim = HEAD // 2
    inv_freq = ROPE_BASE ** (-jnp.arange(half_dim, dtype=jnp.float32) / half_dim)
    angles = tok_pos[:, None] * inv_freq[None, :]
    bcast_shape = (vals.shape[0],) + (1,) * (vals.ndim - 2) + (half_dim,)
    cos_wide = jnp.cos(angles).reshape(bcast_shape)
    sin_wide = jnp.sin(angles).reshape(bcast_shape)
    first_half = vals[..., :half_dim].astype(jnp.float32)
    second_half = vals[..., half_dim:].astype(jnp.float32)
    rotated = jnp.concatenate([first_half * cos_wide - second_half * sin_wide, second_half * cos_wide + first_half * sin_wide], axis=-1)
    return rotated.astype(jnp.bfloat16)


def attend_block(block_in):
    q_blk, k_blk, v_blk, seg_blk = block_in
    tok_idx = jnp.arange(TOKENS_DEV, dtype=jnp.int32)
    is_first = jnp.concatenate([tok_idx[:1] == 0, seg_blk[1:] != seg_blk[:-1]])
    req_start = lax.cummax(jnp.where(is_first, tok_idx, 0), axis=0)
    tok_pos = (tok_idx - req_start).astype(jnp.float32)
    q_rot = rotary(q_blk, tok_pos)
    k_rot = rotary(k_blk, tok_pos)
    scores = jnp.einsum("tkgd,skd->kgts", q_rot.astype(jnp.float32), k_rot.astype(jnp.float32)) * HEAD ** -0.5
    allowed = (seg_blk[:, None] == seg_blk[None, :]) & (tok_idx[None, :] <= tok_idx[:, None])
    scores = jnp.where(allowed, scores, -1e30)
    probs = jax.nn.softmax(scores, axis=-1).astype(jnp.bfloat16)
    mixed = jnp.einsum("kgts,skd->tkgd", probs.astype(jnp.float32), v_blk.astype(jnp.float32))
    return mixed.astype(jnp.bfloat16)


def reference(tokens, seg_ids, w_q, w_k, w_v, w_o, w_gate, w_up, w_down, g_attn, g_mlp):
    seg_blocks = seg_ids.reshape(GROUP, TOKENS_DEV)

    def layer_step(hidden, layer_w):
        lw_q, lw_k, lw_v, lw_o, lw_gate, lw_up, lw_down, lg_attn, lg_mlp = layer_w
        normed = rms_norm(hidden, lg_attn)
        q_all = jnp.dot(normed, lw_q, preferred_element_type=jnp.float32).astype(jnp.bfloat16)
        k_all = jnp.dot(normed, lw_k, preferred_element_type=jnp.float32).astype(jnp.bfloat16)
        v_all = jnp.dot(normed, lw_v, preferred_element_type=jnp.float32).astype(jnp.bfloat16)
        q_blocks = q_all.reshape(GROUP, TOKENS_DEV, KV_HEADS, Q_GROUP, HEAD)
        k_blocks = k_all.reshape(GROUP, TOKENS_DEV, KV_HEADS, HEAD)
        v_blocks = v_all.reshape(GROUP, TOKENS_DEV, KV_HEADS, HEAD)
        mixed = lax.map(attend_block, (q_blocks, k_blocks, v_blocks, seg_blocks))
        hidden = hidden + jnp.dot(mixed.reshape(PART_TOKENS, HEADS * HEAD), lw_o, preferred_element_type=jnp.float32)
        normed = rms_norm(hidden, lg_mlp)
        gate_proj = jnp.dot(normed, lw_gate, preferred_element_type=jnp.float32)
        up_proj = jnp.dot(normed, lw_up, preferred_element_type=jnp.float32)
        act_val = (jax.nn.silu(gate_proj) * up_proj).astype(jnp.bfloat16)
        hidden = hidden + jnp.dot(act_val, lw_down, preferred_element_type=jnp.float32)
        return hidden, None

    hidden_out, _ = lax.scan(layer_step, tokens.astype(jnp.float32), (w_q, w_k, w_v, w_o, w_gate, w_up, w_down, g_attn, g_mlp))
    return hidden_out
```

```python
import functools

import jax
import jax.numpy as jnp
from jax import lax
from jax.experimental import pallas as pl
from jax.experimental.pallas import tpu as pltpu
from jax.sharding import PartitionSpec as P

HEAD = 128
HEADS = 12
KV_HEADS = 2
EPS = 1e-5
ROPE_BASE = 10000.0
MESH = pl.DeviceIdType.MESH

N_DEV = 8
TOK = 1024
D = 1536
KV = KV_HEADS * HEAD
FF = 8960
ROWS = D // N_DEV
FROWS = FF // N_DEV
TF = 640
N_GU = FF // TF
DR = 160
N_DN = FROWS // DR
PER = 2 + N_DN + N_GU
GU0 = 2 + N_DN
LAYERS = 2
TOTAL = PER * LAYERS
RING = 8
MB = 256
SCALE = HEAD ** -0.5


def kernel(tok, seg_c, seg_r, freq, g_attn, g_mlp, w_q, w_k, w_v, w_o, w_g, w_u, w_d,
           out, f_q, f_k, f_v, f_o, f_g, f_u, f_d,
           x, h, q, k, v, o, cos_t, sin_t, mask, vq, vk, vv, vo, vg, vu, vd,
           b_q, b_k, b_v, b_o, b_g, b_u, b_d,
           send, recv, loc, ld):
    me = lax.axis_index("fsdp")
    core = lax.rem(me, 2)
    xc = lax.rem(me // 2, 2)
    yc = me // 4
    xn = me + 2 - 4 * xc
    yn = me + 4 - 8 * yc
    cn = me + 1 - 2 * core
    dg = xn + 4 - 8 * yc

    barrier = pltpu.get_barrier_semaphore()
    for nb in (xn, yn, cn):
        pl.semaphore_signal(barrier, inc=1, device_id={"fsdp": nb}, device_id_type=MESH)
    pl.semaphore_wait(barrier, 3)

    def pieces(rd):
        kind, l, j = rd
        if kind == "qkv":
            return [(w_q, f_q, ROWS, ROWS, 0, 0, D, b_q), (w_k, f_k, ROWS, ROWS, 0, 0, KV, b_k), (w_v, f_v, ROWS, ROWS, 0, 0, KV, b_v)]
        if kind == "o":
            return [(w_o, f_o, ROWS, ROWS, 0, 0, D, b_o)]
        par = lax.rem(j, 4)
        if kind == "dn":
            return [(w_d, f_d, FROWS, DR, j * DR, 0, D, b_d.at[par])]
        return [(w_g, f_g, ROWS, ROWS, 0, j * TF, TF, b_g.at[par]), (w_u, f_u, ROWS, ROWS, 0, j * TF, TF, b_u.at[par])]

    def al(i, n):
        return i if isinstance(i, int) else pl.multiple_of(i, n)

    def own_view(p, l):
        src, _, _, nr, r0, c0, nc, _ = p
        return src.at[l, pl.ds(al(r0, 16), nr), pl.ds(al(c0, 128), nc)]

    def gview(p, l, dev, half=None):
        _, dst, span, nr, r0, c0, nc, _ = p
        off, n = {None: (0, nr), "A": (0, nr // 2), "B": (nr // 2, nr // 2)}[half]
        return dst.at[l, pl.ds(al(dev * span + r0 + off, 16), n), pl.ds(al(c0, 128), nc)]

    def tx(p, l, slot, m, t):
        if t == 0:
            s, d, dev = own_view(p, l), gview(p, l, me), xn
        elif t == 1:
            s, d, dev = own_view(p, l), gview(p, l, me), yn
        elif t == 2:
            s, d, dev = own_view(p, l), gview(p, l, me), cn
        else:
            owner, half, dev = {3: (yn, "A", xn), 4: (xn, "B", yn), 5: (xn, None, cn), 6: (yn, None, cn), 7: (dg, "A", cn), 8: (dg, "B", cn)}[t]
            s = gview(p, l, owner, half)
            d = s
        return pltpu.make_async_remote_copy(src_ref=s, dst_ref=d, send_sem=send.at[slot, m, t], recv_sem=recv.at[slot, m, t],
                                            device_id={"fsdp": dev}, device_id_type=MESH)

    def bounce_in(p, l, slot, m):
        return pltpu.make_async_copy(own_view(p, l), p[7], loc.at[slot, m, 0])

    def bounce_out(p, l, slot, m):
        return pltpu.make_async_copy(p[7], gview(p, l, me), loc.at[slot, m, 1])

    def step_e(rd, slot):
        for m, p in enumerate(pieces(rd)):
            for t in (0, 1, 2):
                tx(p, rd[1], slot, m, t).start()
            bounce_in(p, rd[1], slot, m).start()

    def step_a(rd, slot):
        for m, p in enumerate(pieces(rd)):
            tx(p, rd[1], slot, m, 0).wait_recv()
            tx(p, rd[1], slot, m, 4).start()
            tx(p, rd[1], slot, m, 5).start()
            tx(p, rd[1], slot, m, 1).wait_recv()
            tx(p, rd[1], slot, m, 3).start()
            tx(p, rd[1], slot, m, 6).start()
            bounce_in(p, rd[1], slot, m).wait()
            bounce_out(p, rd[1], slot, m).start()

    def step_b(rd, slot):
        for m, p in enumerate(pieces(rd)):
            tx(p, rd[1], slot, m, 3).wait_recv()
            tx(p, rd[1], slot, m, 7).start()
            tx(p, rd[1], slot, m, 4).wait_recv()
            tx(p, rd[1], slot, m, 8).start()

    def step_c(rd, slot):
        for m, p in enumerate(pieces(rd)):
            for t in (2, 5, 6, 7, 8):
                tx(p, rd[1], slot, m, t).wait_recv()
            for t in range(9):
                tx(p, rd[1], slot, m, t).wait_send()
            bounce_out(p, rd[1], slot, m).wait()

    STEPS = ((step_c, -3), (step_b, -2), (step_a, -1), (step_e, 1))

    def round_of(r):
        l, i = divmod(r, PER)
        if i == 0:
            return ("qkv", l, 0)
        if i == 1:
            return ("o", l, 0)
        if i < GU0:
            return ("dn", l, i - 2)
        return ("gu", l, i - GU0)

    def service(r):
        for fn, off in STEPS:
            if 0 <= r + off < TOTAL:
                fn(round_of(r + off), (r + off) % RING)

    def service_loop(l, t):
        for fn, off in STEPS:
            lag = 3 + off
            base = PER * l + GU0

            def dyn(fn=fn, lag=lag, base=base):
                fn(("gu", l, t + lag), lax.rem(base + lag + t, RING))

            if lag == 0:
                dyn()
                continue
            pl.when(t + lag < N_GU)(dyn)
            for kk in range(lag):
                r = PER * (l + 1) + kk
                if r < TOTAL:
                    def stat(fn=fn, r=r):
                        fn(round_of(r), r % RING)
                    pl.when(t == N_GU + kk - lag)(stat)

    step_e(round_of(0), 0)
    tok_in = pltpu.make_async_copy(tok, o, ld.at[0])
    tok_in.start()
    service(0)

    def tables(i, c):
        rows = pl.ds(pl.multiple_of(i * MB, MB), MB)
        same = seg_c[rows, :] == seg_r[...]
        rr = lax.broadcasted_iota(jnp.int32, (MB, TOK), 0) + i * MB
        cc = lax.broadcasted_iota(jnp.int32, (MB, TOK), 1)
        ok = jnp.where(same & (cc <= rr), 1.0, 0.0)
        mask[rows, :] = ok
        pos = jnp.sum(ok, axis=1, keepdims=True) - 1.0
        ang = pos * freq[...]
        lane = lax.broadcasted_iota(jnp.int32, (MB, HEAD), 1)
        cos_t[rows, :] = jnp.cos(ang)
        sn = jnp.sin(ang)
        sin_t[rows, :] = jnp.where(lane < HEAD // 2, -sn, sn)
        return c

    lax.fori_loop(0, TOK // MB, tables, 0)
    tok_in.wait()

    def widen(i, c):
        rows = pl.ds(pl.multiple_of(i * MB, MB), MB)
        x[rows, :] = o[rows, :].astype(jnp.float32)
        return c

    lax.fori_loop(0, TOK // MB, widen, 0)

    def norm_rows(gain_ref, l):
        def body(i, c):
            rows = pl.ds(pl.multiple_of(i * MB, MB), MB)
            xv = x[rows, :]
            inv = lax.rsqrt(jnp.mean(xv * xv, axis=-1, keepdims=True) + EPS)
            h[rows, :] = (xv * inv * gain_ref[l:l + 1, :].astype(jnp.float32)).astype(jnp.bfloat16)
            return c
        lax.fori_loop(0, TOK // MB, body, 0)

    def rope(val, rows):
        f = val.astype(jnp.bfloat16).astype(jnp.float32)
        return (f * cos_t[rows, :] + pltpu.roll(f, HEAD // 2, 1) * sin_t[rows, :]).astype(jnp.bfloat16)

    def qkv_rows(i, c):
        rows = pl.ds(pl.multiple_of(i * MB, MB), MB)
        hv = h[rows, :]
        for g in range(HEADS // 4):
            val = jnp.dot(hv, vq[:, g * 512:(g + 1) * 512], preferred_element_type=jnp.float32)
            for e in range(4):
                q[rows, g * 512 + e * HEAD:g * 512 + (e + 1) * HEAD] = rope(val[:, e * HEAD:(e + 1) * HEAD], rows)
        val = jnp.dot(hv, vk[...], preferred_element_type=jnp.float32)
        for e in range(KV_HEADS):
            k[rows, e * HEAD:(e + 1) * HEAD] = rope(val[:, e * HEAD:(e + 1) * HEAD], rows)
        v[rows, :] = jnp.dot(hv, vv[...], preferred_element_type=jnp.float32).astype(jnp.bfloat16)
        return c

    def head_body(hd, c):
        qc = pl.ds(pl.multiple_of(hd * HEAD, HEAD), HEAD)
        kc = pl.ds(pl.multiple_of((hd // (HEADS // KV_HEADS)) * HEAD, HEAD), HEAD)
        for i in range(TOK // MB):
            n = (i + 1) * MB
            s = lax.dot_general(q[i * MB:n, qc], k[0:n, kc], (((1,), (1,)), ((), ())), preferred_element_type=jnp.float32) * SCALE
            s = jnp.where(mask[i * MB:n, 0:n] > 0.5, s, -1e30)
            e = jnp.exp(s - jnp.max(s, axis=1, keepdims=True))
            p = (e / jnp.sum(e, axis=1, keepdims=True)).astype(jnp.bfloat16)
            o[i * MB:n, qc] = jnp.dot(p, v[0:n, kc], preferred_element_type=jnp.float32).astype(jnp.bfloat16)
        return c

    def proj_rows(i, c):
        rows = pl.ds(pl.multiple_of(i * MB, MB), MB)
        x[rows, :] += jnp.dot(o[rows, :], vo[...], preferred_element_type=jnp.float32)
        return c

    def mlp_rows(i, c):
        rows = pl.ds(pl.multiple_of(i * MB, MB), MB)
        hv = h[rows, :]
        gt = jnp.dot(hv, vg[...], preferred_element_type=jnp.float32)
        up = jnp.dot(hv, vu[...], preferred_element_type=jnp.float32)
        a = (gt * jax.nn.sigmoid(gt) * up).astype(jnp.bfloat16)
        x[rows, :] += jnp.dot(a, vd[...], preferred_element_type=jnp.float32)
        return c

    for l in range(LAYERS):
        if l == 0:
            for r in range(1, 3):
                service(r)
        norm_rows(g_attn, l)
        base = PER * l
        service(base + 3)
        loads = [pltpu.make_async_copy(f_q.at[l], vq, ld.at[0]), pltpu.make_async_copy(f_k.at[l], vk, ld.at[1]), pltpu.make_async_copy(f_v.at[l], vv, ld.at[2])]
        for c in loads:
            c.start()
        for c in loads:
            c.wait()
        lax.fori_loop(0, TOK // MB, qkv_rows, 0)
        service(base + 4)
        load_o = pltpu.make_async_copy(f_o.at[l], vo, ld.at[0])
        load_o.start()
        per_group = HEADS // 6
        for g in range(6):
            lax.fori_loop(g * per_group, (g + 1) * per_group, head_body, 0)
            service(base + 5 + g)
        load_o.wait()
        lax.fori_loop(0, TOK // MB, proj_rows, 0)
        norm_rows(g_mlp, l)
        for r in range(base + 11, base + GU0 + 3):
            service(r)

        def tile(t, c):
            service_loop(l, t)
            cols = pl.ds(pl.multiple_of(t * TF, 128), TF)
            loads = [pltpu.make_async_copy(f_g.at[l, :, cols], vg, ld.at[0]), pltpu.make_async_copy(f_u.at[l, :, cols], vu, ld.at[1]), pltpu.make_async_copy(f_d.at[l, cols, :], vd, ld.at[2])]
            for cp in loads:
                cp.start()
            for cp in loads:
                cp.wait()
            lax.fori_loop(0, TOK // MB, mlp_rows, 0)
            return c

        lax.fori_loop(0, N_GU, tile, 0)
    done = pltpu.make_async_copy(x, out, ld.at[0])
    done.start()
    done.wait()


def solution(mesh):
    tok_spec = P(("rep", "fsdp"), None)
    seg_spec = P(("rep", "fsdp"))
    mat_spec = P(None, "fsdp", None)
    gain_spec = P(None, None)
    bf, f32 = jnp.bfloat16, jnp.float32

    def per_device(tokens, seg_ids, w_q, w_k, w_v, w_o, w_gate, w_up, w_down, g_attn, g_mlp):
        half = HEAD // 2
        inv = ROPE_BASE ** (-jnp.arange(half, dtype=f32) / half)
        freq = jnp.concatenate([inv, inv]).reshape(1, HEAD)
        any_s = pl.BlockSpec(memory_space=pl.ANY)
        vm = pl.BlockSpec(memory_space=pltpu.VMEM)
        full = [(LAYERS, D, D), (LAYERS, D, KV), (LAYERS, D, KV), (LAYERS, D, D), (LAYERS, D, FF), (LAYERS, D, FF), (LAYERS, FF, D)]
        res = pl.pallas_call(
            kernel,
            out_shape=[jax.ShapeDtypeStruct((TOK, D), f32)] + [jax.ShapeDtypeStruct(s, bf) for s in full],
            in_specs=[any_s, vm, vm, vm, vm, vm] + [any_s] * 7,
            out_specs=[any_s] * 8,
            scratch_shapes=[
                pltpu.VMEM((TOK, D), f32), pltpu.VMEM((TOK, D), bf), pltpu.VMEM((TOK, D), bf),
                pltpu.VMEM((TOK, KV), bf), pltpu.VMEM((TOK, KV), bf), pltpu.VMEM((TOK, D), bf),
                pltpu.VMEM((TOK, HEAD), f32), pltpu.VMEM((TOK, HEAD), f32), pltpu.VMEM((TOK, TOK), f32),
                pltpu.VMEM((D, D), bf), pltpu.VMEM((D, KV), bf), pltpu.VMEM((D, KV), bf), pltpu.VMEM((D, D), bf),
                pltpu.VMEM((D, TF), bf), pltpu.VMEM((D, TF), bf), pltpu.VMEM((TF, D), bf),
                pltpu.VMEM((ROWS, D), bf), pltpu.VMEM((ROWS, KV), bf), pltpu.VMEM((ROWS, KV), bf), pltpu.VMEM((ROWS, D), bf),
                pltpu.VMEM((4, ROWS, TF), bf), pltpu.VMEM((4, ROWS, TF), bf), pltpu.VMEM((4, DR, D), bf),
                pltpu.SemaphoreType.DMA((RING, 3, 9)), pltpu.SemaphoreType.DMA((RING, 3, 9)),
                pltpu.SemaphoreType.DMA((RING, 3, 2)), pltpu.SemaphoreType.DMA((4,)),
            ],
            compiler_params=pltpu.CompilerParams(collective_id=0, has_side_effects=True, vmem_limit_bytes=66 * 1000 * 1000),
        )(tokens, seg_ids.reshape(TOK, 1), seg_ids.reshape(1, TOK), freq, g_attn, g_mlp, w_q, w_k, w_v, w_o, w_gate, w_up, w_down)
        return res[0]

    return jax.shard_map(per_device, mesh=mesh, in_specs=(tok_spec, seg_spec, mat_spec, mat_spec, mat_spec, mat_spec, mat_spec, mat_spec, mat_spec, gain_spec, gain_spec), out_specs=tok_spec, check_vma=False)
```

```python
import jax
import jax.numpy as jnp
from jax import lax
from jax.experimental import pallas as pl
from jax.experimental.pallas import tpu as pltpu
from jax.sharding import PartitionSpec as P

HEAD = 128
HEADS = 12
KV_HEADS = 2
EPS = 1e-5
ROPE_BASE = 10000.0
MESH = pl.DeviceIdType.MESH

N_DEV = 8
TOK = 1024
D = 1536
KV = KV_HEADS * HEAD
FF = 8960
HALF = FF // 2
ROWS = D // N_DEV
FROWS = FF // N_DEV
TF = 640
N_G0 = HALF // TF
N_G1 = FF // TF
DR = 160
N_DN = FROWS // DR
LAYERS = 2
MB = 256
NB = TOK // MB
SCALE = HEAD ** -0.5

RATE = {"X": 46600.0, "Y": 46600.0, "D": 500000.0, "L": 800000.0}
LAT = {"X": 2.5, "Y": 2.5, "D": 1.5, "L": 1.0}
HORIZON = 24.0
T_TABLES, T_WIDEN, T_NORM, T_QKV, T_HEAD, T_PROJ, T_TILE, T_ADD = 8.0, 2.0, 3.5, 2.6, 4.0, 2.0, 8.5, 1.5
OWN_FIRST = 3
N_SEM = 230


class Transfer:
    def __init__(self, key, link, size, n_sem, start, wait, done, deps):
        self.key, self.link, self.size, self.n_sem = key, link, size, n_sem
        self.start, self.wait, self.done, self.deps = start, wait, done, set(deps)
        self.sems = []


class Planner:
    def __init__(self):
        self.now = 0.0
        self.free = dict.fromkeys("XYDL", 0.0)
        self.all, self.queue, self.users, self.mates = {}, {"X": [], "Y": []}, {}, {}
        self.pool = list(range(N_SEM))
        self.issued, self.arrived, self.flying, self.sent, self.ops = set(), set(), [], [], []

    def add(self, tr):
        self.all[tr.key] = tr
        for dep in tr.deps:
            self.users.setdefault(dep, []).append(tr.key)

    def issue(self, key):
        tr = self.all[key]
        self.issued.add(key)
        tr.sems, self.pool = self.pool[:tr.n_sem], self.pool[tr.n_sem:]
        self.ops.append(tr.start)
        self.free[tr.link] = max(self.free[tr.link], self.now) + tr.size / RATE[tr.link]
        self.flying.append((self.free[tr.link] + LAT[tr.link], key))
        for mate in self.mates.get(key, ()):
            if mate not in self.issued and self.all[mate].deps <= self.arrived:
                self.issue(mate)

    def mark(self, key):
        self.arrived.add(key)
        for user in self.users.get(key, ()):
            tr = self.all[user]
            if tr.link in "DL" and user not in self.issued and tr.deps <= self.arrived:
                self.issue(user)

    def receive(self, item):
        self.flying.remove(item)
        tr = self.all[item[1]]
        self.ops.append(tr.wait)
        if tr.done is not None:
            self.sent.append((item[0] + 2.0, item[1]))
        else:
            self.pool += tr.sems
        self.mark(item[1])

    def fill(self):
        for link in "XY":
            while self.free[link] - self.now < HORIZON:
                ready = [k for k in self.queue[link] if self.all[k].deps <= self.arrived]
                if not ready:
                    break
                self.queue[link].remove(ready[0])
                self.issue(ready[0])

    def retire(self, keys=None, everything=False):
        for item in list(self.sent):
            if everything or (keys is not None and item[1] in keys) or (keys is None and item[0] <= self.now):
                self.sent.remove(item)
                self.ops.append(self.all[item[1]].done)
                self.pool += self.all[item[1]].sems

    def service(self):
        while True:
            due = sorted(i for i in self.flying if i[0] <= self.now)
            if not due:
                break
            self.receive(due[0])
            self.fill()
        self.fill()
        self.retire()

    def need(self, keys):
        keys = set(keys)
        while not keys <= self.arrived:
            self.fill()
            item = min(self.flying)
            self.now = max(self.now, item[0])
            self.receive(item)
        self.service()

    def spend(self, us):
        self.now += us

    def take(self):
        ops, self.ops = self.ops, []
        return ops


def run(ops):
    for op in ops:
        op()


def run_at(index, table):
    for k, ops in (table.items() if isinstance(table, dict) else enumerate(table)):
        if ops:
            pl.when(index == k)(lambda ops=ops: run(ops))


def kernel(tok, seg_c, seg_r, freq, g_attn, g_mlp, w_q, w_k, w_v, w_o, w_g, w_u, w_d,
           out, f_q, f_k, f_v, f_o, f_g, f_u, f_d, f_p,
           x, h, q, k, v, o, cos_t, sin_t, mask, vq, vk, vv, vo, vg, vu, vd,
           b_q, b_k, b_v, b_o, b_g, b_u, b_d,
           send, recv, ld):
    me = lax.axis_index("fsdp")
    core = lax.rem(me, 2)
    xc = lax.rem(me // 2, 2)
    yc = me // 4
    xn = me + 2 - 4 * xc
    yn = me + 4 - 8 * yc
    cn = me + 1 - 2 * core
    dg = xn + 4 - 8 * yc

    barrier = pltpu.get_barrier_semaphore()
    for nb in (xn, yn, cn):
        pl.semaphore_signal(barrier, inc=1, device_id={"fsdp": nb}, device_id_type=MESH)
    pl.semaphore_wait(barrier, 3)

    plan = Planner()

    def al(i, n):
        return i if isinstance(i, int) else pl.multiple_of(i, n)

    def view(ref, l, r0, nr, c0, nc):
        return ref.at[l, pl.ds(al(r0, 16), nr), pl.ds(al(c0, 128), nc)]

    def remote(key, link, pairs, dev, deps):
        sizes = [n for n, _ in pairs]

        def each():
            for i, (_, make) in zip(plan.all[key].sems, pairs):
                src, dst = make()
                yield pltpu.make_async_remote_copy(src_ref=src, dst_ref=dst, send_sem=send.at[i], recv_sem=recv.at[i],
                                                   device_id={"fsdp": dev}, device_id_type=MESH)

        plan.add(Transfer(key, link, sum(sizes), len(pairs), lambda: [c.start() for c in each()], lambda: [c.wait_recv() for c in each()],
                          lambda: [c.wait_send() for c in each()], deps))

    def local(key, pairs, deps):
        sizes = [n for n, _ in pairs]

        def each():
            for i, (_, make) in zip(plan.all[key].sems, pairs):
                src, dst = make()
                yield pltpu.make_async_copy(src, dst, send.at[i])

        plan.add(Transfer(key, "L", sum(sizes), len(pairs), lambda: [c.start() for c in each()], lambda: [c.wait() for c in each()], None, deps))

    def add_round(rd):
        kind, l, j = rd
        if kind == "qkv":
            mats = [(w_q, f_q, ROWS, ROWS, 0, D, b_q), (w_k, f_k, ROWS, ROWS, 0, KV, b_k), (w_v, f_v, ROWS, ROWS, 0, KV, b_v)]
        elif kind == "o":
            mats = [(w_o, f_o, ROWS, ROWS, 0, D, b_o)]
        elif kind == "dn":
            mats = [(w_d, f_d, FROWS, DR, j * DR, D, b_d.at[j % 4])]
        else:
            mats = [(w_g, f_g, ROWS, ROWS, j * TF, TF, b_g.at[j % 4]), (w_u, f_u, ROWS, ROWS, j * TF, TF, b_u.at[j % 4])]
        rowwise = kind == "dn"
        paired = l == 0 and kind == "gu"
        col_mine = yc * HALF if paired else 0
        col_other = (1 - yc) * HALF if paired else 0

        def own_src(m, other=False):
            src, _, _, nr, off, nc, _ = m
            r0, c0 = (off, 0) if rowwise else (0, off + (col_other if other else col_mine))
            return view(src, l, r0, nr, c0, nc)

        def held_at(m, dev, part=None, other=False):
            _, dst, span, nr, off, nc, _ = m
            r0, c0 = (off, 0) if rowwise else (0, off + (col_other if other else col_mine))
            cut, n = {None: (0, nr), "A": (0, nr // 2), "B": (nr // 2, nr // 2)}[part]
            return view(dst, l, dev * span + r0 + cut, n, c0, nc)

        def own(other=False):
            return [(2 * m[3] * m[5], lambda m=m: (own_src(m, other), held_at(m, me, other=other))) for m in mats]

        def held(dev, part=None):
            return [(2 * m[3] * m[5] // (2 if part else 1), lambda m=m: (held_at(m, dev, part),) * 2) for m in mats]

        K = lambda t: (rd, t)
        names = ["X", "D", "DX", "bin", "bout"]
        remote(K("X"), "X", own(), xn, [])
        remote(K("D"), "D", own(), cn, [])
        remote(K("DX"), "D", held(xn), cn, [K("X")])
        prev = [((kind, l, j - 4), "bout")] if j >= 4 else ([(("dn", 0, j + 4 if j < 3 else j), "bout")] if kind == "dn" and l == 1 else ([(("gu", 0, j + 4 if j < 3 else j), "bout")] if kind == "gu" and l == 1 else ([((kind, 0, 0), "bout")] if l == 1 else [])))
        local(K("bin"), [(2 * m[3] * m[5], lambda m=m: (own_src(m), m[6])) for m in mats], prev)
        local(K("bout"), [(2 * m[3] * m[5], lambda m=m: (m[6], held_at(m, me))) for m in mats], [K("bin")])
        plan.mates[K("X")] = [K("D"), K("bin")]
        if not (l == 0 and kind == "dn"):
            remote(K("Y"), "Y", own(other=True), yn, [])
            remote(K("DY"), "D", held(yn), cn, [K("Y")])
            names += ["Y", "DY"]
            if l == 0 or kind in ("qkv", "o"):
                remote(K("XR"), "X", held(yn), xn, [K("Y")])
                remote(K("DR"), "D", held(dg), cn, [K("XR")])
                names += ["XR", "DR"]
            else:
                remote(K("XR"), "X", held(yn, "A"), xn, [K("Y")])
                remote(K("YR"), "Y", held(xn, "B"), yn, [K("X")])
                remote(K("DR"), "D", held(dg, "A"), cn, [K("XR")])
                remote(K("DS"), "D", held(dg, "B"), cn, [K("YR")])
                names += ["XR", "YR", "DR", "DS"]
        return [K(n) for n in names]

    needs = {}
    for l, n_gu in ((0, N_G0), (1, N_G1)):
        for rd in [("qkv", l, 0), ("o", l, 0)] + [("dn", l, j) for j in range(N_DN)] + [("gu", l, j) for j in range(n_gu)]:
            needs[rd] = add_round(rd)
    for i in range(NB):
        mine, theirs = pl.ds(i * MB, MB), pl.ds(TOK + i * MB, MB)
        remote(("h", i), "Y", [(2 * MB * D, lambda mine=mine, theirs=theirs: (h.at[mine, :], h.at[theirs, :]))], yn, [("h ready", i)])
        remote(("p", i), "Y", [(4 * MB * D, lambda mine=mine, theirs=theirs: (x.at[theirs, :], f_p.at[mine, :]))], yn, ["p ready"])
    dns = {l: [key for j in range(N_DN) for key in needs[("dn", l, j)]] for l in (0, 1)}

    def seq(kind, l, n, *ts):
        return [((kind, l, j), t) for j in range(n) for t in ts]

    attn = lambda l, t: [(("qkv", l, 0), t), (("o", l, 0), t)]
    plan.queue["X"] = (attn(0, "X") + attn(0, "XR") + seq("dn", 0, N_DN, "X") + seq("gu", 0, N_G0, "X", "XR")
                       + attn(1, "X") + attn(1, "XR") + seq("dn", 1, N_DN, "X", "XR") + seq("gu", 1, N_G1, "X", "XR"))
    plan.queue["Y"] = ([("p", i) for i in range(NB)] + [("h", i) for i in range(NB)] + attn(0, "Y") + seq("gu", 0, N_G0, "Y")
                       + attn(1, "Y") + seq("dn", 1, N_DN, "Y") + seq("dn", 1, N_DN, "YR") + seq("gu", 1, N_G1, "Y", "YR"))

    def rows_of(i):
        return pl.ds(pl.multiple_of(i * MB, MB), MB)

    def load(pairs):
        cps = [pltpu.make_async_copy(s, d, ld.at[i]) for i, (s, d) in enumerate(pairs)]
        for c in cps:
            c.start()
        for c in cps:
            c.wait()

    plan.service()
    run(plan.take())
    tok_in = pltpu.make_async_copy(tok, o, ld.at[0])
    tok_in.start()

    def tables(i, c):
        rows = rows_of(i)
        same = seg_c[rows, :] == seg_r[...]
        rr = lax.broadcasted_iota(jnp.int32, (MB, TOK), 0) + i * MB
        cc = lax.broadcasted_iota(jnp.int32, (MB, TOK), 1)
        ok = jnp.where(same & (cc <= rr), 1.0, 0.0)
        mask[rows, :] = ok
        pos = jnp.sum(ok, axis=1, keepdims=True) - 1.0
        ang = pos * freq[...]
        lane = lax.broadcasted_iota(jnp.int32, (MB, HEAD), 1)
        cos_t[rows, :] = jnp.cos(ang)
        sn = jnp.sin(ang)
        sin_t[rows, :] = jnp.where(lane < HEAD // 2, -sn, sn)
        return c

    lax.fori_loop(0, NB, tables, 0)
    plan.spend(T_TABLES)
    plan.service()
    run(plan.take())
    tok_in.wait()

    def widen(i, c):
        rows = rows_of(i)
        x[rows, :] = o[rows, :].astype(jnp.float32)
        x[rows_of(i + NB), :] = jnp.zeros((MB, D), jnp.float32)
        return c

    lax.fori_loop(0, NB, widen, 0)
    plan.spend(T_WIDEN)

    def norm_row(gain_ref, l, i):
        rows = rows_of(i)
        xv = x[rows, :]
        inv = lax.rsqrt(jnp.mean(xv * xv, axis=-1, keepdims=True) + EPS)
        h[rows, :] = (xv * inv * gain_ref[l:l + 1, :].astype(jnp.float32)).astype(jnp.bfloat16)

    def rope(val, rows):
        f = val.astype(jnp.bfloat16).astype(jnp.float32)
        return (f * cos_t[rows, :] + pltpu.roll(f, HEAD // 2, 1) * sin_t[rows, :]).astype(jnp.bfloat16)

    def qkv_row(i):
        rows = rows_of(i)
        hv = h[rows, :]
        for g in range(HEADS // 4):
            val = jnp.dot(hv, vq[:, g * 512:(g + 1) * 512], preferred_element_type=jnp.float32)
            for e in range(4):
                q[rows, g * 512 + e * HEAD:g * 512 + (e + 1) * HEAD] = rope(val[:, e * HEAD:(e + 1) * HEAD], rows)
        val = jnp.dot(hv, vk[...], preferred_element_type=jnp.float32)
        for e in range(KV_HEADS):
            k[rows, e * HEAD:(e + 1) * HEAD] = rope(val[:, e * HEAD:(e + 1) * HEAD], rows)
        v[rows, :] = jnp.dot(hv, vv[...], preferred_element_type=jnp.float32).astype(jnp.bfloat16)

    def one_head(hd):
        qc = pl.ds(pl.multiple_of(hd * HEAD, HEAD), HEAD)
        kc = pl.ds(pl.multiple_of((hd // (HEADS // KV_HEADS)) * HEAD, HEAD), HEAD)
        for i in range(NB):
            n = (i + 1) * MB
            s = lax.dot_general(q[i * MB:n, qc], k[0:n, kc], (((1,), (1,)), ((), ())), preferred_element_type=jnp.float32) * SCALE
            s = jnp.where(mask[i * MB:n, 0:n] > 0.5, s, -1e30)
            e = jnp.exp(s - jnp.max(s, axis=1, keepdims=True))
            p = (e / jnp.sum(e, axis=1, keepdims=True)).astype(jnp.bfloat16)
            o[i * MB:n, qc] = jnp.dot(p, v[0:n, kc], preferred_element_type=jnp.float32).astype(jnp.bfloat16)

    def mlp_row(i, c):
        rows = rows_of(i)
        hv = h[rows, :]
        gt = jnp.dot(hv, vg[...], preferred_element_type=jnp.float32)
        up = jnp.dot(hv, vu[...], preferred_element_type=jnp.float32)
        a = (gt * jax.nn.sigmoid(gt) * up).astype(jnp.bfloat16)
        x[rows, :] += jnp.dot(a, vd[...], preferred_element_type=jnp.float32)
        return c

    for l in range(LAYERS):
        plan.need(needs[("qkv", l, 0)])
        run(plan.take())
        load([(f_q.at[l], vq), (f_k.at[l], vk), (f_v.at[l], vv)])
        plan.spend(3.0)
        table = []
        for i in range(NB):
            if l == 1:
                plan.need([("p", i)])
                plan.retire(keys=[("p", i)])
            plan.service()
            table.append(plan.take())
            plan.spend(T_QKV + T_NORM / NB + (T_ADD if l == 1 else 0.0))

        def qkv_step(i, c):
            run_at(i, table)
            if l == 1:
                load([(f_p.at[rows_of(i), :], x.at[rows_of(i + NB), :])])
                x[rows_of(i), :] += x[rows_of(i + NB), :]
            norm_row(g_attn, l, i)
            qkv_row(i)
            return c

        lax.fori_loop(0, NB, qkv_step, 0)

        table_h = []
        for i in range(HEADS):
            plan.service()
            table_h.append(plan.take())
            plan.spend(T_HEAD)

        def head_step(hd, c):
            run_at(hd, table_h)
            one_head(hd)
            return c

        lax.fori_loop(0, HEADS, head_step, 0)

        plan.need(needs[("o", l, 0)])
        run(plan.take())
        load([(f_o.at[l], vo)])
        plan.spend(2.0)
        table_o = []
        for i in range(NB):
            plan.service()
            if l == 0 and i >= 2:
                plan.mark(("h ready", i - 2))
                plan.fill()
            table_o.append(plan.take())
            plan.spend(T_PROJ + T_NORM / NB)

        def proj_step(i, c):
            run_at(i, table_o)
            rows = rows_of(i)
            x[rows, :] += jnp.dot(o[rows, :], vo[...], preferred_element_type=jnp.float32)
            norm_row(g_mlp, l, i)
            return c

        lax.fori_loop(0, NB, proj_step, 0)

        if l == 0:
            items = [(j, 0) for j in range(OWN_FIRST)] + [(j, 1) for j in range(N_G0)] + [(j, 0) for j in range(OWN_FIRST, N_G0)]
        else:
            items = [(j, 0) for j in range(N_G1)]
        table_a, table_b = [], []
        for w, (j, other) in enumerate(items):
            if l == 0 and w < 2:
                plan.mark(("h ready", NB - 2 + w))
            keys = needs[("gu", l, j)] + dns[l] + ([("h", i) for i in range(NB)] if other else [])
            plan.need(keys)
            table_a.append(plan.take())
            plan.spend(2.0)
            if l == 0 and w == OWN_FIRST + N_G0:
                plan.mark("p ready")
            plan.service()
            table_b.append(plan.take())
            plan.spend(T_TILE)

        def tiles(start, stop, base, first):
            def body(t, c):
                run_at(t, {w - base: ops for w, ops in enumerate(table_a) if start <= w < stop})
                cols = pl.ds(pl.multiple_of((yc * HALF if l == 0 else 0) + t * TF, 128), TF)
                load([(f_g.at[l, :, cols], vg), (f_u.at[l, :, cols], vu), (f_d.at[l, cols, :], vd)])
                run_at(t, {w - base: ops for w, ops in enumerate(table_b) if start <= w < stop})
                lax.fori_loop(first, first + NB, mlp_row, 0)
                return c

            lax.fori_loop(start - base, stop - base, body, 0)

        if l == 0:
            tiles(0, OWN_FIRST, 0, 0)
            tiles(OWN_FIRST, OWN_FIRST + N_G0, OWN_FIRST, NB)
            tiles(OWN_FIRST + N_G0, 2 * N_G0, N_G0, 0)
        else:
            tiles(0, N_G1, 0, 0)

    plan.need(plan.all)
    plan.retire(everything=True)
    run(plan.take())
    load([(x.at[pl.ds(0, TOK), :], out)])


def solution(mesh):
    tok_spec = P(("rep", "fsdp"), None)
    seg_spec = P(("rep", "fsdp"))
    mat_spec = P(None, "fsdp", None)
    gain_spec = P(None, None)
    bf, f32 = jnp.bfloat16, jnp.float32

    def per_device(tokens, seg_ids, w_q, w_k, w_v, w_o, w_gate, w_up, w_down, g_attn, g_mlp):
        half = HEAD // 2
        inv = ROPE_BASE ** (-jnp.arange(half, dtype=f32) / half)
        freq = jnp.concatenate([inv, inv]).reshape(1, HEAD)
        any_s = pl.BlockSpec(memory_space=pl.ANY)
        vm = pl.BlockSpec(memory_space=pltpu.VMEM)
        full = [(LAYERS, D, D), (LAYERS, D, KV), (LAYERS, D, KV), (LAYERS, D, D), (LAYERS, D, FF), (LAYERS, D, FF), (LAYERS, FF, D)]
        res = pl.pallas_call(
            kernel,
            out_shape=[jax.ShapeDtypeStruct((TOK, D), f32)] + [jax.ShapeDtypeStruct(s, bf) for s in full] + [jax.ShapeDtypeStruct((TOK, D), f32)],
            in_specs=[any_s, vm, vm, vm, vm, vm] + [any_s] * 7,
            out_specs=[any_s] * 9,
            scratch_shapes=[
                pltpu.VMEM((2 * TOK, D), f32), pltpu.VMEM((2 * TOK, D), bf), pltpu.VMEM((TOK, D), bf),
                pltpu.VMEM((TOK, KV), bf), pltpu.VMEM((TOK, KV), bf), pltpu.VMEM((TOK, D), bf),
                pltpu.VMEM((TOK, HEAD), f32), pltpu.VMEM((TOK, HEAD), f32), pltpu.VMEM((TOK, TOK), f32),
                pltpu.VMEM((D, D), bf), pltpu.VMEM((D, KV), bf), pltpu.VMEM((D, KV), bf), pltpu.VMEM((D, D), bf),
                pltpu.VMEM((D, TF), bf), pltpu.VMEM((D, TF), bf), pltpu.VMEM((TF, D), bf),
                pltpu.VMEM((ROWS, D), bf), pltpu.VMEM((ROWS, KV), bf), pltpu.VMEM((ROWS, KV), bf), pltpu.VMEM((ROWS, D), bf),
                pltpu.VMEM((4, ROWS, TF), bf), pltpu.VMEM((4, ROWS, TF), bf), pltpu.VMEM((4, DR, D), bf),
                pltpu.SemaphoreType.DMA((N_SEM,)), pltpu.SemaphoreType.DMA((N_SEM,)), pltpu.SemaphoreType.DMA((4,)),
            ],
            compiler_params=pltpu.CompilerParams(collective_id=0, has_side_effects=True, vmem_limit_bytes=66 * 1000 * 1000),
        )(tokens, seg_ids.reshape(TOK, 1), seg_ids.reshape(1, TOK), freq, g_attn, g_mlp, w_q, w_k, w_v, w_o, w_gate, w_up, w_down)
        return res[0]

    return jax.shard_map(per_device, mesh=mesh, in_specs=(tok_spec, seg_spec, mat_spec, mat_spec, mat_spec, mat_spec, mat_spec, mat_spec, mat_spec, gain_spec, gain_spec), out_specs=tok_spec, check_vma=False)
```

```python
import jax
import jax.numpy as jnp
import numpy as np
from jax import lax
from jax.experimental import pallas as pl
from jax.experimental.pallas import tpu as pltpu
from jax.sharding import PartitionSpec as P

HEAD = 128
HEADS = 12
KV_HEADS = 2
EPS = 1e-5
ROPE_BASE = 10000.0
MESH = pl.DeviceIdType.MESH

N_DEV = 8
TOK = 1024
D = 1536
KV = KV_HEADS * HEAD
FF = 8960
HALF = FF // 2
ROWS = D // N_DEV
FROWS = FF // N_DEV
TF = 640
N_G0 = HALF // TF
N_G1 = FF // TF
DR = 160
N_DN = FROWS // DR
LAYERS = 2
MB = 256
NB = TOK // MB
SCALE = HEAD ** -0.5

RATE = {"X": 46600.0, "Y": 46600.0, "D": 500000.0, "L": 800000.0}
LAT = {"X": 2.5, "Y": 2.5, "D": 1.5, "L": 1.0}
HORIZON = 20.0
T_TABLES, T_WIDEN, T_NORM, T_QKV, T_HEAD, T_PROJ, T_TILE, T_ADD = 3.0, 1.6, 0.4, 1.8, 2.0, 1.1, 6.6, 1.5
OWN_FIRST = 3
N_SEM = 230


class Transfer:
    def __init__(self, key, link, size, n_sem, start, wait, done, deps):
        self.key, self.link, self.size, self.n_sem = key, link, size, n_sem
        self.start, self.wait, self.done, self.deps = start, wait, done, set(deps)
        self.sems = []


class Planner:
    def __init__(self):
        self.now = 0.0
        self.free = dict.fromkeys("XYDL", 0.0)
        self.all, self.queue, self.users, self.mates = {}, {"X": [], "Y": []}, {}, {}
        self.pool = list(range(N_SEM))
        self.issued, self.arrived, self.flying, self.sent, self.ops = set(), set(), [], [], []

    def add(self, tr):
        self.all[tr.key] = tr
        for dep in tr.deps:
            self.users.setdefault(dep, []).append(tr.key)

    def issue(self, key):
        tr = self.all[key]
        self.issued.add(key)
        tr.sems, self.pool = self.pool[:tr.n_sem], self.pool[tr.n_sem:]
        self.ops.append(tr.start)
        self.free[tr.link] = max(self.free[tr.link], self.now) + tr.size / RATE[tr.link]
        self.flying.append((self.free[tr.link] + LAT[tr.link], key))
        for mate in self.mates.get(key, ()):
            if mate not in self.issued and self.all[mate].deps <= self.arrived:
                self.issue(mate)

    def mark(self, key):
        self.arrived.add(key)
        for user in self.users.get(key, ()):
            tr = self.all[user]
            if tr.link in "DL" and user not in self.issued and tr.deps <= self.arrived:
                self.issue(user)

    def receive(self, item):
        self.flying.remove(item)
        tr = self.all[item[1]]
        self.ops.append(tr.wait)
        if tr.done is not None:
            self.sent.append((item[0] + 2.0, item[1]))
        else:
            self.pool += tr.sems
        self.mark(item[1])

    def fill(self):
        for link in "XY":
            while self.free[link] - self.now < HORIZON:
                ready = [k for k in self.queue[link] if self.all[k].deps <= self.arrived]
                if not ready:
                    break
                self.queue[link].remove(ready[0])
                self.issue(ready[0])

    def retire(self, keys=None, everything=False):
        for item in list(self.sent):
            if everything or (keys is not None and item[1] in keys) or (keys is None and item[0] <= self.now):
                self.sent.remove(item)
                self.ops.append(self.all[item[1]].done)
                self.pool += self.all[item[1]].sems

    def service(self):
        while True:
            due = sorted(i for i in self.flying if i[0] <= self.now)
            if not due:
                break
            self.receive(due[0])
            self.fill()
        self.fill()
        self.retire()

    def need(self, keys):
        keys = set(keys)
        while not keys <= self.arrived:
            self.fill()
            item = min(self.flying)
            self.now = max(self.now, item[0])
            self.receive(item)
        self.service()

    def spend(self, us):
        self.now += us

    def take(self):
        ops, self.ops = self.ops, []
        return ops


def run(ops):
    for op in ops:
        op()


def run_at(index, table):
    for k, ops in (table.items() if isinstance(table, dict) else enumerate(table)):
        if ops:
            pl.when(index == k)(lambda ops=ops: run(ops))


def kernel(tok, seg_r, freq, g_attn, g_mlp, w_q, w_k, w_v, w_o, w_g, w_u, w_d,
           out, out_a, out_d, f_q, f_k, f_v, f_o, f_g, f_u, f_d, f_p,
           x, h, q, k, v, o, cos_t, sin_t, mask, vq, vk, vv, vo, vg, vu, vd,
           b_q, b_k, b_v, b_o, b_g, b_u, b_d,
           send, recv, ld):
    me = lax.axis_index("fsdp")
    core = lax.rem(me, 2)
    xc = lax.rem(me // 2, 2)
    yc = me // 4
    xn = me + 2 - 4 * xc
    yn = me + 4 - 8 * yc
    cn = me + 1 - 2 * core
    dg = xn + 4 - 8 * yc

    barrier = pltpu.get_barrier_semaphore()
    for nb in (xn, yn, cn):
        pl.semaphore_signal(barrier, inc=1, device_id={"fsdp": nb}, device_id_type=MESH)
    pl.semaphore_wait(barrier, 3)

    plan = Planner()

    def al(i, n):
        return i if isinstance(i, int) else pl.multiple_of(i, n)

    def view(ref, l, r0, nr, c0, nc):
        return ref.at[l, pl.ds(al(r0, 16), nr), pl.ds(al(c0, 128), nc)]

    def remote(key, link, pairs, dev, deps):
        sizes = [n for n, _ in pairs]

        def each():
            for i, (_, make) in zip(plan.all[key].sems, pairs):
                src, dst = make()
                yield pltpu.make_async_remote_copy(src_ref=src, dst_ref=dst, send_sem=send.at[i], recv_sem=recv.at[i],
                                                   device_id={"fsdp": dev}, device_id_type=MESH)

        plan.add(Transfer(key, link, sum(sizes), len(pairs), lambda: [c.start() for c in each()], lambda: [c.wait_recv() for c in each()],
                          lambda: [c.wait_send() for c in each()], deps))

    def local(key, pairs, deps):
        sizes = [n for n, _ in pairs]

        def each():
            for i, (_, make) in zip(plan.all[key].sems, pairs):
                src, dst = make()
                yield pltpu.make_async_copy(src, dst, send.at[i])

        plan.add(Transfer(key, "L", sum(sizes), len(pairs), lambda: [c.start() for c in each()], lambda: [c.wait() for c in each()], None, deps))

    def add_round(rd):
        kind, l, j = rd
        if kind == "qkv":
            mats = [(w_q, f_q, ROWS, ROWS, 0, D, b_q), (w_k, f_k, ROWS, ROWS, 0, KV, b_k), (w_v, f_v, ROWS, ROWS, 0, KV, b_v)]
        elif kind == "o":
            mats = [(w_o, f_o, ROWS, ROWS, 0, D, b_o)]
        elif kind == "dn":
            mats = [(w_d, f_d, FROWS, DR, j * DR, D, b_d.at[j % 4])]
        else:
            mats = [(w_g, f_g, ROWS, ROWS, j * TF, TF, b_g.at[j % 4]), (w_u, f_u, ROWS, ROWS, j * TF, TF, b_u.at[j % 4])]
        rowwise = kind == "dn"
        paired = l == 0 and kind == "gu"
        col_mine = yc * HALF if paired else 0
        col_other = (1 - yc) * HALF if paired else 0

        def own_src(m, other=False):
            src, _, _, nr, off, nc, _ = m
            r0, c0 = (off, 0) if rowwise else (0, off + (col_other if other else col_mine))
            return view(src, l, r0, nr, c0, nc)

        def held_at(m, dev, part=None, other=False):
            _, dst, span, nr, off, nc, _ = m
            r0, c0 = (off, 0) if rowwise else (0, off + (col_other if other else col_mine))
            cut, n = {None: (0, nr), "A": (0, nr // 2), "B": (nr // 2, nr // 2)}[part]
            return view(dst, l, dev * span + r0 + cut, n, c0, nc)

        def own(other=False):
            return [(2 * m[3] * m[5], lambda m=m: (own_src(m, other), held_at(m, me, other=other))) for m in mats]

        def held(dev, part=None):
            return [(2 * m[3] * m[5] // (2 if part else 1), lambda m=m: (held_at(m, dev, part),) * 2) for m in mats]

        K = lambda t: (rd, t)
        names = ["X", "D", "DX", "bin", "bout"]
        remote(K("X"), "X", own(), xn, [])
        remote(K("D"), "D", own(), cn, [])
        remote(K("DX"), "D", held(xn), cn, [K("X")])
        prev = [((kind, l, j - 4), "bout")] if j >= 4 else ([(("dn", 0, j + 4 if j < 3 else j), "bout")] if kind == "dn" and l == 1 else ([(("gu", 0, j + 4 if j < 3 else j), "bout")] if kind == "gu" and l == 1 else ([((kind, 0, 0), "bout")] if l == 1 else [])))
        local(K("bin"), [(2 * m[3] * m[5], lambda m=m: (own_src(m), m[6])) for m in mats], prev)
        local(K("bout"), [(2 * m[3] * m[5], lambda m=m: (m[6], held_at(m, me))) for m in mats], [K("bin")])
        plan.mates[K("X")] = [K("D"), K("bin")]
        if not (l == 0 and kind == "dn"):
            remote(K("Y"), "Y", own(other=True), yn, [])
            remote(K("DY"), "D", held(yn), cn, [K("Y")])
            names += ["Y", "DY"]
            if l == 0 or kind in ("qkv", "o"):
                remote(K("XR"), "X", held(yn), xn, [K("Y")])
                remote(K("DR"), "D", held(dg), cn, [K("XR")])
                names += ["XR", "DR"]
            else:
                remote(K("XR"), "X", held(yn, "A"), xn, [K("Y")])
                remote(K("YR"), "Y", held(xn, "B"), yn, [K("X")])
                remote(K("DR"), "D", held(dg, "A"), cn, [K("XR")])
                remote(K("DS"), "D", held(dg, "B"), cn, [K("YR")])
                names += ["XR", "YR", "DR", "DS"]
        return [K(n) for n in names]

    needs = {}
    for l, n_gu in ((0, N_G0), (1, N_G1)):
        for rd in [("qkv", l, 0), ("o", l, 0)] + [("dn", l, j) for j in range(N_DN)] + [("gu", l, j) for j in range(n_gu)]:
            needs[rd] = add_round(rd)
    for i in range(NB):
        mine, theirs = pl.ds(i * MB, MB), pl.ds(TOK + i * MB, MB)
        remote(("h", i), "Y", [(2 * MB * D, lambda mine=mine, theirs=theirs: (h.at[mine, :], h.at[theirs, :]))], yn, [("h ready", i)])
        remote(("p", i), "Y", [(4 * MB * D, lambda mine=mine, theirs=theirs: (x.at[theirs, :], f_p.at[mine, :]))], yn, ["p ready"])
    dns = {l: [key for j in range(N_DN) for key in needs[("dn", l, j)]] for l in (0, 1)}

    def seq(kind, l, n, *ts):
        return [((kind, l, j), t) for j in range(n) for t in ts]

    attn = lambda l, t: [(("qkv", l, 0), t), (("o", l, 0), t)]
    plan.queue["X"] = (attn(0, "X") + attn(0, "XR") + seq("dn", 0, N_DN, "X") + seq("gu", 0, N_G0, "X", "XR")
                       + attn(1, "X") + attn(1, "XR") + seq("dn", 1, N_DN, "X", "XR") + seq("gu", 1, N_G1, "X", "XR"))
    plan.queue["Y"] = ([("p", i) for i in range(NB)] + [("h", i) for i in range(NB)] + attn(0, "Y") + seq("gu", 0, N_G0, "Y")
                       + attn(1, "Y") + seq("dn", 1, N_DN, "Y") + seq("dn", 1, N_DN, "YR") + seq("gu", 1, N_G1, "Y", "YR"))

    def rows_of(i):
        return pl.ds(pl.multiple_of(i * MB, MB), MB)

    def load(pairs):
        cps = [pltpu.make_async_copy(s, d, ld.at[i]) for i, (s, d) in enumerate(pairs)]
        for c in cps:
            c.start()
        for c in cps:
            c.wait()

    plan.service()
    run(plan.take())
    tok_in = pltpu.make_async_copy(tok, o, ld.at[0])
    tok_in.start()

    def tables(i, c):
        rows = rows_of(i)
        rr = lax.broadcasted_iota(jnp.int32, (MB, TOK), 0) + i * MB
        cc = lax.broadcasted_iota(jnp.int32, (MB, TOK), 1)
        seg = jnp.broadcast_to(seg_r[...], (MB, TOK)).astype(jnp.float32)
        seg_c = jnp.sum(jnp.where(cc == rr, seg, 0.0), axis=1, keepdims=True)
        ok = jnp.where((seg == seg_c) & (cc <= rr), 1.0, 0.0)
        mask[rows, :] = ok
        pos = jnp.sum(ok, axis=1, keepdims=True) - 1.0
        ang = pos * freq[...]
        lane = lax.broadcasted_iota(jnp.int32, (MB, HEAD), 1)
        cos_t[rows, :] = jnp.cos(ang)
        sn = jnp.sin(ang)
        sin_t[rows, :] = jnp.where(lane < HEAD // 2, -sn, sn)
        return c

    lax.fori_loop(0, NB, tables, 0)
    plan.spend(T_TABLES)
    plan.service()
    run(plan.take())
    tok_in.wait()

    def widen(i, c):
        rows = rows_of(i)
        x[rows, :] = o[rows, :].astype(jnp.float32)
        x[rows_of(i + NB), :] = jnp.zeros((MB, D), jnp.float32)
        return c

    lax.fori_loop(0, NB, widen, 0)
    plan.spend(T_WIDEN)

    def norm_row(gain_ref, l, i):
        rows = rows_of(i)
        xv = x[rows, :]
        inv = lax.rsqrt(jnp.mean(xv * xv, axis=-1, keepdims=True) + EPS)
        h[rows, :] = (xv * inv * gain_ref[l:l + 1, :].astype(jnp.float32)).astype(jnp.bfloat16)

    def rope(val, rows):
        f = val.astype(jnp.bfloat16).astype(jnp.float32)
        return (f * cos_t[rows, :] + pltpu.roll(f, HEAD // 2, 1) * sin_t[rows, :]).astype(jnp.bfloat16)

    def qkv_row(i):
        rows = rows_of(i)
        hv = h[rows, :]
        for g in range(HEADS // 4):
            val = jnp.dot(hv, vq[:, g * 512:(g + 1) * 512], preferred_element_type=jnp.float32)
            for e in range(4):
                q[rows, g * 512 + e * HEAD:g * 512 + (e + 1) * HEAD] = rope(val[:, e * HEAD:(e + 1) * HEAD], rows)
        val = jnp.dot(hv, vk[...], preferred_element_type=jnp.float32)
        for e in range(KV_HEADS):
            k[rows, e * HEAD:(e + 1) * HEAD] = rope(val[:, e * HEAD:(e + 1) * HEAD], rows)
        v[rows, :] = jnp.dot(hv, vv[...], preferred_element_type=jnp.float32).astype(jnp.bfloat16)

    def one_head(hd):
        qc = pl.ds(pl.multiple_of(hd * HEAD, HEAD), HEAD)
        kc = pl.ds(pl.multiple_of((hd // (HEADS // KV_HEADS)) * HEAD, HEAD), HEAD)
        for i in range(NB):
            n = (i + 1) * MB
            s = lax.dot_general(q[i * MB:n, qc], k[0:n, kc], (((1,), (1,)), ((), ())), preferred_element_type=jnp.float32) * SCALE
            s = jnp.where(mask[i * MB:n, 0:n] > 0.5, s, -1e30)
            e = jnp.exp(s - jnp.max(s, axis=1, keepdims=True))
            p = (e / jnp.sum(e, axis=1, keepdims=True)).astype(jnp.bfloat16)
            o[i * MB:n, qc] = jnp.dot(p, v[0:n, kc], preferred_element_type=jnp.float32).astype(jnp.bfloat16)

    def act(hv):
        gt = jnp.dot(hv, vg[...], preferred_element_type=jnp.float32)
        up = jnp.dot(hv, vu[...], preferred_element_type=jnp.float32)
        return (gt * jax.nn.sigmoid(gt) * up).astype(jnp.bfloat16)

    def mlp_row(i, c):
        rows = rows_of(i)
        x[rows, :] += jnp.dot(act(h[rows, :]), vd[...], preferred_element_type=jnp.float32)
        return c

    for l in range(LAYERS):
        plan.need(needs[("qkv", l, 0)])
        run(plan.take())
        load([(f_q.at[l], vq), (f_k.at[l], vk), (f_v.at[l], vv)])
        plan.spend(3.0)
        table = []
        for i in range(NB):
            if l == 1:
                plan.need([("p", i)])
                plan.retire(keys=[("p", i)])
            plan.service()
            table.append(plan.take())
            plan.spend(T_QKV + T_NORM / NB + (T_ADD if l == 1 else 0.0))

        def qkv_step(i, c):
            run_at(i, table)
            if l == 1:
                load([(f_p.at[rows_of(i), :], x.at[rows_of(i + NB), :])])
                x[rows_of(i), :] += x[rows_of(i + NB), :]
            norm_row(g_attn, l, i)
            qkv_row(i)
            return c

        lax.fori_loop(0, NB, qkv_step, 0)

        table_h = []
        for i in range(HEADS):
            plan.service()
            table_h.append(plan.take())
            plan.spend(T_HEAD)

        def head_step(hd, c):
            run_at(hd, table_h)
            one_head(hd)
            return c

        lax.fori_loop(0, HEADS, head_step, 0)

        plan.need(needs[("o", l, 0)])
        run(plan.take())
        load([(f_o.at[l], vo)])
        plan.spend(2.0)
        table_o = []
        for i in range(NB):
            plan.service()
            if l == 0 and i >= 2:
                plan.mark(("h ready", i - 2))
                plan.fill()
            table_o.append(plan.take())
            plan.spend(T_PROJ + T_NORM / NB)

        def proj_step(i, c):
            run_at(i, table_o)
            rows = rows_of(i)
            x[rows, :] += jnp.dot(o[rows, :], vo[...], preferred_element_type=jnp.float32)
            norm_row(g_mlp, l, i)
            return c

        lax.fori_loop(0, NB, proj_step, 0)

        if l == 0:
            items = [(j, 0) for j in range(OWN_FIRST)] + [(j, 1) for j in range(N_G0)] + [(j, 0) for j in range(OWN_FIRST, N_G0)]
        else:
            items = [(j, 0) for j in range(N_G1)]
        table_a, table_b = [], []
        for w, (j, other) in enumerate(items):
            if l == 0 and w < 2:
                plan.mark(("h ready", NB - 2 + w))
            keys = needs[("gu", l, j)] + dns[l] + ([("h", i) for i in range(NB)] if other else [])
            plan.need(keys)
            table_a.append(plan.take())
            plan.spend(2.0)
            if l == 0 and w == OWN_FIRST + N_G0:
                plan.mark("p ready")
            plan.service()
            table_b.append(plan.take())
            plan.spend(T_TILE)

        def tiles(start, stop, base, first):
            def body(t, c):
                run_at(t, {w - base: ops for w, ops in enumerate(table_a) if start <= w < stop})
                cols = pl.ds(pl.multiple_of((yc * HALF if l == 0 else 0) + t * TF, 128), TF)
                load([(f_g.at[l, :, cols], vg), (f_u.at[l, :, cols], vu), (f_d.at[l, cols, :], vd)])
                run_at(t, {w - base: ops for w, ops in enumerate(table_b) if start <= w < stop})
                lax.fori_loop(first, first + NB, mlp_row, 0)
                return c

            lax.fori_loop(start - base, stop - base, body, 0)

        if l == 0:
            tiles(0, OWN_FIRST, 0, 0)
            tiles(OWN_FIRST, OWN_FIRST + N_G0, OWN_FIRST, NB)
            tiles(OWN_FIRST + N_G0, 2 * N_G0, N_G0, 0)
        else:
            tiles(0, N_G1 - 1, 0, 0)
            run(table_a[-1])
            cols = pl.ds(FF - TF, TF)
            load([(f_g.at[l, :, cols], vg), (f_u.at[l, :, cols], vu), (f_d.at[l, cols, :], vd)])
            run(table_b[-1])
            outs = [pltpu.make_async_copy(x.at[pl.ds(0, TOK), :], out, ld.at[0]), pltpu.make_async_copy(vd, out_d, ld.at[1])]
            for c in outs:
                c.start()

            def act_row(i, c):
                rows = rows_of(i)
                q[rows, 0:TF] = act(h[rows, :])
                return c

            lax.fori_loop(0, NB, act_row, 0)

    plan.need(plan.all)
    plan.retire(everything=True)
    run(plan.take())
    for c in outs:
        c.wait()
    load([(q.at[:, pl.ds(0, TF)], out_a)])


def solution(mesh):
    tok_spec = P(("rep", "fsdp"), None)
    seg_spec = P(("rep", "fsdp"))
    mat_spec = P(None, "fsdp", None)
    gain_spec = P(None, None)
    bf, f32 = jnp.bfloat16, jnp.float32

    def per_device(tokens, seg_ids, w_q, w_k, w_v, w_o, w_gate, w_up, w_down, g_attn, g_mlp):
        half = HEAD // 2
        inv = np.float32(ROPE_BASE) ** (-np.arange(half, dtype=np.float32) / np.float32(half))
        freq = jnp.asarray(np.concatenate([inv, inv]).reshape(1, HEAD), f32)
        any_s = pl.BlockSpec(memory_space=pl.ANY)
        vm = pl.BlockSpec(memory_space=pltpu.VMEM)
        full = [(LAYERS, D, D), (LAYERS, D, KV), (LAYERS, D, KV), (LAYERS, D, D), (LAYERS, D, FF), (LAYERS, D, FF), (LAYERS, FF, D)]
        res = pl.pallas_call(
            kernel,
            out_shape=[jax.ShapeDtypeStruct((TOK, D), f32), jax.ShapeDtypeStruct((TOK, TF), bf), jax.ShapeDtypeStruct((TF, D), bf)] + [jax.ShapeDtypeStruct(s, bf) for s in full] + [jax.ShapeDtypeStruct((TOK, D), f32)],
            in_specs=[any_s, vm, vm, vm, vm] + [any_s] * 7,
            out_specs=[any_s] * 11,
            scratch_shapes=[
                pltpu.VMEM((2 * TOK, D), f32), pltpu.VMEM((2 * TOK, D), bf), pltpu.VMEM((TOK, D), bf),
                pltpu.VMEM((TOK, KV), bf), pltpu.VMEM((TOK, KV), bf), pltpu.VMEM((TOK, D), bf),
                pltpu.VMEM((TOK, HEAD), f32), pltpu.VMEM((TOK, HEAD), f32), pltpu.VMEM((TOK, TOK), f32),
                pltpu.VMEM((D, D), bf), pltpu.VMEM((D, KV), bf), pltpu.VMEM((D, KV), bf), pltpu.VMEM((D, D), bf),
                pltpu.VMEM((D, TF), bf), pltpu.VMEM((D, TF), bf), pltpu.VMEM((TF, D), bf),
                pltpu.VMEM((ROWS, D), bf), pltpu.VMEM((ROWS, KV), bf), pltpu.VMEM((ROWS, KV), bf), pltpu.VMEM((ROWS, D), bf),
                pltpu.VMEM((4, ROWS, TF), bf), pltpu.VMEM((4, ROWS, TF), bf), pltpu.VMEM((4, DR, D), bf),
                pltpu.SemaphoreType.DMA((N_SEM,)), pltpu.SemaphoreType.DMA((N_SEM,)), pltpu.SemaphoreType.DMA((4,)),
            ],
            compiler_params=pltpu.CompilerParams(collective_id=0, has_side_effects=True, vmem_limit_bytes=66 * 1000 * 1000),
        )(tokens, seg_ids.reshape(1, TOK), freq, g_attn, g_mlp, w_q, w_k, w_v, w_o, w_gate, w_up, w_down)
        return res[0] + jnp.dot(res[1], res[2], preferred_element_type=f32)

    return jax.shard_map(per_device, mesh=mesh, in_specs=(tok_spec, seg_spec, mat_spec, mat_spec, mat_spec, mat_spec, mat_spec, mat_spec, mat_spec, gain_spec, gain_spec), out_specs=tok_spec, check_vma=False)
```

```python
import jax
import jax.numpy as jnp
import numpy as np
from jax import lax
from jax.experimental import pallas as pl
from jax.experimental.pallas import tpu as pltpu
from jax.sharding import PartitionSpec as P

HEAD = 128
HEADS = 12
KV_HEADS = 2
EPS = 1e-5
ROPE_BASE = 10000.0
MESH = pl.DeviceIdType.MESH

N_DEV = 8
TOK = 1024
D = 1536
KV = KV_HEADS * HEAD
FF = 8960
HALF = FF // 2
ROWS = D // N_DEV
FROWS = FF // N_DEV
TF = 640
N_G0 = HALF // TF
TP_TILES = (1, 2, 3, 4, 5)
N_DP = 4
DR = 160
N_DT = 5
N_DD = 2
N_DN = FROWS // DR
LAYERS = 2
MB = 256
NB = TOK // MB
SCALE = HEAD ** -0.5

RATE = {"X": 46600.0, "Y": 46600.0, "D": 500000.0, "L": 800000.0}
LAT = {"X": 2.5, "Y": 2.5, "D": 1.5, "L": 1.0}
HORIZON = 20.0
T_TABLES, T_WIDEN, T_NORM, T_QKV, T_HEAD, T_PROJ, T_TILE, T_ADD = 3.0, 1.6, 0.4, 1.8, 2.0, 1.1, 6.6, 1.5
OWN_FIRST = 3
L1_ORDER = ("lo", "hi", "own", "dp")
N_SEM = 230


class Transfer:
    def __init__(self, key, link, size, n_sem, start, wait, done, deps):
        self.key, self.link, self.size, self.n_sem = key, link, size, n_sem
        self.start, self.wait, self.done, self.deps = start, wait, done, set(deps)
        self.sems = []


class Planner:
    def __init__(self):
        self.now = 0.0
        self.free = dict.fromkeys("XYDL", 0.0)
        self.all, self.queue, self.users, self.mates = {}, {"X": [], "Y": []}, {}, {}
        self.pool = list(range(N_SEM))
        self.issued, self.arrived, self.flying, self.sent, self.ops = set(), set(), [], [], []

    def add(self, tr):
        self.all[tr.key] = tr
        for dep in tr.deps:
            self.users.setdefault(dep, []).append(tr.key)

    def issue(self, key):
        tr = self.all[key]
        self.issued.add(key)
        tr.sems, self.pool = self.pool[:tr.n_sem], self.pool[tr.n_sem:]
        self.ops.append(tr.start)
        self.free[tr.link] = max(self.free[tr.link], self.now) + tr.size / RATE[tr.link]
        self.flying.append((self.free[tr.link] + LAT[tr.link], key))
        for mate in self.mates.get(key, ()):
            if mate not in self.issued and self.all[mate].deps <= self.arrived:
                self.issue(mate)

    def mark(self, key):
        self.arrived.add(key)
        for user in self.users.get(key, ()):
            tr = self.all[user]
            if tr.link in "DL" and user not in self.issued and tr.deps <= self.arrived:
                self.issue(user)

    def receive(self, item):
        self.flying.remove(item)
        tr = self.all[item[1]]
        self.ops.append(tr.wait)
        if tr.done is not None:
            self.sent.append((item[0] + 2.0, item[1]))
        else:
            self.pool += tr.sems
        self.mark(item[1])

    def fill(self):
        for link in "XY":
            while self.free[link] - self.now < HORIZON:
                ready = [k for k in self.queue[link] if self.all[k].deps <= self.arrived]
                if not ready:
                    break
                self.queue[link].remove(ready[0])
                self.issue(ready[0])

    def retire(self, keys=None, everything=False):
        for item in list(self.sent):
            if everything or (keys is not None and item[1] in keys) or (keys is None and item[0] <= self.now):
                self.sent.remove(item)
                self.ops.append(self.all[item[1]].done)
                self.pool += self.all[item[1]].sems

    def service(self):
        while True:
            due = sorted(i for i in self.flying if i[0] <= self.now)
            if not due:
                break
            self.receive(due[0])
            self.fill()
        self.fill()
        self.retire()

    def need(self, keys):
        keys = set(keys)
        while not keys <= self.arrived:
            self.fill()
            item = min(self.flying)
            self.now = max(self.now, item[0])
            self.receive(item)
        self.service()

    def spend(self, us):
        self.now += us

    def take(self):
        ops, self.ops = self.ops, []
        return ops


def run(ops):
    for op in ops:
        op()


def run_at(index, table):
    for k, ops in (table.items() if isinstance(table, dict) else enumerate(table)):
        if ops:
            pl.when(index == k)(lambda ops=ops: run(ops))


def kernel(tok, seg_r, freq, g_attn, g_mlp, w_q, w_k, w_v, w_o, w_g, w_u, w_d,
           out, out_p, f_q, f_k, f_v, f_o, f_g, f_u, f_d, f_p,
           x, h, q, k, v, o, cos_t, sin_t, mask, vq, vk, vv, vo, vg, vu, vd,
           b_q, b_k, b_v, b_o, b_g, b_u, b_d,
           send, recv, ld):
    me = lax.axis_index("fsdp")
    core = lax.rem(me, 2)
    xc = lax.rem(me // 2, 2)
    yc = me // 4
    xn = me + 2 - 4 * xc
    yn = me + 4 - 8 * yc
    cn = me + 1 - 2 * core
    dg = xn + 4 - 8 * yc

    barrier = pltpu.get_barrier_semaphore()
    for nb in (xn, yn, cn):
        pl.semaphore_signal(barrier, inc=1, device_id={"fsdp": nb}, device_id_type=MESH)
    pl.semaphore_wait(barrier, 3)

    plan = Planner()

    def al(i, n):
        return i if isinstance(i, int) else pl.multiple_of(i, n)

    def view(ref, l, r0, nr, c0, nc):
        return ref.at[l, pl.ds(al(r0, 16), nr), pl.ds(al(c0, 128), nc)]

    def remote(key, link, pairs, dev, deps):
        sizes = [n for n, _ in pairs]

        def each():
            for i, (_, make) in zip(plan.all[key].sems, pairs):
                src, dst = make()
                yield pltpu.make_async_remote_copy(src_ref=src, dst_ref=dst, send_sem=send.at[i], recv_sem=recv.at[i],
                                                   device_id={"fsdp": dev}, device_id_type=MESH)

        plan.add(Transfer(key, link, sum(sizes), len(pairs), lambda: [c.start() for c in each()], lambda: [c.wait_recv() for c in each()],
                          lambda: [c.wait_send() for c in each()], deps))

    def local(key, pairs, deps):
        sizes = [n for n, _ in pairs]

        def each():
            for i, (_, make) in zip(plan.all[key].sems, pairs):
                src, dst = make()
                yield pltpu.make_async_copy(src, dst, send.at[i])

        plan.add(Transfer(key, "L", sum(sizes), len(pairs), lambda: [c.start() for c in each()], lambda: [c.wait() for c in each()], None, deps))

    def block(src, dst, l, col, other_col, nc, stage):
        def at(dev, other=False):
            return view(dst, l, dev * ROWS, ROWS, other_col if other else col, nc)

        def part(dev, p):
            return view(dst, l, dev * ROWS + (ROWS // 2) * p, ROWS // 2, col, nc)
        return (2 * ROWS * nc, lambda other=False: view(src, l, 0, ROWS, other_col if other else col, nc), at, stage)

    def down_block(l, j, stage):
        return (2 * DR * D, lambda other=False: view(w_d, l, j * DR, DR, 0, D), lambda dev, other=False: view(f_d, l, dev * FROWS + j * DR, DR, 0, D), stage)

    def shared_block(row_of):
        at = lambda dev, other=False: view(f_d, 1, row_of(dev), DR, 0, D)
        return (2 * DR * D, lambda other=False: at(me), at, None)

    def place(dev):
        return dev // 4, lax.rem(dev // 2, 2), lax.rem(dev, 2)

    def tp_row(j):
        def row(dev):
            yy, xx, cc = place(dev)
            return yy * HALF + xx * (2 * FROWS) + TF * (1 - xx) + (N_DT * DR) * cc + j * DR
        return row

    def dp_row(j):
        def row(dev):
            yy, xx, cc = place(dev)
            return yy * HALF + xx * (2 * FROWS) + (2 * FROWS - TF) * xx + (N_DD * DR) * cc + j * DR
        return row

    def add_round(rd, mats, parts, deps=(), before=None):
        K = lambda t: (rd, t)

        def own(other=False):
            return [(m[0], lambda m=m: (m[1](other), m[2](me, other))) for m in mats]

        def held(dev):
            return [(m[0], lambda m=m: (m[2](dev), m[2](dev))) for m in mats]

        for t in parts:
            if t == "X":
                remote(K(t), "X", own(), xn, deps)
            elif t == "Y":
                remote(K(t), "Y", own(other=True), yn, deps)
            elif t == "D":
                remote(K(t), "D", own(), cn, [])
            elif t == "XR":
                remote(K(t), "X", held(yn), xn, [K("Y")])
            elif t == "DX":
                remote(K(t), "D", held(xn), cn, [K("X")])
            elif t == "DY":
                remote(K(t), "D", held(yn), cn, [K("Y")])
            elif t == "DR":
                remote(K(t), "D", held(dg), cn, [K("XR")])
            elif t == "bin":
                local(K(t), [(m[0], lambda m=m: (m[1](), m[3])) for m in mats], [before] if before else [])
            else:
                local(K(t), [(m[0], lambda m=m: (m[3], m[2](me))) for m in mats], [K("bin")])
        if "D" in parts and "X" in parts:
            plan.mates[K("X")] = [K("D"), K("bin")]
        needs[rd] = [K(t) for t in parts]

    needs = {}
    FULL = ("X", "Y", "D", "XR", "DX", "DY", "DR", "bin", "bout")
    for l in (0, 1):
        add_round(("qkv", l), [block(w_q, f_q, l, 0, 0, D, b_q), block(w_k, f_k, l, 0, 0, KV, b_k), block(w_v, f_v, l, 0, 0, KV, b_v)], FULL,
                  before=(("qkv", 0), "bout") if l else None)
        add_round(("o", l), [block(w_o, f_o, l, 0, 0, D, b_o)], FULL, before=(("o", 0), "bout") if l else None)
    dn_seq = [("dn", l, j) for l in (0, 1) for j in range(N_DN)]
    for n, rd in enumerate(dn_seq):
        add_round(rd, [down_block(rd[1], rd[2], b_d.at[n % 4])], ("X", "D", "DX", "bin", "bout") if rd[1] == 0 else ("D", "bin", "bout"),
                  before=(dn_seq[n - 4], "bout") if n >= 4 else None)
    dn1 = [key for j in range(N_DN) for key in needs[("dn", 1, j)]]
    for j in range(N_DT):
        add_round(("dt", j), [shared_block(tp_row(j))], ("X", "DX"), deps=dn1)
    for j in range(N_DD):
        add_round(("dd", j), [shared_block(dp_row(j))], ("X", "Y", "XR", "DX", "DY", "DR"), deps=dn1)
    gu_seq = [("gu", j) for j in range(N_G0)] + [("gt", j) for j in TP_TILES] + [("gd", j) for j in range(N_DP)]
    for n, rd in enumerate(gu_seq):
        kind, j = rd
        l = 0 if kind == "gu" else 1
        if kind == "gd":
            col = (j % 2) * HALF + (j // 2) * (HALF - TF)
            other = col
        else:
            col, other = yc * HALF + j * TF, (1 - yc) * HALF + j * TF
        add_round(rd, [block(w_g, f_g, l, col, other, TF, b_g.at[n % 4]), block(w_u, f_u, l, col, other, TF, b_u.at[n % 4])], FULL,
                  before=(gu_seq[n - 4], "bout") if n >= 4 else None)
    for j in range(N_DN):
        plan.mates[(("gu", j), "X")] += [(("dn", 1, j), "D"), (("dn", 1, j), "bin")]
    for i in range(NB):
        mine, theirs = pl.ds(i * MB, MB), pl.ds(TOK + i * MB, MB)
        for l, land in ((0, f_p), (1, out_p)):
            remote(("h", l, i), "Y", [(2 * MB * D, lambda mine=mine, theirs=theirs: (h.at[mine, :], h.at[theirs, :]))], yn, [("h ready", l, i)])
            remote(("p", l, i), "Y", [(4 * MB * D, lambda mine=mine, theirs=theirs, land=land: (x.at[theirs, :], land.at[mine, :]))], yn, [("p ready", l, i)])

    def seq(rds, *ts):
        return [(rd, t) for rd in rds for t in ts]

    attn = lambda l: [("qkv", l), ("o", l)]
    gus, gts, gds = [("gu", j) for j in range(N_G0)], [("gt", j) for j in TP_TILES], [("gd", j) for j in range(N_DP)]
    dts, dds = [("dt", j) for j in range(N_DT)], [("dd", j) for j in range(N_DD)]
    plan.queue["X"] = (seq(attn(0), "X") + seq(attn(0), "XR") + seq(dn_seq[:N_DN], "X") + seq(gus, "X", "XR")
                       + seq(attn(1), "X") + seq(attn(1), "XR") + seq(dts, "X") + seq(gts, "X", "XR") + seq(dds, "X", "XR") + seq(gds, "X", "XR"))
    tok_sends = [(c, l, i) for c, l in (("p", 0), ("h", 0), ("h", 1), ("p", 1)) for i in range(NB)]
    plan.queue["Y"] = tok_sends + seq(attn(0), "Y") + seq(gus, "Y") + seq(attn(1), "Y") + seq(gts, "Y") + seq(dds, "Y") + seq(gds, "Y")

    def rows_of(i):
        return pl.ds(i * MB if isinstance(i, int) else pl.multiple_of(i * MB, MB), MB)

    def load(pairs):
        cps = [pltpu.make_async_copy(s, d, ld.at[i]) for i, (s, d) in enumerate(pairs)]
        for c in cps:
            c.start()
        for c in cps:
            c.wait()

    plan.service()
    run(plan.take())
    tok_in = pltpu.make_async_copy(tok, o, ld.at[0])
    tok_in.start()

    def tables(i, c):
        rows = rows_of(i)
        rr = lax.broadcasted_iota(jnp.int32, (MB, TOK), 0) + i * MB
        cc = lax.broadcasted_iota(jnp.int32, (MB, TOK), 1)
        seg = jnp.broadcast_to(seg_r[...], (MB, TOK)).astype(jnp.float32)
        seg_c = jnp.sum(jnp.where(cc == rr, seg, 0.0), axis=1, keepdims=True)
        ok = jnp.where((seg == seg_c) & (cc <= rr), 1.0, 0.0)
        mask[rows, :] = ok
        pos = jnp.sum(ok, axis=1, keepdims=True) - 1.0
        ang = pos * freq[...]
        lane = lax.broadcasted_iota(jnp.int32, (MB, HEAD), 1)
        cos_t[rows, :] = jnp.cos(ang)
        sn = jnp.sin(ang)
        sin_t[rows, :] = jnp.where(lane < HEAD // 2, -sn, sn)
        return c

    lax.fori_loop(0, NB, tables, 0)
    plan.spend(T_TABLES)
    plan.service()
    run(plan.take())
    tok_in.wait()

    def widen(i, c):
        rows = rows_of(i)
        x[rows, :] = o[rows, :].astype(jnp.float32)
        x[rows_of(i + NB), :] = jnp.zeros((MB, D), jnp.float32)
        return c

    lax.fori_loop(0, NB, widen, 0)
    plan.spend(T_WIDEN)

    def norm_row(gain_ref, l, i):
        rows = rows_of(i)
        xv = x[rows, :]
        inv = lax.rsqrt(jnp.mean(xv * xv, axis=-1, keepdims=True) + EPS)
        h[rows, :] = (xv * inv * gain_ref[l:l + 1, :].astype(jnp.float32)).astype(jnp.bfloat16)

    def rope(val, rows):
        f = val.astype(jnp.bfloat16).astype(jnp.float32)
        return (f * cos_t[rows, :] + pltpu.roll(f, HEAD // 2, 1) * sin_t[rows, :]).astype(jnp.bfloat16)

    def qkv_row(i):
        rows = rows_of(i)
        hv = h[rows, :]
        for g in range(HEADS // 4):
            val = jnp.dot(hv, vq[:, g * 512:(g + 1) * 512], preferred_element_type=jnp.float32)
            for e in range(4):
                q[rows, g * 512 + e * HEAD:g * 512 + (e + 1) * HEAD] = rope(val[:, e * HEAD:(e + 1) * HEAD], rows)
        val = jnp.dot(hv, vk[...], preferred_element_type=jnp.float32)
        for e in range(KV_HEADS):
            k[rows, e * HEAD:(e + 1) * HEAD] = rope(val[:, e * HEAD:(e + 1) * HEAD], rows)
        v[rows, :] = jnp.dot(hv, vv[...], preferred_element_type=jnp.float32).astype(jnp.bfloat16)

    def one_head(hd, blocks):
        qc = pl.ds(pl.multiple_of(hd * HEAD, HEAD), HEAD)
        kc = pl.ds(pl.multiple_of((hd // (HEADS // KV_HEADS)) * HEAD, HEAD), HEAD)
        for i in blocks:
            n = (i + 1) * MB
            s = lax.dot_general(q[i * MB:n, qc], k[0:n, kc], (((1,), (1,)), ((), ())), preferred_element_type=jnp.float32) * SCALE
            s = jnp.where(mask[i * MB:n, 0:n] > 0.5, s, -1e30)
            e = jnp.exp(s - jnp.max(s, axis=1, keepdims=True))
            p = (e / jnp.sum(e, axis=1, keepdims=True)).astype(jnp.bfloat16)
            o[i * MB:n, qc] = jnp.dot(p, v[0:n, kc], preferred_element_type=jnp.float32).astype(jnp.bfloat16)

    def act(hv):
        gt = jnp.dot(hv, vg[...], preferred_element_type=jnp.float32)
        up = jnp.dot(hv, vu[...], preferred_element_type=jnp.float32)
        return (gt * jax.nn.sigmoid(gt) * up).astype(jnp.bfloat16)

    def mlp_row(i, c):
        rows = rows_of(i)
        x[rows, :] += jnp.dot(act(h[rows, :]), vd[...], preferred_element_type=jnp.float32)
        return c

    def get_qkv(l):
        plan.need(needs[("qkv", l)])
        run(plan.take())
        load([(f_q.at[l], vq), (f_k.at[l], vk), (f_v.at[l], vv)])
        plan.spend(3.0)

    def get_o(l):
        plan.need(needs[("o", l)])
        run(plan.take())
        load([(f_o.at[l], vo)])
        plan.spend(2.0)

    def heads(blocks):
        table = []
        for i in range(HEADS):
            if i % 2 == 0 or len(blocks) == NB:
                plan.service()
            table.append(plan.take())
            plan.spend(T_HEAD * sum(b + 1 for b in blocks) / 10)

        def head_step(hd, c):
            run_at(hd, table)
            one_head(hd, blocks)
            return c

        lax.fori_loop(0, HEADS, head_step, 0)

    def proj_row(l, i):
        rows = rows_of(i)
        x[rows, :] += jnp.dot(o[rows, :], vo[...], preferred_element_type=jnp.float32)
        norm_row(g_mlp, l, i)

    def tiles(l, steps, offset, first, n_rows, marks=None):
        pre, post = {}, {}
        for n, (t, keys) in enumerate(steps):
            for key in (marks or {}).get((n, "pre"), ()):
                plan.mark(key)
            plan.need(keys)
            pre[t] = plan.take()
            plan.spend(2.2)
            for key in (marks or {}).get((n, "post"), ()):
                plan.mark(key)
            plan.service()
            post[t] = plan.take()
            plan.spend(T_TILE * n_rows / NB)

        def body(t, c):
            run_at(t, pre)
            cols = pl.ds(pl.multiple_of(offset(t), 128), TF)
            load([(f_g.at[l, :, cols], vg), (f_u.at[l, :, cols], vu), (f_d.at[l, cols, :], vd)])
            run_at(t, post)
            lax.fori_loop(first, first + n_rows, mlp_row, 0)
            return c

        lax.fori_loop(steps[0][0], steps[-1][0] + 1, body, 0)

    get_qkv(0)
    table_q = []
    for i in range(NB):
        plan.service()
        table_q.append(plan.take())
        plan.spend(T_QKV + T_NORM)

    def qkv_step(i, c):
        run_at(i, table_q)
        norm_row(g_attn, 0, i)
        qkv_row(i)
        return c

    lax.fori_loop(0, NB, qkv_step, 0)
    heads(range(NB))
    get_o(0)
    table_o = []
    for i in range(NB):
        plan.service()
        if i >= 2:
            plan.mark(("h ready", 0, i - 2))
            plan.fill()
        table_o.append(plan.take())
        plan.spend(T_PROJ + T_NORM)

    def proj_step(i, c):
        run_at(i, table_o)
        proj_row(0, i)
        return c

    lax.fori_loop(0, NB, proj_step, 0)

    dn0 = [key for j in range(N_DN) for key in needs[("dn", 0, j)]]
    half_off = lambda t: yc * HALF + t * TF
    steps = [(j, needs[("gu", j)] + dn0) for j in range(N_G0)]
    got_h = lambda l, *chunks: [("h", l, i) for i in chunks]
    tiles(0, steps[:OWN_FIRST], half_off, 0, NB, {(0, "pre"): [("h ready", 0, NB - 2)], (0, "post"): [("h ready", 0, NB - 1)]})
    tiles(0, [(j, keys + got_h(0, *range(NB))) for j, keys in steps], half_off, NB, NB)
    tiles(0, steps[OWN_FIRST:], half_off, 0, NB, {(0, "post"): [("p ready", 0, i) for i in range(NB)]})

    get_qkv(1)
    for i in range(NB):
        plan.need([("p", 0, i)])
        plan.retire(keys=[("p", 0, i)])
        if i:
            plan.mark(("h ready", 1, i - 1))
            plan.service()
        run(plan.take())
        load([(f_p.at[rows_of(i), :], x.at[rows_of(i + NB), :])])
        x[rows_of(i), :] += x[rows_of(i + NB), :]
        x[rows_of(i + NB), :] = jnp.zeros((MB, D), jnp.float32)
        norm_row(g_attn, 1, i)
        qkv_row(i)
        plan.spend(T_QKV + T_NORM + T_ADD)
        heads([i])
        if i == 0:
            get_o(1)
        proj_row(1, i)
        plan.spend(T_PROJ + T_NORM)

    dt1 = dn1 + [key for j in range(N_DT) for key in needs[("dt", j)]]
    dd1 = dn1 + [key for j in range(N_DD) for key in needs[("dd", j)]]
    steps = [(j, needs[("gt", j)] + dt1) for j in TP_TILES]
    h_mark = {(0, "pre"): [("h ready", 1, NB - 1)]}
    run_order = L1_ORDER
    marks = {}
    for n, what in enumerate(run_order):
        if what == "own":
            tiles(1, steps, half_off, 0, NB, {**h_mark, **marks})
            marks, h_mark = {}, {}
        elif what in ("lo", "hi"):
            chunks = (0, 1) if what == "lo" else (2, 3)
            tiles(1, [(j, keys + got_h(1, *chunks)) for j, keys in steps], half_off, NB + chunks[0], 2, {**h_mark, **marks})
            marks, h_mark = {(0, "post"): [("p ready", 1, i) for i in chunks]}, {}
        else:
            tiles(1, [(j, needs[("gd", j)] + dd1) for j in range(N_DP)],
                  lambda t: lax.rem(t, 2) * HALF + lax.div(t, 2) * (HALF - TF), 0, NB, {**h_mark, **marks})
            marks, h_mark = {}, {}

    done = pltpu.make_async_copy(x.at[pl.ds(0, TOK), :], out, ld.at[0])
    done.start()
    plan.need(plan.all)
    plan.retire(everything=True)
    run(plan.take())
    done.wait()


def solution(mesh):
    tok_spec = P(("rep", "fsdp"), None)
    seg_spec = P(("rep", "fsdp"))
    mat_spec = P(None, "fsdp", None)
    gain_spec = P(None, None)
    bf, f32 = jnp.bfloat16, jnp.float32

    def per_device(tokens, seg_ids, w_q, w_k, w_v, w_o, w_gate, w_up, w_down, g_attn, g_mlp):
        half = HEAD // 2
        inv = np.float32(ROPE_BASE) ** (-np.arange(half, dtype=np.float32) / np.float32(half))
        freq = jnp.asarray(np.concatenate([inv, inv]).reshape(1, HEAD), f32)
        any_s = pl.BlockSpec(memory_space=pl.ANY)
        vm = pl.BlockSpec(memory_space=pltpu.VMEM)
        full = [(LAYERS, D, D), (LAYERS, D, KV), (LAYERS, D, KV), (LAYERS, D, D), (LAYERS, D, FF), (LAYERS, D, FF), (LAYERS, FF, D)]
        res = pl.pallas_call(
            kernel,
            out_shape=[jax.ShapeDtypeStruct((TOK, D), f32)] * 2 + [jax.ShapeDtypeStruct(s, bf) for s in full] + [jax.ShapeDtypeStruct((TOK, D), f32)],
            in_specs=[any_s, vm, vm, vm, vm] + [any_s] * 7,
            out_specs=[any_s] * 10,
            scratch_shapes=[
                pltpu.VMEM((2 * TOK, D), f32), pltpu.VMEM((2 * TOK, D), bf), pltpu.VMEM((TOK, D), bf),
                pltpu.VMEM((TOK, KV), bf), pltpu.VMEM((TOK, KV), bf), pltpu.VMEM((TOK, D), bf),
                pltpu.VMEM((TOK, HEAD), f32), pltpu.VMEM((TOK, HEAD), f32), pltpu.VMEM((TOK, TOK), f32),
                pltpu.VMEM((D, D), bf), pltpu.VMEM((D, KV), bf), pltpu.VMEM((D, KV), bf), pltpu.VMEM((D, D), bf),
                pltpu.VMEM((D, TF), bf), pltpu.VMEM((D, TF), bf), pltpu.VMEM((TF, D), bf),
                pltpu.VMEM((ROWS, D), bf), pltpu.VMEM((ROWS, KV), bf), pltpu.VMEM((ROWS, KV), bf), pltpu.VMEM((ROWS, D), bf),
                pltpu.VMEM((4, ROWS, TF), bf), pltpu.VMEM((4, ROWS, TF), bf), pltpu.VMEM((4, DR, D), bf),
                pltpu.SemaphoreType.DMA((N_SEM,)), pltpu.SemaphoreType.DMA((N_SEM,)), pltpu.SemaphoreType.DMA((4,)),
            ],
            compiler_params=pltpu.CompilerParams(collective_id=0, has_side_effects=True, vmem_limit_bytes=66 * 1000 * 1000),
        )(tokens, seg_ids.reshape(1, TOK), freq, g_attn, g_mlp, w_q, w_k, w_v, w_o, w_gate, w_up, w_down)
        return res[0] + res[1]

    return jax.shard_map(per_device, mesh=mesh, in_specs=(tok_spec, seg_spec, mat_spec, mat_spec, mat_spec, mat_spec, mat_spec, mat_spec, mat_spec, gain_spec, gain_spec), out_specs=tok_spec, check_vma=False)
```

```python
import jax
import jax.numpy as jnp
import numpy as np
from jax import lax
from jax.experimental import pallas as pl
from jax.experimental.pallas import tpu as pltpu
from jax.sharding import PartitionSpec as P

HEAD = 128
HEADS = 12
KV_HEADS = 2
EPS = 1e-5
ROPE_BASE = 10000.0
MESH = pl.DeviceIdType.MESH

N_DEV = 8
TOK = 1024
D = 1536
KV = KV_HEADS * HEAD
FF = 8960
HALF = FF // 2
ROWS = D // N_DEV
FROWS = FF // N_DEV
TF = 640
N_G0 = HALF // TF
TP_TILES = (1, 2, 3, 4, 5)
N_DP = 4
DR = 160
N_DT = 5
N_DD = 2
N_DN = FROWS // DR
LAYERS = 2
MB = 256
NB = TOK // MB
SCALE = HEAD ** -0.5

RATE = {"X": 46600.0, "Y": 46600.0, "D": 500000.0, "L": 800000.0}
LAT = {"X": 2.5, "Y": 2.5, "D": 1.5, "L": 1.0}
HORIZON = 20.0
T_TABLES, T_WIDEN, T_NORM, T_QKV, T_HEAD, T_PROJ, T_TILE, T_ADD = 3.0, 1.6, 0.4, 1.8, 2.0, 1.1, 6.6, 1.5
OWN_FIRST = 3
L1_ORDER = ("lo", "hi", "own", "dp")
TOKEN_ORDER = [(c, l, i) for c, l in (("h", 0), ("p", 0), ("h", 1), ("p", 1)) for i in range(NB)]
N_SEM = 230
FB = 128


class Transfer:
    def __init__(self, key, link, size, n_sem, start, wait, done, deps):
        self.key, self.link, self.size, self.n_sem = key, link, size, n_sem
        self.start, self.wait, self.done, self.deps = start, wait, done, set(deps)
        self.sems = []


class Planner:
    def __init__(self):
        self.now = 0.0
        self.free = dict.fromkeys("XYDL", 0.0)
        self.all, self.queue, self.users, self.mates = {}, {"X": [], "Y": []}, {}, {}
        self.pool = list(range(N_SEM))
        self.issued, self.arrived, self.flying, self.sent, self.ops = set(), set(), [], [], []

    def add(self, tr):
        self.all[tr.key] = tr
        for dep in tr.deps:
            self.users.setdefault(dep, []).append(tr.key)

    def issue(self, key):
        tr = self.all[key]
        self.issued.add(key)
        tr.sems, self.pool = self.pool[:tr.n_sem], self.pool[tr.n_sem:]
        self.ops.append(tr.start)
        self.free[tr.link] = max(self.free[tr.link], self.now) + tr.size / RATE[tr.link]
        self.flying.append((self.free[tr.link] + LAT[tr.link], key))
        for mate in self.mates.get(key, ()):
            if mate not in self.issued and self.all[mate].deps <= self.arrived:
                self.issue(mate)

    def mark(self, key):
        self.arrived.add(key)
        for user in self.users.get(key, ()):
            tr = self.all[user]
            if tr.link in "DL" and user not in self.issued and tr.deps <= self.arrived:
                self.issue(user)

    def receive(self, item):
        self.flying.remove(item)
        tr = self.all[item[1]]
        self.ops.append(tr.wait)
        if tr.done is not None:
            self.sent.append((item[0] + 2.0, item[1]))
        else:
            self.pool += tr.sems
        self.mark(item[1])

    def fill(self):
        for link in "XY":
            while self.free[link] - self.now < HORIZON:
                ready = [k for k in self.queue[link] if self.all[k].deps <= self.arrived]
                if not ready:
                    break
                self.queue[link].remove(ready[0])
                self.issue(ready[0])

    def retire(self, keys=None, everything=False):
        for item in list(self.sent):
            if everything or (keys is not None and item[1] in keys) or (keys is None and item[0] <= self.now):
                self.sent.remove(item)
                self.ops.append(self.all[item[1]].done)
                self.pool += self.all[item[1]].sems

    def service(self):
        while True:
            due = sorted(i for i in self.flying if i[0] <= self.now)
            if not due:
                break
            self.receive(due[0])
            self.fill()
        self.fill()
        self.retire()

    def need(self, keys):
        keys = set(keys)
        while not keys <= self.arrived:
            self.fill()
            item = min(self.flying)
            self.now = max(self.now, item[0])
            self.receive(item)
        self.service()

    def spend(self, us):
        self.now += us

    def take(self):
        ops, self.ops = self.ops, []
        return ops


def run(ops):
    for op in ops:
        op()


def run_at(index, table):
    for k, ops in (table.items() if isinstance(table, dict) else enumerate(table)):
        if ops:
            pl.when(index == k)(lambda ops=ops: run(ops))


def kernel(tok, seg_r, freq, g_attn, g_mlp, w_q, w_k, w_v, w_o, w_g, w_u, w_d,
           out, f_r, f_q, f_k, f_v, f_o, f_g, f_u, f_d, f_p,
           x, h, q, k, v, o, cos_t, sin_t, mask, vq, vk, vv, vo, vg, vu, vd,
           b_q, b_k, b_v, b_o, b_g, b_u, b_d,
           send, recv, ld):
    me = lax.axis_index("fsdp")
    core = lax.rem(me, 2)
    xc = lax.rem(me // 2, 2)
    yc = me // 4
    xn = me + 2 - 4 * xc
    yn = me + 4 - 8 * yc
    cn = me + 1 - 2 * core
    dg = xn + 4 - 8 * yc

    barrier = pltpu.get_barrier_semaphore()
    for nb in (xn, yn, cn):
        pl.semaphore_signal(barrier, inc=1, device_id={"fsdp": nb}, device_id_type=MESH)
    pl.semaphore_wait(barrier, 3)

    plan = Planner()

    def al(i, n):
        return i if isinstance(i, int) else pl.multiple_of(i, n)

    def view(ref, l, r0, nr, c0, nc):
        return ref.at[l, pl.ds(al(r0, 16), nr), pl.ds(al(c0, 128), nc)]

    def remote(key, link, pairs, dev, deps):
        sizes = [n for n, _ in pairs]

        def each():
            for i, (_, make) in zip(plan.all[key].sems, pairs):
                src, dst = make()
                yield pltpu.make_async_remote_copy(src_ref=src, dst_ref=dst, send_sem=send.at[i], recv_sem=recv.at[i],
                                                   device_id={"fsdp": dev}, device_id_type=MESH)

        plan.add(Transfer(key, link, sum(sizes), len(pairs), lambda: [c.start() for c in each()], lambda: [c.wait_recv() for c in each()],
                          lambda: [c.wait_send() for c in each()], deps))

    def local(key, pairs, deps):
        sizes = [n for n, _ in pairs]

        def each():
            for i, (_, make) in zip(plan.all[key].sems, pairs):
                src, dst = make()
                yield pltpu.make_async_copy(src, dst, send.at[i])

        plan.add(Transfer(key, "L", sum(sizes), len(pairs), lambda: [c.start() for c in each()], lambda: [c.wait() for c in each()], None, deps))

    def block(src, dst, l, col, other_col, nc, stage):
        def at(dev, other=False):
            return view(dst, l, dev * ROWS, ROWS, other_col if other else col, nc)

        def part(dev, p):
            return view(dst, l, dev * ROWS + (ROWS // 2) * p, ROWS // 2, col, nc)
        return (2 * ROWS * nc, lambda other=False: view(src, l, 0, ROWS, other_col if other else col, nc), at, stage)

    def down_block(l, j, stage):
        return (2 * DR * D, lambda other=False: view(w_d, l, j * DR, DR, 0, D), lambda dev, other=False: view(f_d, l, dev * FROWS + j * DR, DR, 0, D), stage)

    def shared_block(row_of):
        at = lambda dev, other=False: view(f_d, 1, row_of(dev), DR, 0, D)
        return (2 * DR * D, lambda other=False: at(me), at, None)

    def place(dev):
        return dev // 4, lax.rem(dev // 2, 2), lax.rem(dev, 2)

    def tp_row(j):
        def row(dev):
            yy, xx, cc = place(dev)
            return yy * HALF + xx * (2 * FROWS) + TF * (1 - xx) + (N_DT * DR) * cc + j * DR
        return row

    def dp_row(j):
        def row(dev):
            yy, xx, cc = place(dev)
            return yy * HALF + xx * (2 * FROWS) + (2 * FROWS - TF) * xx + (N_DD * DR) * cc + j * DR
        return row

    def add_round(rd, mats, parts, deps=(), before=None):
        K = lambda t: (rd, t)

        def own(other=False):
            return [(m[0], lambda m=m: (m[1](other), m[2](me, other))) for m in mats]

        def held(dev):
            return [(m[0], lambda m=m: (m[2](dev), m[2](dev))) for m in mats]

        for t in parts:
            if t == "X":
                remote(K(t), "X", own(), xn, deps)
            elif t == "Y":
                remote(K(t), "Y", own(other=True), yn, deps)
            elif t == "D":
                remote(K(t), "D", own(), cn, [])
            elif t == "XR":
                remote(K(t), "X", held(yn), xn, [K("Y")])
            elif t == "DX":
                remote(K(t), "D", held(xn), cn, [K("X")])
            elif t == "DY":
                remote(K(t), "D", held(yn), cn, [K("Y")])
            elif t == "DR":
                remote(K(t), "D", held(dg), cn, [K("XR")])
            elif t == "bin":
                local(K(t), [(m[0], lambda m=m: (m[1](), m[3])) for m in mats], [before] if before else [])
            else:
                local(K(t), [(m[0], lambda m=m: (m[3], m[2](me))) for m in mats], [K("bin")])
        if "D" in parts and "X" in parts:
            plan.mates[K("X")] = [K("D"), K("bin")]
        needs[rd] = [K(t) for t in parts]

    needs = {}
    FULL = ("X", "Y", "D", "XR", "DX", "DY", "DR", "bin", "bout")
    for l in (0, 1):
        add_round(("qkv", l), [block(w_q, f_q, l, 0, 0, D, b_q), block(w_k, f_k, l, 0, 0, KV, b_k), block(w_v, f_v, l, 0, 0, KV, b_v)], FULL,
                  before=(("qkv", 0), "bout") if l else None)
        add_round(("o", l), [block(w_o, f_o, l, 0, 0, D, b_o)], FULL, before=(("o", 0), "bout") if l else None)
    dn_seq = [("dn", l, j) for l in (0, 1) for j in range(N_DN)]
    for n, rd in enumerate(dn_seq):
        add_round(rd, [down_block(rd[1], rd[2], b_d.at[n % 4])], ("X", "D", "DX", "bin", "bout") if rd[1] == 0 else ("D", "bin", "bout"),
                  before=(dn_seq[n - 4], "bout") if n >= 4 else None)
    dn1 = [key for j in range(N_DN) for key in needs[("dn", 1, j)]]
    for j in range(N_DT):
        add_round(("dt", j), [shared_block(tp_row(j))], ("X", "DX"), deps=dn1)
    for j in range(N_DD):
        add_round(("dd", j), [shared_block(dp_row(j))], ("X", "Y", "XR", "DX", "DY", "DR"), deps=dn1)
    gu_seq = [("gu", j) for j in range(N_G0)] + [("gt", j) for j in TP_TILES] + [("gd", j) for j in range(N_DP)]
    for n, rd in enumerate(gu_seq):
        kind, j = rd
        l = 0 if kind == "gu" else 1
        if kind == "gd":
            col = (j % 2) * HALF + (j // 2) * (HALF - TF)
            other = col
        else:
            col, other = yc * HALF + j * TF, (1 - yc) * HALF + j * TF
        add_round(rd, [block(w_g, f_g, l, col, other, TF, b_g.at[n % 4]), block(w_u, f_u, l, col, other, TF, b_u.at[n % 4])], FULL,
                  before=(gu_seq[n - 4], "bout") if n >= 4 else None)
    for j in range(N_DN):
        plan.mates[(("gu", j), "X")] += [(("dn", 1, j), "D"), (("dn", 1, j), "bin")]
    for i in range(NB):
        mine, theirs = pl.ds(i * MB, MB), pl.ds(TOK + i * MB, MB)
        for l, land in ((0, f_p), (1, f_r)):
            remote(("h", l, i), "Y", [(2 * MB * D, lambda mine=mine, theirs=theirs: (h.at[mine, :], h.at[theirs, :]))], yn, [("h ready", l, i)])
            remote(("p", l, i), "Y", [(4 * MB * D, lambda mine=mine, theirs=theirs, land=land: (x.at[theirs, :], land.at[mine, :]))], yn, [("p ready", l, i)])

    def seq(rds, *ts):
        return [(rd, t) for rd in rds for t in ts]

    attn = lambda l: [("qkv", l), ("o", l)]
    gus, gts, gds = [("gu", j) for j in range(N_G0)], [("gt", j) for j in TP_TILES], [("gd", j) for j in range(N_DP)]
    dts, dds = [("dt", j) for j in range(N_DT)], [("dd", j) for j in range(N_DD)]
    plan.queue["X"] = (seq(attn(0), "X") + seq(attn(0), "XR") + seq(dn_seq[:N_DN], "X") + seq(gus, "X", "XR")
                       + seq(attn(1), "X") + seq(attn(1), "XR") + seq(dts, "X") + seq(gts, "X", "XR") + seq(dds, "X", "XR") + seq(gds, "X", "XR"))
    plan.queue["Y"] = TOKEN_ORDER + seq(attn(0), "Y") + seq(gus, "Y") + seq(attn(1), "Y") + seq(gts, "Y") + seq(dds, "Y") + seq(gds, "Y")

    def rows_of(i):
        return pl.ds(i * MB if isinstance(i, int) else pl.multiple_of(i * MB, MB), MB)

    def load(pairs):
        cps = [pltpu.make_async_copy(s, d, ld.at[i]) for i, (s, d) in enumerate(pairs)]
        for c in cps:
            c.start()
        for c in cps:
            c.wait()

    plan.service()
    run(plan.take())
    tok_in = pltpu.make_async_copy(tok, o, ld.at[0])
    tok_in.start()

    def tables(i, c):
        rows = rows_of(i)
        rr = lax.broadcasted_iota(jnp.int32, (MB, TOK), 0) + i * MB
        cc = lax.broadcasted_iota(jnp.int32, (MB, TOK), 1)
        seg = jnp.broadcast_to(seg_r[...], (MB, TOK)).astype(jnp.float32)
        seg_c = jnp.sum(jnp.where(cc == rr, seg, 0.0), axis=1, keepdims=True)
        ok = jnp.where((seg == seg_c) & (cc <= rr), 1.0, 0.0)
        mask[rows, :] = ok
        pos = jnp.sum(ok, axis=1, keepdims=True) - 1.0
        ang = pos * freq[...]
        lane = lax.broadcasted_iota(jnp.int32, (MB, HEAD), 1)
        cos_t[rows, :] = jnp.cos(ang)
        sn = jnp.sin(ang)
        sin_t[rows, :] = jnp.where(lane < HEAD // 2, -sn, sn)
        return c

    lax.fori_loop(0, NB, tables, 0)
    plan.spend(T_TABLES)
    plan.service()
    run(plan.take())
    tok_in.wait()

    def widen(i, c):
        rows = rows_of(i)
        x[rows, :] = o[rows, :].astype(jnp.float32)
        x[rows_of(i + NB), :] = jnp.zeros((MB, D), jnp.float32)
        return c

    lax.fori_loop(0, NB, widen, 0)
    plan.spend(T_WIDEN)

    def norm_row(gain_ref, l, i):
        rows = rows_of(i)
        xv = x[rows, :]
        inv = lax.rsqrt(jnp.mean(xv * xv, axis=-1, keepdims=True) + EPS)
        h[rows, :] = (xv * inv * gain_ref[l:l + 1, :].astype(jnp.float32)).astype(jnp.bfloat16)

    def rope(val, rows):
        f = val.astype(jnp.bfloat16).astype(jnp.float32)
        return (f * cos_t[rows, :] + pltpu.roll(f, HEAD // 2, 1) * sin_t[rows, :]).astype(jnp.bfloat16)

    def qkv_row(i):
        rows = rows_of(i)
        hv = h[rows, :]
        for g in range(HEADS // 4):
            val = jnp.dot(hv, vq[:, g * 512:(g + 1) * 512], preferred_element_type=jnp.float32)
            for e in range(4):
                q[rows, g * 512 + e * HEAD:g * 512 + (e + 1) * HEAD] = rope(val[:, e * HEAD:(e + 1) * HEAD], rows)
        val = jnp.dot(hv, vk[...], preferred_element_type=jnp.float32)
        for e in range(KV_HEADS):
            k[rows, e * HEAD:(e + 1) * HEAD] = rope(val[:, e * HEAD:(e + 1) * HEAD], rows)
        v[rows, :] = jnp.dot(hv, vv[...], preferred_element_type=jnp.float32).astype(jnp.bfloat16)

    def one_head(hd, blocks):
        qc = pl.ds(pl.multiple_of(hd * HEAD, HEAD), HEAD)
        kc = pl.ds(pl.multiple_of((hd // (HEADS // KV_HEADS)) * HEAD, HEAD), HEAD)
        for i in blocks:
            n = (i + 1) * MB
            s = lax.dot_general(q[i * MB:n, qc], k[0:n, kc], (((1,), (1,)), ((), ())), preferred_element_type=jnp.float32) * SCALE
            s = jnp.where(mask[i * MB:n, 0:n] > 0.5, s, -1e30)
            e = jnp.exp(s - jnp.max(s, axis=1, keepdims=True))
            p = (e / jnp.sum(e, axis=1, keepdims=True)).astype(jnp.bfloat16)
            o[i * MB:n, qc] = jnp.dot(p, v[0:n, kc], preferred_element_type=jnp.float32).astype(jnp.bfloat16)

    def act(hv):
        gt = jnp.dot(hv, vg[...], preferred_element_type=jnp.float32)
        up = jnp.dot(hv, vu[...], preferred_element_type=jnp.float32)
        return (gt * jax.nn.sigmoid(gt) * up).astype(jnp.bfloat16)

    def mlp_row(i, c):
        rows = rows_of(i)
        x[rows, :] += jnp.dot(act(h[rows, :]), vd[...], preferred_element_type=jnp.float32)
        return c

    def get_qkv(l):
        plan.need(needs[("qkv", l)])
        run(plan.take())
        load([(f_q.at[l], vq), (f_k.at[l], vk), (f_v.at[l], vv)])
        plan.spend(3.0)

    def get_o(l):
        plan.need(needs[("o", l)])
        run(plan.take())
        load([(f_o.at[l], vo)])
        plan.spend(2.0)

    def heads(blocks):
        table = []
        for i in range(HEADS):
            if i % 2 == 0 or len(blocks) == NB:
                plan.service()
            table.append(plan.take())
            plan.spend(T_HEAD * sum(b + 1 for b in blocks) / 10)

        def head_step(hd, c):
            run_at(hd, table)
            one_head(hd, blocks)
            return c

        lax.fori_loop(0, HEADS, head_step, 0)

    def proj_row(l, i):
        rows = rows_of(i)
        x[rows, :] += jnp.dot(o[rows, :], vo[...], preferred_element_type=jnp.float32)
        norm_row(g_mlp, l, i)

    def tiles(l, steps, offset, first, n_rows, marks=None):
        pre, post = {}, {}
        for n, (t, keys) in enumerate(steps):
            for key in (marks or {}).get((n, "pre"), ()):
                plan.mark(key)
            plan.need(keys)
            pre[t] = plan.take()
            plan.spend(2.2)
            for key in (marks or {}).get((n, "post"), ()):
                plan.mark(key)
            plan.service()
            post[t] = plan.take()
            plan.spend(T_TILE * n_rows / NB)

        def body(t, c):
            run_at(t, pre)
            cols = pl.ds(pl.multiple_of(offset(t), 128), TF)
            load([(f_g.at[l, :, cols], vg), (f_u.at[l, :, cols], vu), (f_d.at[l, cols, :], vd)])
            run_at(t, post)
            lax.fori_loop(first, first + n_rows, mlp_row, 0)
            return c

        lax.fori_loop(steps[0][0], steps[-1][0] + 1, body, 0)

    get_qkv(0)
    table_q = []
    for i in range(NB):
        plan.service()
        table_q.append(plan.take())
        plan.spend(T_QKV + T_NORM)

    def qkv_step(i, c):
        run_at(i, table_q)
        norm_row(g_attn, 0, i)
        qkv_row(i)
        return c

    lax.fori_loop(0, NB, qkv_step, 0)
    heads(range(NB))
    get_o(0)
    table_o = []
    for i in range(NB):
        plan.service()
        if i >= 2:
            plan.mark(("h ready", 0, i - 2))
            plan.fill()
        table_o.append(plan.take())
        plan.spend(T_PROJ + T_NORM)

    def proj_step(i, c):
        run_at(i, table_o)
        proj_row(0, i)
        return c

    lax.fori_loop(0, NB, proj_step, 0)

    dn0 = [key for j in range(N_DN) for key in needs[("dn", 0, j)]]
    half_off = lambda t: yc * HALF + t * TF
    steps = [(j, needs[("gu", j)] + dn0) for j in range(N_G0)]
    got_h = lambda l, *chunks: [("h", l, i) for i in chunks]
    tiles(0, steps[:OWN_FIRST], half_off, 0, NB, {(0, "pre"): [("h ready", 0, NB - 2)], (0, "post"): [("h ready", 0, NB - 1)]})
    tiles(0, [(j, keys + got_h(0, *range(NB))) for j, keys in steps], half_off, NB, NB)
    tiles(0, steps[OWN_FIRST:], half_off, 0, NB, {(0, "post"): [("p ready", 0, i) for i in range(NB)]})

    get_qkv(1)
    for i in range(NB):
        plan.need([("p", 0, i)])
        plan.retire(keys=[("p", 0, i)])
        if i:
            plan.mark(("h ready", 1, i - 1))
            plan.service()
        run(plan.take())
        load([(f_p.at[rows_of(i), :], x.at[rows_of(i + NB), :])])
        x[rows_of(i), :] += x[rows_of(i + NB), :]
        x[rows_of(i + NB), :] = jnp.zeros((MB, D), jnp.float32)
        norm_row(g_attn, 1, i)
        qkv_row(i)
        plan.spend(T_QKV + T_NORM + T_ADD)
        heads([i])
        if i == 0:
            get_o(1)
        proj_row(1, i)
        plan.spend(T_PROJ + T_NORM)

    dt1 = dn1 + [key for j in range(N_DT) for key in needs[("dt", j)]]
    dd1 = dn1 + [key for j in range(N_DD) for key in needs[("dd", j)]]
    steps = [(j, needs[("gt", j)] + dt1) for j in TP_TILES]
    h_mark = {(0, "pre"): [("h ready", 1, NB - 1)]}
    run_order = L1_ORDER
    marks = {}
    for n, what in enumerate(run_order):
        if what == "own":
            tiles(1, steps, half_off, 0, NB, {**h_mark, **marks})
            marks, h_mark = {}, {}
        elif what in ("lo", "hi"):
            chunks = (0, 1) if what == "lo" else (2, 3)
            tiles(1, [(j, keys + got_h(1, *chunks)) for j, keys in steps], half_off, NB + chunks[0], 2, {**h_mark, **marks})
            marks, h_mark = {(0, "pre"): [("p ready", 1, chunks[0])], (0, "post"): [("p ready", 1, chunks[1])]}, {}
        else:
            tiles(1, [(j, needs[("gd", j)] + dd1) for j in range(N_DP)],
                  lambda t: lax.rem(t, 2) * HALF + lax.div(t, 2) * (HALF - TF), 0, NB, {**h_mark, **marks})
            marks, h_mark = {}, {}

    for i in range(NB - 1):
        plan.need([("p", 1, i)])
        plan.retire(keys=[("p", 1, i)])
        run(plan.take())
        load([(f_r.at[rows_of(i), :], x.at[rows_of(i + NB), :])])
        x[rows_of(i), :] += x[rows_of(i + NB), :]
        plan.spend(T_ADD)
    plan.service()
    done = pltpu.make_async_copy(x.at[pl.ds(0, TOK), :], out, ld.at[0])
    done.start()
    plan.need(plan.all)
    plan.retire(everything=True)
    run(plan.take())
    done.wait()


def finish(x_ref, r_ref, out_ref):
    last = pl.program_id(0) >= (NB - 1) * MB // FB

    @pl.when(last)
    def _():
        out_ref[...] = x_ref[...] + r_ref[...]

    @pl.when(jnp.logical_not(last))
    def _():
        out_ref[...] = x_ref[...]


def solution(mesh):
    tok_spec = P(("rep", "fsdp"), None)
    seg_spec = P(("rep", "fsdp"))
    mat_spec = P(None, "fsdp", None)
    gain_spec = P(None, None)
    bf, f32 = jnp.bfloat16, jnp.float32

    def per_device(tokens, seg_ids, w_q, w_k, w_v, w_o, w_gate, w_up, w_down, g_attn, g_mlp):
        half = HEAD // 2
        inv = np.float32(ROPE_BASE) ** (-np.arange(half, dtype=np.float32) / np.float32(half))
        freq = jnp.asarray(np.concatenate([inv, inv]).reshape(1, HEAD), f32)
        any_s = pl.BlockSpec(memory_space=pl.ANY)
        vm = pl.BlockSpec(memory_space=pltpu.VMEM)
        full = [(LAYERS, D, D), (LAYERS, D, KV), (LAYERS, D, KV), (LAYERS, D, D), (LAYERS, D, FF), (LAYERS, D, FF), (LAYERS, FF, D)]
        res = pl.pallas_call(
            kernel,
            out_shape=[jax.ShapeDtypeStruct((TOK, D), f32)] * 2 + [jax.ShapeDtypeStruct(s, bf) for s in full] + [jax.ShapeDtypeStruct((TOK, D), f32)],
            in_specs=[any_s, vm, vm, vm, vm] + [any_s] * 7,
            out_specs=[any_s] * 10,
            scratch_shapes=[
                pltpu.VMEM((2 * TOK, D), f32), pltpu.VMEM((2 * TOK, D), bf), pltpu.VMEM((TOK, D), bf),
                pltpu.VMEM((TOK, KV), bf), pltpu.VMEM((TOK, KV), bf), pltpu.VMEM((TOK, D), bf),
                pltpu.VMEM((TOK, HEAD), f32), pltpu.VMEM((TOK, HEAD), f32), pltpu.VMEM((TOK, TOK), f32),
                pltpu.VMEM((D, D), bf), pltpu.VMEM((D, KV), bf), pltpu.VMEM((D, KV), bf), pltpu.VMEM((D, D), bf),
                pltpu.VMEM((D, TF), bf), pltpu.VMEM((D, TF), bf), pltpu.VMEM((TF, D), bf),
                pltpu.VMEM((ROWS, D), bf), pltpu.VMEM((ROWS, KV), bf), pltpu.VMEM((ROWS, KV), bf), pltpu.VMEM((ROWS, D), bf),
                pltpu.VMEM((4, ROWS, TF), bf), pltpu.VMEM((4, ROWS, TF), bf), pltpu.VMEM((4, DR, D), bf),
                pltpu.SemaphoreType.DMA((N_SEM,)), pltpu.SemaphoreType.DMA((N_SEM,)), pltpu.SemaphoreType.DMA((4,)),
            ],
            compiler_params=pltpu.CompilerParams(collective_id=0, has_side_effects=True, vmem_limit_bytes=66 * 1000 * 1000),
        )(tokens, seg_ids.reshape(1, TOK), freq, g_attn, g_mlp, w_q, w_k, w_v, w_o, w_gate, w_up, w_down)
        return pl.pallas_call(
            finish,
            grid=(TOK // FB,),
            out_shape=jax.ShapeDtypeStruct((TOK, D), f32),
            in_specs=[pl.BlockSpec((FB, D), lambda i: (i, 0)), pl.BlockSpec((FB, D), lambda i: (jnp.maximum(i, (NB - 1) * MB // FB), 0))],
            out_specs=pl.BlockSpec((FB, D), lambda i: (i, 0)),
        )(res[0], res[1])

    return jax.shard_map(per_device, mesh=mesh, in_specs=(tok_spec, seg_spec, mat_spec, mat_spec, mat_spec, mat_spec, mat_spec, mat_spec, mat_spec, gain_spec, gain_spec), out_specs=tok_spec, check_vma=False)
```

```python
import jax
import jax.numpy as jnp
import numpy as np
from jax import lax
from jax.experimental import pallas as pl
from jax.experimental.pallas import tpu as pltpu
from jax.sharding import PartitionSpec as P

HEAD = 128
HEADS = 12
KV_HEADS = 2
EPS = 1e-5
ROPE_BASE = 10000.0
MESH = pl.DeviceIdType.MESH

N_DEV = 8
TOK = 1024
D = 1536
KV = KV_HEADS * HEAD
FF = 8960
HALF = FF // 2
ROWS = D // N_DEV
FROWS = FF // N_DEV
TF = 640
N_G0 = HALF // TF
TP_TILES = (1, 2, 3, 4, 5)
N_DP = 4
DR = 160
N_DT = 5
N_DD = 2
N_DN = FROWS // DR
LAYERS = 2
MB = 256
NB = TOK // MB
SCALE = HEAD ** -0.5

RATE = {"X": 46600.0, "Y": 46600.0, "D": 500000.0, "L": 800000.0}
LAT = {"X": 2.5, "Y": 2.5, "D": 1.5, "L": 1.0}
HORIZON = 20.0
T_TABLES, T_WIDEN, T_NORM, T_QKV, T_HEAD, T_PROJ, T_TILE, T_ADD = 3.0, 1.6, 0.4, 1.8, 2.0, 1.1, 6.6, 1.5
OWN_FIRST = 3
L1_ORDER = ("lo", "hi", "own", "dp")
TOKEN_ORDER = [(c, l, i) for c, l in (("h", 0), ("p", 0), ("h", 1), ("p", 1)) for i in range(NB)]
N_SEM = 230
FB = 128


class Transfer:
    def __init__(self, key, link, size, n_sem, start, wait, done, deps):
        self.key, self.link, self.size, self.n_sem = key, link, size, n_sem
        self.start, self.wait, self.done, self.deps = start, wait, done, set(deps)
        self.sems = []


class Planner:
    def __init__(self):
        self.now = 0.0
        self.free = dict.fromkeys("XYDL", 0.0)
        self.all, self.queue, self.users, self.mates = {}, {"X": [], "Y": []}, {}, {}
        self.pool = list(range(N_SEM))
        self.issued, self.arrived, self.flying, self.sent, self.ops = set(), set(), [], [], []

    def add(self, tr):
        self.all[tr.key] = tr
        for dep in tr.deps:
            self.users.setdefault(dep, []).append(tr.key)

    def issue(self, key):
        tr = self.all[key]
        self.issued.add(key)
        tr.sems, self.pool = self.pool[:tr.n_sem], self.pool[tr.n_sem:]
        self.ops.append(tr.start)
        self.free[tr.link] = max(self.free[tr.link], self.now) + tr.size / RATE[tr.link]
        self.flying.append((self.free[tr.link] + LAT[tr.link], key))
        for mate in self.mates.get(key, ()):
            if mate not in self.issued and self.all[mate].deps <= self.arrived:
                self.issue(mate)

    def mark(self, key):
        self.arrived.add(key)
        for user in self.users.get(key, ()):
            tr = self.all[user]
            if tr.link in "DL" and user not in self.issued and tr.deps <= self.arrived:
                self.issue(user)

    def receive(self, item):
        self.flying.remove(item)
        tr = self.all[item[1]]
        self.ops.append(tr.wait)
        if tr.done is not None:
            self.sent.append((item[0] + 2.0, item[1]))
        else:
            self.pool += tr.sems
        self.mark(item[1])

    def fill(self):
        for link in "XY":
            while self.free[link] - self.now < HORIZON:
                ready = [k for k in self.queue[link] if self.all[k].deps <= self.arrived]
                if not ready:
                    break
                self.queue[link].remove(ready[0])
                self.issue(ready[0])

    def retire(self, keys=None, everything=False):
        for item in list(self.sent):
            if everything or (keys is not None and item[1] in keys) or (keys is None and item[0] <= self.now):
                self.sent.remove(item)
                self.ops.append(self.all[item[1]].done)
                self.pool += self.all[item[1]].sems

    def service(self):
        while True:
            due = sorted(i for i in self.flying if i[0] <= self.now)
            if not due:
                break
            self.receive(due[0])
            self.fill()
        self.fill()
        self.retire()

    def need(self, keys):
        keys = set(keys)
        while not keys <= self.arrived:
            self.fill()
            item = min(self.flying)
            self.now = max(self.now, item[0])
            self.receive(item)
        self.service()

    def spend(self, us):
        self.now += us

    def take(self):
        ops, self.ops = self.ops, []
        return ops


def run(ops):
    for op in ops:
        op()


def run_at(index, table):
    for k, ops in (table.items() if isinstance(table, dict) else enumerate(table)):
        if ops:
            pl.when(index == k)(lambda ops=ops: run(ops))


def kernel(tok, seg_r, freq, g_attn, g_mlp, w_q, w_k, w_v, w_o, w_g, w_u, w_d,
           out, f_r, f_q, f_k, f_v, f_o, f_g, f_u, f_d, f_p,
           x, h, q, k, v, o, cos_t, sin_t, mask, vq, vk, vv, vo, vg, vu, vd,
           b_q, b_k, b_v, b_o, b_g, b_u, b_d,
           send, recv, ld):
    me = lax.axis_index("fsdp")
    core = lax.rem(me, 2)
    xc = lax.rem(me // 2, 2)
    yc = me // 4
    xn = me + 2 - 4 * xc
    yn = me + 4 - 8 * yc
    cn = me + 1 - 2 * core
    dg = xn + 4 - 8 * yc

    barrier = pltpu.get_barrier_semaphore()
    for nb in (xn, yn, cn):
        pl.semaphore_signal(barrier, inc=1, device_id={"fsdp": nb}, device_id_type=MESH)
    pl.semaphore_wait(barrier, 3)

    plan = Planner()

    def al(i, n):
        return i if isinstance(i, int) else pl.multiple_of(i, n)

    def view(ref, l, r0, nr, c0, nc):
        return ref.at[l, pl.ds(al(r0, 16), nr), pl.ds(al(c0, 128), nc)]

    def remote(key, link, pairs, dev, deps):
        sizes = [n for n, _ in pairs]

        def each():
            for i, (_, make) in zip(plan.all[key].sems, pairs):
                src, dst = make()
                yield pltpu.make_async_remote_copy(src_ref=src, dst_ref=dst, send_sem=send.at[i], recv_sem=recv.at[i],
                                                   device_id={"fsdp": dev}, device_id_type=MESH)

        plan.add(Transfer(key, link, sum(sizes), len(pairs), lambda: [c.start() for c in each()], lambda: [c.wait_recv() for c in each()],
                          lambda: [c.wait_send() for c in each()], deps))

    def local(key, pairs, deps):
        sizes = [n for n, _ in pairs]

        def each():
            for i, (_, make) in zip(plan.all[key].sems, pairs):
                src, dst = make()
                yield pltpu.make_async_copy(src, dst, send.at[i])

        plan.add(Transfer(key, "L", sum(sizes), len(pairs), lambda: [c.start() for c in each()], lambda: [c.wait() for c in each()], None, deps))

    def block(src, dst, l, col, other_col, nc, stage):
        def at(dev, other=False):
            return view(dst, l, dev * ROWS, ROWS, other_col if other else col, nc)

        def part(dev, p):
            return view(dst, l, dev * ROWS + (ROWS // 2) * p, ROWS // 2, col, nc)
        return (2 * ROWS * nc, lambda other=False: view(src, l, 0, ROWS, other_col if other else col, nc), at, stage)

    def down_block(l, j, stage):
        return (2 * DR * D, lambda other=False: view(w_d, l, j * DR, DR, 0, D), lambda dev, other=False: view(f_d, l, dev * FROWS + j * DR, DR, 0, D), stage)

    def shared_block(row_of):
        at = lambda dev, other=False: view(f_d, 1, row_of(dev), DR, 0, D)
        return (2 * DR * D, lambda other=False: at(me), at, None)

    def place(dev):
        return dev // 4, lax.rem(dev // 2, 2), lax.rem(dev, 2)

    def tp_row(j):
        def row(dev):
            yy, xx, cc = place(dev)
            return yy * HALF + xx * (2 * FROWS) + TF * (1 - xx) + (N_DT * DR) * cc + j * DR
        return row

    def dp_row(j):
        def row(dev):
            yy, xx, cc = place(dev)
            return yy * HALF + xx * (2 * FROWS) + (2 * FROWS - TF) * xx + (N_DD * DR) * cc + j * DR
        return row

    def add_round(rd, mats, parts, deps=(), before=None):
        K = lambda t: (rd, t)

        def own(other=False):
            return [(m[0], lambda m=m: (m[1](other), m[2](me, other))) for m in mats]

        def held(dev):
            return [(m[0], lambda m=m: (m[2](dev), m[2](dev))) for m in mats]

        for t in parts:
            if t == "X":
                remote(K(t), "X", own(), xn, deps)
            elif t == "Y":
                remote(K(t), "Y", own(other=True), yn, deps)
            elif t == "D":
                remote(K(t), "D", own(), cn, [])
            elif t == "XR":
                remote(K(t), "X", held(yn), xn, [K("Y")])
            elif t == "DX":
                remote(K(t), "D", held(xn), cn, [K("X")])
            elif t == "DY":
                remote(K(t), "D", held(yn), cn, [K("Y")])
            elif t == "DR":
                remote(K(t), "D", held(dg), cn, [K("XR")])
            elif t == "bin":
                local(K(t), [(m[0], lambda m=m: (m[1](), m[3])) for m in mats], [before] if before else [])
            else:
                local(K(t), [(m[0], lambda m=m: (m[3], m[2](me))) for m in mats], [K("bin")])
        if "D" in parts and "X" in parts:
            plan.mates[K("X")] = [K("D"), K("bin")]
        needs[rd] = [K(t) for t in parts]

    needs = {}
    FULL = ("X", "Y", "D", "XR", "DX", "DY", "DR", "bin", "bout")
    for l in (0, 1):
        add_round(("qkv", l), [block(w_q, f_q, l, 0, 0, D, b_q), block(w_k, f_k, l, 0, 0, KV, b_k), block(w_v, f_v, l, 0, 0, KV, b_v)], FULL,
                  before=(("qkv", 0), "bout") if l else None)
        add_round(("o", l), [block(w_o, f_o, l, 0, 0, D, b_o)], FULL, before=(("o", 0), "bout") if l else None)
    dn_seq = [("dn", l, j) for l in (0, 1) for j in range(N_DN)]
    for n, rd in enumerate(dn_seq):
        add_round(rd, [down_block(rd[1], rd[2], b_d.at[n % 4])], ("X", "D", "DX", "bin", "bout") if rd[1] == 0 else ("D", "bin", "bout"),
                  before=(dn_seq[n - 4], "bout") if n >= 4 else None)
    dn1 = [key for j in range(N_DN) for key in needs[("dn", 1, j)]]
    for j in range(N_DT):
        add_round(("dt", j), [shared_block(tp_row(j))], ("X", "DX"), deps=dn1)
    for j in range(N_DD):
        add_round(("dd", j), [shared_block(dp_row(j))], ("X", "Y", "XR", "DX", "DY", "DR"), deps=dn1)
    gu_seq = [("gu", j) for j in range(N_G0)] + [("gt", j) for j in TP_TILES] + [("gd", j) for j in range(N_DP)]
    for n, rd in enumerate(gu_seq):
        kind, j = rd
        l = 0 if kind == "gu" else 1
        if kind == "gd":
            col = (j % 2) * HALF + (j // 2) * (HALF - TF)
            other = col
        else:
            col, other = yc * HALF + j * TF, (1 - yc) * HALF + j * TF
        add_round(rd, [block(w_g, f_g, l, col, other, TF, b_g.at[n % 4]), block(w_u, f_u, l, col, other, TF, b_u.at[n % 4])], FULL,
                  before=(gu_seq[n - 4], "bout") if n >= 4 else None)
    for j in range(N_DN):
        plan.mates[(("gu", j), "X")] += [(("dn", 1, j), "D"), (("dn", 1, j), "bin")]
    for i in range(NB):
        mine, theirs = pl.ds(i * MB, MB), pl.ds(TOK + i * MB, MB)
        for l, land in ((0, f_p), (1, f_r)):
            remote(("h", l, i), "Y", [(2 * MB * D, lambda mine=mine, theirs=theirs: (h.at[mine, :], h.at[theirs, :]))], yn, [("h ready", l, i)])
            remote(("p", l, i), "Y", [(4 * MB * D, lambda mine=mine, theirs=theirs, land=land: (x.at[theirs, :], land.at[mine, :]))], yn, [("p ready", l, i)])

    def seq(rds, *ts):
        return [(rd, t) for rd in rds for t in ts]

    attn = lambda l: [("qkv", l), ("o", l)]
    gus, gts, gds = [("gu", j) for j in range(N_G0)], [("gt", j) for j in TP_TILES], [("gd", j) for j in range(N_DP)]
    dts, dds = [("dt", j) for j in range(N_DT)], [("dd", j) for j in range(N_DD)]
    plan.queue["X"] = (seq(attn(0), "X") + seq(attn(0), "XR") + seq(dn_seq[:N_DN], "X") + seq(gus, "X", "XR")
                       + seq(attn(1), "X") + seq(attn(1), "XR") + seq(dts, "X") + seq(gts, "X", "XR") + seq(dds, "X", "XR") + seq(gds, "X", "XR"))
    plan.queue["Y"] = TOKEN_ORDER + seq(attn(0), "Y") + seq(gus, "Y") + seq(attn(1), "Y") + seq(gts, "Y") + seq(dds, "Y") + seq(gds, "Y")

    def rows_of(i):
        return pl.ds(i * MB if isinstance(i, int) else pl.multiple_of(i * MB, MB), MB)

    def load(pairs):
        cps = [pltpu.make_async_copy(s, d, ld.at[i]) for i, (s, d) in enumerate(pairs)]
        for c in cps:
            c.start()
        for c in cps:
            c.wait()

    plan.service()
    run(plan.take())
    tok_in = pltpu.make_async_copy(tok, o, ld.at[0])
    tok_in.start()

    def tables(i, c):
        rows = rows_of(i)
        rr = lax.broadcasted_iota(jnp.int32, (MB, TOK), 0) + i * MB
        cc = lax.broadcasted_iota(jnp.int32, (MB, TOK), 1)
        seg = jnp.broadcast_to(seg_r[...], (MB, TOK)).astype(jnp.float32)
        seg_c = jnp.sum(jnp.where(cc == rr, seg, 0.0), axis=1, keepdims=True)
        ok = jnp.where((seg == seg_c) & (cc <= rr), 1.0, 0.0)
        mask[rows, :] = ok
        pos = jnp.sum(ok, axis=1, keepdims=True) - 1.0
        ang = pos * freq[...]
        lane = lax.broadcasted_iota(jnp.int32, (MB, HEAD), 1)
        cos_t[rows, :] = jnp.cos(ang)
        sn = jnp.sin(ang)
        sin_t[rows, :] = jnp.where(lane < HEAD // 2, -sn, sn)
        return c

    lax.fori_loop(0, NB, tables, 0)
    plan.spend(T_TABLES)
    plan.service()
    run(plan.take())
    tok_in.wait()

    def widen(i, c):
        rows = rows_of(i)
        x[rows, :] = o[rows, :].astype(jnp.float32)
        x[rows_of(i + NB), :] = jnp.zeros((MB, D), jnp.float32)
        return c

    lax.fori_loop(0, NB, widen, 0)
    plan.spend(T_WIDEN)

    def norm_row(gain_ref, l, i):
        rows = rows_of(i)
        xv = x[rows, :]
        inv = lax.rsqrt(jnp.mean(xv * xv, axis=-1, keepdims=True) + EPS)
        h[rows, :] = (xv * inv * gain_ref[l:l + 1, :].astype(jnp.float32)).astype(jnp.bfloat16)

    def rope(val, rows):
        f = val.astype(jnp.bfloat16).astype(jnp.float32)
        return (f * cos_t[rows, :] + pltpu.roll(f, HEAD // 2, 1) * sin_t[rows, :]).astype(jnp.bfloat16)

    def qkv_row(i):
        rows = rows_of(i)
        hv = h[rows, :]
        for g in range(HEADS // 4):
            val = jnp.dot(hv, vq[:, g * 512:(g + 1) * 512], preferred_element_type=jnp.float32)
            for e in range(4):
                q[rows, g * 512 + e * HEAD:g * 512 + (e + 1) * HEAD] = rope(val[:, e * HEAD:(e + 1) * HEAD], rows)
        val = jnp.dot(hv, vk[...], preferred_element_type=jnp.float32)
        for e in range(KV_HEADS):
            k[rows, e * HEAD:(e + 1) * HEAD] = rope(val[:, e * HEAD:(e + 1) * HEAD], rows)
        v[rows, :] = jnp.dot(hv, vv[...], preferred_element_type=jnp.float32).astype(jnp.bfloat16)

    def one_head(hd, blocks):
        qc = pl.ds(pl.multiple_of(hd * HEAD, HEAD), HEAD)
        kc = pl.ds(pl.multiple_of((hd // (HEADS // KV_HEADS)) * HEAD, HEAD), HEAD)
        for i in blocks:
            n = (i + 1) * MB
            s = lax.dot_general(q[i * MB:n, qc], k[0:n, kc], (((1,), (1,)), ((), ())), preferred_element_type=jnp.float32) * SCALE
            s = jnp.where(mask[i * MB:n, 0:n] > 0.5, s, -1e30)
            e = jnp.exp(s - jnp.max(s, axis=1, keepdims=True))
            p = (e / jnp.sum(e, axis=1, keepdims=True)).astype(jnp.bfloat16)
            o[i * MB:n, qc] = jnp.dot(p, v[0:n, kc], preferred_element_type=jnp.float32).astype(jnp.bfloat16)

    def act(hv):
        gt = jnp.dot(hv, vg[...], preferred_element_type=jnp.float32)
        up = jnp.dot(hv, vu[...], preferred_element_type=jnp.float32)
        return (gt * jax.nn.sigmoid(gt) * up).astype(jnp.bfloat16)

    def mlp_row(i, c):
        rows = rows_of(i)
        x[rows, :] += jnp.dot(act(h[rows, :]), vd[...], preferred_element_type=jnp.float32)
        return c

    def get_qkv(l):
        plan.need(needs[("qkv", l)])
        run(plan.take())
        load([(f_q.at[l], vq), (f_k.at[l], vk), (f_v.at[l], vv)])
        plan.spend(3.0)

    def get_o(l):
        plan.need(needs[("o", l)])
        run(plan.take())
        load([(f_o.at[l], vo)])
        plan.spend(2.0)

    def heads(blocks):
        table = []
        for i in range(HEADS):
            if i % 2 == 0 or len(blocks) == NB:
                plan.service()
            table.append(plan.take())
            plan.spend(T_HEAD * sum(b + 1 for b in blocks) / 10)

        def head_step(hd, c):
            run_at(hd, table)
            one_head(hd, blocks)
            return c

        lax.fori_loop(0, HEADS, head_step, 0)

    def proj_row(l, i):
        rows = rows_of(i)
        x[rows, :] += jnp.dot(o[rows, :], vo[...], preferred_element_type=jnp.float32)
        norm_row(g_mlp, l, i)

    def tiles(l, steps, offset, first, n_rows, marks=None):
        pre, post = {}, {}
        for n, (t, keys) in enumerate(steps):
            for key in (marks or {}).get((n, "pre"), ()):
                plan.mark(key)
            plan.need(keys)
            pre[t] = plan.take()
            plan.spend(2.2)
            for key in (marks or {}).get((n, "post"), ()):
                plan.mark(key)
            plan.service()
            post[t] = plan.take()
            plan.spend(T_TILE * n_rows / NB)

        def body(t, c):
            run_at(t, pre)
            cols = pl.ds(pl.multiple_of(offset(t), 128), TF)
            load([(f_g.at[l, :, cols], vg), (f_u.at[l, :, cols], vu), (f_d.at[l, cols, :], vd)])
            run_at(t, post)
            lax.fori_loop(first, first + n_rows, mlp_row, 0)
            return c

        lax.fori_loop(steps[0][0], steps[-1][0] + 1, body, 0)

    get_qkv(0)
    table_q = []
    for i in range(NB):
        plan.service()
        table_q.append(plan.take())
        plan.spend(T_QKV + T_NORM)

    def qkv_step(i, c):
        run_at(i, table_q)
        norm_row(g_attn, 0, i)
        qkv_row(i)
        return c

    lax.fori_loop(0, NB, qkv_step, 0)
    heads(range(NB))
    get_o(0)
    table_o = []
    for i in range(NB):
        plan.service()
        if i >= 2:
            plan.mark(("h ready", 0, i - 2))
            plan.fill()
        table_o.append(plan.take())
        plan.spend(T_PROJ + T_NORM)

    def proj_step(i, c):
        run_at(i, table_o)
        proj_row(0, i)
        return c

    lax.fori_loop(0, NB, proj_step, 0)

    dn0 = [key for j in range(N_DN) for key in needs[("dn", 0, j)]]
    half_off = lambda t: yc * HALF + t * TF
    steps = [(j, needs[("gu", j)] + dn0) for j in range(N_G0)]
    got_h = lambda l, *chunks: [("h", l, i) for i in chunks]
    tiles(0, steps[:OWN_FIRST], half_off, 0, NB, {(0, "pre"): [("h ready", 0, NB - 2)], (0, "post"): [("h ready", 0, NB - 1)]})
    tiles(0, [(j, keys + got_h(0, *range(NB))) for j, keys in steps], half_off, NB, NB)
    tiles(0, steps[OWN_FIRST:], half_off, 0, NB, {(0, "post"): [("p ready", 0, i) for i in range(NB)]})

    get_qkv(1)
    for i in range(NB):
        plan.need([("p", 0, i)])
        plan.retire(keys=[("p", 0, i)])
        if i:
            plan.mark(("h ready", 1, i - 1))
            plan.service()
        run(plan.take())
        load([(f_p.at[rows_of(i), :], x.at[rows_of(i + NB), :])])
        x[rows_of(i), :] += x[rows_of(i + NB), :]
        x[rows_of(i + NB), :] = jnp.zeros((MB, D), jnp.float32)
        norm_row(g_attn, 1, i)
        qkv_row(i)
        plan.spend(T_QKV + T_NORM + T_ADD)
        heads([i])
        if i == 0:
            get_o(1)
        proj_row(1, i)
        plan.spend(T_PROJ + T_NORM)

    dt1 = dn1 + [key for j in range(N_DT) for key in needs[("dt", j)]]
    dd1 = dn1 + [key for j in range(N_DD) for key in needs[("dd", j)]]
    steps = [(j, needs[("gt", j)] + dt1) for j in TP_TILES]
    h_mark = {(0, "pre"): [("h ready", 1, NB - 1)]}
    run_order = L1_ORDER
    marks = {}
    for n, what in enumerate(run_order):
        if what == "own":
            tiles(1, steps, half_off, 0, NB, {**h_mark, **marks})
            marks, h_mark = {}, {}
        elif what in ("lo", "hi"):
            chunks = (0, 1) if what == "lo" else (2, 3)
            tiles(1, [(j, keys + got_h(1, *chunks)) for j, keys in steps], half_off, NB + chunks[0], 2, {**h_mark, **marks})
            marks, h_mark = {(0, "pre"): [("p ready", 1, chunks[0])], (0, "post"): [("p ready", 1, chunks[1])]}, {}
        else:
            tiles(1, [(j, needs[("gd", j)] + dd1) for j in range(N_DP)],
                  lambda t: lax.rem(t, 2) * HALF + lax.div(t, 2) * (HALF - TF), 0, NB, {**h_mark, **marks})
            marks, h_mark = {}, {}

    for i in range(NB - 1):
        plan.need([("p", 1, i)])
        plan.retire(keys=[("p", 1, i)])
        run(plan.take())
        load([(f_r.at[rows_of(i), :], x.at[rows_of(i + NB), :])])
        x[rows_of(i), :] += x[rows_of(i + NB), :]
        plan.spend(T_ADD)
    plan.service()
    done = pltpu.make_async_copy(x.at[pl.ds(0, TOK), :], out, ld.at[0])
    done.start()
    plan.need(plan.all)
    plan.retire(everything=True)
    run(plan.take())
    done.wait()


def finish(x_in, r_in, out, xv, rv, sem):
    n = TOK // FB
    first = (NB - 1) * MB // FB
    rows = [pl.ds(i * FB, FB) for i in range(n)]
    order = list(range(first, n)) + list(range(first))
    got = {i: pltpu.make_async_copy(x_in.at[rows[i], :], xv.at[rows[i], :], sem.at[0, i]) for i in range(n)}
    ret = {i: pltpu.make_async_copy(r_in.at[rows[i], :], rv.at[pl.ds((i - first) * FB, FB), :], sem.at[1, i]) for i in range(first, n)}
    put = {i: pltpu.make_async_copy(xv.at[rows[i], :], out.at[rows[i], :], sem.at[2, i]) for i in range(n)}
    for i in order:
        if i in ret:
            ret[i].start()
        got[i].start()
    for i in range(first, n):
        ret[i].wait()
        got[i].wait()
        xv[rows[i], :] += rv[pl.ds((i - first) * FB, FB), :]
    for i in range(first):
        got[i].wait()
        put[i].start()
    for i in range(first, n):
        put[i].start()
    for i in range(n):
        put[i].wait()


def solution(mesh):
    tok_spec = P(("rep", "fsdp"), None)
    seg_spec = P(("rep", "fsdp"))
    mat_spec = P(None, "fsdp", None)
    gain_spec = P(None, None)
    bf, f32 = jnp.bfloat16, jnp.float32

    def per_device(tokens, seg_ids, w_q, w_k, w_v, w_o, w_gate, w_up, w_down, g_attn, g_mlp):
        half = HEAD // 2
        inv = np.float32(ROPE_BASE) ** (-np.arange(half, dtype=np.float32) / np.float32(half))
        freq = jnp.asarray(np.concatenate([inv, inv]).reshape(1, HEAD), f32)
        any_s = pl.BlockSpec(memory_space=pl.ANY)
        vm = pl.BlockSpec(memory_space=pltpu.VMEM)
        full = [(LAYERS, D, D), (LAYERS, D, KV), (LAYERS, D, KV), (LAYERS, D, D), (LAYERS, D, FF), (LAYERS, D, FF), (LAYERS, FF, D)]
        res = pl.pallas_call(
            kernel,
            out_shape=[jax.ShapeDtypeStruct((TOK, D), f32)] * 2 + [jax.ShapeDtypeStruct(s, bf) for s in full] + [jax.ShapeDtypeStruct((TOK, D), f32)],
            in_specs=[any_s, vm, vm, vm, vm] + [any_s] * 7,
            out_specs=[any_s] * 10,
            scratch_shapes=[
                pltpu.VMEM((2 * TOK, D), f32), pltpu.VMEM((2 * TOK, D), bf), pltpu.VMEM((TOK, D), bf),
                pltpu.VMEM((TOK, KV), bf), pltpu.VMEM((TOK, KV), bf), pltpu.VMEM((TOK, D), bf),
                pltpu.VMEM((TOK, HEAD), f32), pltpu.VMEM((TOK, HEAD), f32), pltpu.VMEM((TOK, TOK), f32),
                pltpu.VMEM((D, D), bf), pltpu.VMEM((D, KV), bf), pltpu.VMEM((D, KV), bf), pltpu.VMEM((D, D), bf),
                pltpu.VMEM((D, TF), bf), pltpu.VMEM((D, TF), bf), pltpu.VMEM((TF, D), bf),
                pltpu.VMEM((ROWS, D), bf), pltpu.VMEM((ROWS, KV), bf), pltpu.VMEM((ROWS, KV), bf), pltpu.VMEM((ROWS, D), bf),
                pltpu.VMEM((4, ROWS, TF), bf), pltpu.VMEM((4, ROWS, TF), bf), pltpu.VMEM((4, DR, D), bf),
                pltpu.SemaphoreType.DMA((N_SEM,)), pltpu.SemaphoreType.DMA((N_SEM,)), pltpu.SemaphoreType.DMA((4,)),
            ],
            compiler_params=pltpu.CompilerParams(collective_id=0, has_side_effects=True, vmem_limit_bytes=66 * 1000 * 1000),
        )(tokens, seg_ids.reshape(1, TOK), freq, g_attn, g_mlp, w_q, w_k, w_v, w_o, w_gate, w_up, w_down)
        return pl.pallas_call(
            finish,
            out_shape=jax.ShapeDtypeStruct((TOK, D), f32),
            in_specs=[any_s, any_s],
            out_specs=any_s,
            scratch_shapes=[pltpu.VMEM((TOK, D), f32), pltpu.VMEM((MB, D), f32), pltpu.SemaphoreType.DMA((3, TOK // FB))],
            compiler_params=pltpu.CompilerParams(vmem_limit_bytes=66 * 1000 * 1000),
        )(res[0], res[1])

    return jax.shard_map(per_device, mesh=mesh, in_specs=(tok_spec, seg_spec, mat_spec, mat_spec, mat_spec, mat_spec, mat_spec, mat_spec, mat_spec, gain_spec, gain_spec), out_specs=tok_spec, check_vma=False)
```

```python
import jax
import jax.numpy as jnp
import numpy as np
from jax import lax
from jax.experimental import pallas as pl
from jax.experimental.pallas import tpu as pltpu
from jax.sharding import PartitionSpec as P

HEAD = 128
HEADS = 12
KV_HEADS = 2
EPS = 1e-5
ROPE_BASE = 10000.0
MESH = pl.DeviceIdType.MESH

N_DEV = 8
TOK = 1024
D = 1536
KV = KV_HEADS * HEAD
FF = 8960
HALF = FF // 2
ROWS = D // N_DEV
FROWS = FF // N_DEV
TF = 640
N_G0 = HALF // TF
TP_TILES = (1, 2, 3, 4, 5)
N_DP = 4
DR = 160
N_DT = 5
N_DD = 2
N_DN = FROWS // DR
LAYERS = 2
MB = 256
NB = TOK // MB
SCALE = HEAD ** -0.5

RATE = {"X": 46600.0, "Y": 46600.0, "D": 500000.0, "L": 800000.0}
LAT = {"X": 2.5, "Y": 2.5, "D": 1.5, "L": 1.0}
HORIZON = 20.0
T_TABLES, T_WIDEN, T_NORM, T_QKV, T_HEAD, T_PROJ, T_TILE, T_ADD = 3.0, 1.6, 0.4, 1.8, 2.0, 1.1, 6.6, 1.5
OWN_FIRST = 3
P_AFTER = {3: [("h ready", 1, 1)]}
L1_ORDER = ("c0", "c1", "hi", "own", "dp")
GROUPS = {"c0": (0,), "c1": (1,), "lo": (0, 1), "hi": (2, 3), "c123": (1, 2, 3)}
TOKEN_ORDER = [(c, l, i) for c, l in (("h", 0), ("p", 0), ("h", 1), ("p", 1)) for i in range(NB)]
N_SEM = 230
FB = 128


class Transfer:
    def __init__(self, key, link, size, n_sem, start, wait, done, deps):
        self.key, self.link, self.size, self.n_sem = key, link, size, n_sem
        self.start, self.wait, self.done, self.deps = start, wait, done, set(deps)
        self.sems = []


class Planner:
    def __init__(self):
        self.now = 0.0
        self.free = dict.fromkeys("XYDL", 0.0)
        self.all, self.queue, self.users, self.mates = {}, {"X": [], "Y": []}, {}, {}
        self.pool = list(range(N_SEM))
        self.issued, self.arrived, self.flying, self.sent, self.ops = set(), set(), [], [], []

    def add(self, tr):
        self.all[tr.key] = tr
        for dep in tr.deps:
            self.users.setdefault(dep, []).append(tr.key)

    def issue(self, key):
        tr = self.all[key]
        self.issued.add(key)
        tr.sems, self.pool = self.pool[:tr.n_sem], self.pool[tr.n_sem:]
        self.ops.append(tr.start)
        self.free[tr.link] = max(self.free[tr.link], self.now) + tr.size / RATE[tr.link]
        self.flying.append((self.free[tr.link] + LAT[tr.link], key))
        for mate in self.mates.get(key, ()):
            if mate not in self.issued and self.all[mate].deps <= self.arrived:
                self.issue(mate)

    def mark(self, key):
        self.arrived.add(key)
        for user in self.users.get(key, ()):
            tr = self.all[user]
            if tr.link in "DL" and user not in self.issued and tr.deps <= self.arrived:
                self.issue(user)

    def receive(self, item):
        self.flying.remove(item)
        tr = self.all[item[1]]
        self.ops.append(tr.wait)
        if tr.done is not None:
            self.sent.append((item[0] + 2.0, item[1]))
        else:
            self.pool += tr.sems
        self.mark(item[1])

    def fill(self):
        for link in "XY":
            while self.free[link] - self.now < HORIZON:
                ready = [k for k in self.queue[link] if self.all[k].deps <= self.arrived]
                if not ready:
                    break
                self.queue[link].remove(ready[0])
                self.issue(ready[0])

    def retire(self, keys=None, everything=False):
        for item in list(self.sent):
            if everything or (keys is not None and item[1] in keys) or (keys is None and item[0] <= self.now):
                self.sent.remove(item)
                self.ops.append(self.all[item[1]].done)
                self.pool += self.all[item[1]].sems

    def service(self):
        while True:
            due = sorted(i for i in self.flying if i[0] <= self.now)
            if not due:
                break
            self.receive(due[0])
            self.fill()
        self.fill()
        self.retire()

    def need(self, keys):
        keys = set(keys)
        while not keys <= self.arrived:
            self.fill()
            item = min(self.flying)
            self.now = max(self.now, item[0])
            self.receive(item)
        self.service()

    def spend(self, us):
        self.now += us

    def take(self):
        ops, self.ops = self.ops, []
        return ops


def run(ops):
    for op in ops:
        op()


def run_at(index, table):
    for k, ops in (table.items() if isinstance(table, dict) else enumerate(table)):
        if ops:
            pl.when(index == k)(lambda ops=ops: run(ops))


def kernel(tok, seg_r, freq, g_attn, g_mlp, w_q, w_k, w_v, w_o, w_g, w_u, w_d,
           out, f_r, f_q, f_k, f_v, f_o, f_g, f_u, f_d, f_p,
           x, h, q, k, v, o, cos_t, sin_t, mask, vq, vk, vv, vo, vg, vu, vd,
           b_q, b_k, b_v, b_o, b_g, b_u, b_d,
           send, recv, ld):
    me = lax.axis_index("fsdp")
    core = lax.rem(me, 2)
    xc = lax.rem(me // 2, 2)
    yc = me // 4
    xn = me + 2 - 4 * xc
    yn = me + 4 - 8 * yc
    cn = me + 1 - 2 * core
    dg = xn + 4 - 8 * yc

    barrier = pltpu.get_barrier_semaphore()
    for nb in (xn, yn, cn):
        pl.semaphore_signal(barrier, inc=1, device_id={"fsdp": nb}, device_id_type=MESH)
    pl.semaphore_wait(barrier, 3)

    plan = Planner()

    def al(i, n):
        return i if isinstance(i, int) else pl.multiple_of(i, n)

    def view(ref, l, r0, nr, c0, nc):
        return ref.at[l, pl.ds(al(r0, 16), nr), pl.ds(al(c0, 128), nc)]

    def remote(key, link, pairs, dev, deps):
        sizes = [n for n, _ in pairs]

        def each():
            for i, (_, make) in zip(plan.all[key].sems, pairs):
                src, dst = make()
                yield pltpu.make_async_remote_copy(src_ref=src, dst_ref=dst, send_sem=send.at[i], recv_sem=recv.at[i],
                                                   device_id={"fsdp": dev}, device_id_type=MESH)

        plan.add(Transfer(key, link, sum(sizes), len(pairs), lambda: [c.start() for c in each()], lambda: [c.wait_recv() for c in each()],
                          lambda: [c.wait_send() for c in each()], deps))

    def local(key, pairs, deps):
        sizes = [n for n, _ in pairs]

        def each():
            for i, (_, make) in zip(plan.all[key].sems, pairs):
                src, dst = make()
                yield pltpu.make_async_copy(src, dst, send.at[i])

        plan.add(Transfer(key, "L", sum(sizes), len(pairs), lambda: [c.start() for c in each()], lambda: [c.wait() for c in each()], None, deps))

    def block(src, dst, l, col, other_col, nc, stage):
        def at(dev, other=False):
            return view(dst, l, dev * ROWS, ROWS, other_col if other else col, nc)

        def part(dev, p):
            return view(dst, l, dev * ROWS + (ROWS // 2) * p, ROWS // 2, col, nc)
        return (2 * ROWS * nc, lambda other=False: view(src, l, 0, ROWS, other_col if other else col, nc), at, stage)

    def down_block(l, j, stage):
        return (2 * DR * D, lambda other=False: view(w_d, l, j * DR, DR, 0, D), lambda dev, other=False: view(f_d, l, dev * FROWS + j * DR, DR, 0, D), stage)

    def shared_block(row_of):
        at = lambda dev, other=False: view(f_d, 1, row_of(dev), DR, 0, D)
        return (2 * DR * D, lambda other=False: at(me), at, None)

    def place(dev):
        return dev // 4, lax.rem(dev // 2, 2), lax.rem(dev, 2)

    def tp_row(j):
        def row(dev):
            yy, xx, cc = place(dev)
            return yy * HALF + xx * (2 * FROWS) + TF * (1 - xx) + (N_DT * DR) * cc + j * DR
        return row

    def dp_row(j):
        def row(dev):
            yy, xx, cc = place(dev)
            return yy * HALF + xx * (2 * FROWS) + (2 * FROWS - TF) * xx + (N_DD * DR) * cc + j * DR
        return row

    def add_round(rd, mats, parts, deps=(), before=None):
        K = lambda t: (rd, t)

        def own(other=False):
            return [(m[0], lambda m=m: (m[1](other), m[2](me, other))) for m in mats]

        def held(dev):
            return [(m[0], lambda m=m: (m[2](dev), m[2](dev))) for m in mats]

        for t in parts:
            if t == "X":
                remote(K(t), "X", own(), xn, deps)
            elif t == "Y":
                remote(K(t), "Y", own(other=True), yn, deps)
            elif t == "D":
                remote(K(t), "D", own(), cn, [])
            elif t == "XR":
                remote(K(t), "X", held(yn), xn, [K("Y")])
            elif t == "DX":
                remote(K(t), "D", held(xn), cn, [K("X")])
            elif t == "DY":
                remote(K(t), "D", held(yn), cn, [K("Y")])
            elif t == "DR":
                remote(K(t), "D", held(dg), cn, [K("XR")])
            elif t == "bin":
                local(K(t), [(m[0], lambda m=m: (m[1](), m[3])) for m in mats], [before] if before else [])
            else:
                local(K(t), [(m[0], lambda m=m: (m[3], m[2](me))) for m in mats], [K("bin")])
        if "D" in parts and "X" in parts:
            plan.mates[K("X")] = [K("D"), K("bin")]
        needs[rd] = [K(t) for t in parts]

    needs = {}
    FULL = ("X", "Y", "D", "XR", "DX", "DY", "DR", "bin", "bout")
    for l in (0, 1):
        add_round(("qkv", l), [block(w_q, f_q, l, 0, 0, D, b_q), block(w_k, f_k, l, 0, 0, KV, b_k), block(w_v, f_v, l, 0, 0, KV, b_v)], FULL,
                  before=(("qkv", 0), "bout") if l else None)
        add_round(("o", l), [block(w_o, f_o, l, 0, 0, D, b_o)], FULL, before=(("o", 0), "bout") if l else None)
    dn_seq = [("dn", l, j) for l in (0, 1) for j in range(N_DN)]
    for n, rd in enumerate(dn_seq):
        add_round(rd, [down_block(rd[1], rd[2], b_d.at[n % 4])], ("X", "D", "DX", "bin", "bout") if rd[1] == 0 else ("D", "bin", "bout"),
                  before=(dn_seq[n - 4], "bout") if n >= 4 else None)
    dn1 = [key for j in range(N_DN) for key in needs[("dn", 1, j)]]
    for j in range(N_DT):
        add_round(("dt", j), [shared_block(tp_row(j))], ("X", "DX"), deps=dn1)
    for j in range(N_DD):
        add_round(("dd", j), [shared_block(dp_row(j))], ("X", "Y", "XR", "DX", "DY", "DR"), deps=dn1)
    gu_seq = [("gu", j) for j in range(N_G0)] + [("gt", j) for j in TP_TILES] + [("gd", j) for j in range(N_DP)]
    for n, rd in enumerate(gu_seq):
        kind, j = rd
        l = 0 if kind == "gu" else 1
        if kind == "gd":
            col = (j % 2) * HALF + (j // 2) * (HALF - TF)
            other = col
        else:
            col, other = yc * HALF + j * TF, (1 - yc) * HALF + j * TF
        add_round(rd, [block(w_g, f_g, l, col, other, TF, b_g.at[n % 4]), block(w_u, f_u, l, col, other, TF, b_u.at[n % 4])], FULL,
                  before=(gu_seq[n - 4], "bout") if n >= 4 else None)
    for j in range(N_DN):
        plan.mates[(("gu", j), "X")] += [(("dn", 1, j), "D"), (("dn", 1, j), "bin")]
    for i in range(NB):
        mine, theirs = pl.ds(i * MB, MB), pl.ds(TOK + i * MB, MB)
        for l, land in ((0, f_p), (1, f_r)):
            remote(("h", l, i), "Y", [(2 * MB * D, lambda mine=mine, theirs=theirs: (h.at[mine, :], h.at[theirs, :]))], yn, [("h ready", l, i)])
            remote(("p", l, i), "Y", [(4 * MB * D, lambda mine=mine, theirs=theirs, land=land: (x.at[theirs, :], land.at[mine, :]))], yn, [("p ready", l, i)] + (P_AFTER.get(i, []) if l == 0 else []))

    def seq(rds, *ts):
        return [(rd, t) for rd in rds for t in ts]

    attn = lambda l: [("qkv", l), ("o", l)]
    gus, gts, gds = [("gu", j) for j in range(N_G0)], [("gt", j) for j in TP_TILES], [("gd", j) for j in range(N_DP)]
    dts, dds = [("dt", j) for j in range(N_DT)], [("dd", j) for j in range(N_DD)]
    plan.queue["X"] = (seq(attn(0), "X") + seq(attn(0), "XR") + seq(dn_seq[:N_DN], "X") + seq(gus, "X", "XR")
                       + seq(attn(1), "X") + seq(attn(1), "XR") + seq(dts, "X") + seq(gts, "X", "XR") + seq(dds, "X", "XR") + seq(gds, "X", "XR"))
    plan.queue["Y"] = TOKEN_ORDER + seq(attn(0), "Y") + seq(gus, "Y") + seq(attn(1), "Y") + seq(gts, "Y") + seq(dds, "Y") + seq(gds, "Y")

    def rows_of(i):
        return pl.ds(i * MB if isinstance(i, int) else pl.multiple_of(i * MB, MB), MB)

    def load(pairs):
        cps = [pltpu.make_async_copy(s, d, ld.at[i]) for i, (s, d) in enumerate(pairs)]
        for c in cps:
            c.start()
        for c in cps:
            c.wait()

    plan.service()
    run(plan.take())
    tok_in = pltpu.make_async_copy(tok, o, ld.at[0])
    tok_in.start()

    def tables(i, c):
        rows = rows_of(i)
        rr = lax.broadcasted_iota(jnp.int32, (MB, TOK), 0) + i * MB
        cc = lax.broadcasted_iota(jnp.int32, (MB, TOK), 1)
        seg = jnp.broadcast_to(seg_r[...], (MB, TOK)).astype(jnp.float32)
        seg_c = jnp.sum(jnp.where(cc == rr, seg, 0.0), axis=1, keepdims=True)
        ok = jnp.where((seg == seg_c) & (cc <= rr), 1.0, 0.0)
        mask[rows, :] = ok
        pos = jnp.sum(ok, axis=1, keepdims=True) - 1.0
        ang = pos * freq[...]
        lane = lax.broadcasted_iota(jnp.int32, (MB, HEAD), 1)
        cos_t[rows, :] = jnp.cos(ang)
        sn = jnp.sin(ang)
        sin_t[rows, :] = jnp.where(lane < HEAD // 2, -sn, sn)
        return c

    lax.fori_loop(0, NB, tables, 0)
    plan.spend(T_TABLES)
    plan.service()
    run(plan.take())
    tok_in.wait()

    def widen(i, c):
        rows = rows_of(i)
        x[rows, :] = o[rows, :].astype(jnp.float32)
        x[rows_of(i + NB), :] = jnp.zeros((MB, D), jnp.float32)
        return c

    lax.fori_loop(0, NB, widen, 0)
    plan.spend(T_WIDEN)

    def norm_row(gain_ref, l, i):
        rows = rows_of(i)
        xv = x[rows, :]
        inv = lax.rsqrt(jnp.mean(xv * xv, axis=-1, keepdims=True) + EPS)
        h[rows, :] = (xv * inv * gain_ref[l:l + 1, :].astype(jnp.float32)).astype(jnp.bfloat16)

    def rope(val, rows):
        f = val.astype(jnp.bfloat16).astype(jnp.float32)
        return (f * cos_t[rows, :] + pltpu.roll(f, HEAD // 2, 1) * sin_t[rows, :]).astype(jnp.bfloat16)

    def qkv_row(i):
        rows = rows_of(i)
        hv = h[rows, :]
        for g in range(HEADS // 4):
            val = jnp.dot(hv, vq[:, g * 512:(g + 1) * 512], preferred_element_type=jnp.float32)
            for e in range(4):
                q[rows, g * 512 + e * HEAD:g * 512 + (e + 1) * HEAD] = rope(val[:, e * HEAD:(e + 1) * HEAD], rows)
        val = jnp.dot(hv, vk[...], preferred_element_type=jnp.float32)
        for e in range(KV_HEADS):
            k[rows, e * HEAD:(e + 1) * HEAD] = rope(val[:, e * HEAD:(e + 1) * HEAD], rows)
        v[rows, :] = jnp.dot(hv, vv[...], preferred_element_type=jnp.float32).astype(jnp.bfloat16)

    def one_head(hd, blocks):
        qc = pl.ds(pl.multiple_of(hd * HEAD, HEAD), HEAD)
        kc = pl.ds(pl.multiple_of((hd // (HEADS // KV_HEADS)) * HEAD, HEAD), HEAD)
        for i in blocks:
            n = (i + 1) * MB
            s = lax.dot_general(q[i * MB:n, qc], k[0:n, kc], (((1,), (1,)), ((), ())), preferred_element_type=jnp.float32) * SCALE
            s = jnp.where(mask[i * MB:n, 0:n] > 0.5, s, -1e30)
            e = jnp.exp(s - jnp.max(s, axis=1, keepdims=True))
            p = (e / jnp.sum(e, axis=1, keepdims=True)).astype(jnp.bfloat16)
            o[i * MB:n, qc] = jnp.dot(p, v[0:n, kc], preferred_element_type=jnp.float32).astype(jnp.bfloat16)

    def act(hv):
        gt = jnp.dot(hv, vg[...], preferred_element_type=jnp.float32)
        up = jnp.dot(hv, vu[...], preferred_element_type=jnp.float32)
        return (gt * jax.nn.sigmoid(gt) * up).astype(jnp.bfloat16)

    def mlp_row(i, c):
        rows = rows_of(i)
        x[rows, :] += jnp.dot(act(h[rows, :]), vd[...], preferred_element_type=jnp.float32)
        return c

    def get_qkv(l):
        plan.need(needs[("qkv", l)])
        run(plan.take())
        load([(f_q.at[l], vq), (f_k.at[l], vk), (f_v.at[l], vv)])
        plan.spend(3.0)

    def get_o(l):
        plan.need(needs[("o", l)])
        run(plan.take())
        load([(f_o.at[l], vo)])
        plan.spend(2.0)

    def heads(blocks):
        table = []
        for i in range(HEADS):
            if i % 2 == 0 or len(blocks) == NB:
                plan.service()
            table.append(plan.take())
            plan.spend(T_HEAD * sum(b + 1 for b in blocks) / 10)

        def head_step(hd, c):
            run_at(hd, table)
            one_head(hd, blocks)
            return c

        lax.fori_loop(0, HEADS, head_step, 0)

    def proj_row(l, i):
        rows = rows_of(i)
        x[rows, :] += jnp.dot(o[rows, :], vo[...], preferred_element_type=jnp.float32)
        norm_row(g_mlp, l, i)

    def tiles(l, steps, offset, first, n_rows, marks=None):
        pre, post = {}, {}
        for n, (t, keys) in enumerate(steps):
            for key in (marks or {}).get((n, "pre"), ()):
                plan.mark(key)
            plan.need(keys)
            pre[t] = plan.take()
            plan.spend(2.2)
            for key in (marks or {}).get((n, "post"), ()):
                plan.mark(key)
            plan.service()
            post[t] = plan.take()
            plan.spend(T_TILE * n_rows / NB)

        def body(t, c):
            run_at(t, pre)
            cols = pl.ds(pl.multiple_of(offset(t), 128), TF)
            load([(f_g.at[l, :, cols], vg), (f_u.at[l, :, cols], vu), (f_d.at[l, cols, :], vd)])
            run_at(t, post)
            lax.fori_loop(first, first + n_rows, mlp_row, 0)
            return c

        lax.fori_loop(steps[0][0], steps[-1][0] + 1, body, 0)

    get_qkv(0)
    table_q = []
    for i in range(NB):
        plan.service()
        table_q.append(plan.take())
        plan.spend(T_QKV + T_NORM)

    def qkv_step(i, c):
        run_at(i, table_q)
        norm_row(g_attn, 0, i)
        qkv_row(i)
        return c

    lax.fori_loop(0, NB, qkv_step, 0)
    heads(range(NB))
    get_o(0)
    table_o = []
    for i in range(NB):
        plan.service()
        if i >= 2:
            plan.mark(("h ready", 0, i - 2))
            plan.fill()
        table_o.append(plan.take())
        plan.spend(T_PROJ + T_NORM)

    def proj_step(i, c):
        run_at(i, table_o)
        proj_row(0, i)
        return c

    lax.fori_loop(0, NB, proj_step, 0)

    dn0 = [key for j in range(N_DN) for key in needs[("dn", 0, j)]]
    half_off = lambda t: yc * HALF + t * TF
    steps = [(j, needs[("gu", j)] + dn0) for j in range(N_G0)]
    got_h = lambda l, *chunks: [("h", l, i) for i in chunks]
    tiles(0, steps[:OWN_FIRST], half_off, 0, NB, {(0, "pre"): [("h ready", 0, NB - 2)], (0, "post"): [("h ready", 0, NB - 1)]})
    tiles(0, [(j, keys + got_h(0, *range(NB))) for j, keys in steps], half_off, NB, NB)
    tiles(0, steps[OWN_FIRST:], half_off, 0, NB, {(0, "post"): [("p ready", 0, i) for i in range(NB)]})

    get_qkv(1)
    for i in range(NB):
        plan.need([("p", 0, i)])
        plan.retire(keys=[("p", 0, i)])
        run(plan.take())
        load([(f_p.at[rows_of(i), :], x.at[rows_of(i + NB), :])])
        x[rows_of(i), :] += x[rows_of(i + NB), :]
        norm_row(g_attn, 1, i)
        qkv_row(i)
        plan.spend(T_QKV + T_NORM + T_ADD)
        heads([i])
        if i == 0:
            get_o(1)
        proj_row(1, i)
        x[rows_of(i + NB), :] = jnp.zeros((MB, D), jnp.float32)
        plan.spend(T_PROJ + T_NORM + 0.4)
        plan.mark(("h ready", 1, i))
        plan.service()
        run(plan.take())

    dt1 = dn1 + [key for j in range(N_DT) for key in needs[("dt", j)]]
    dd1 = dn1 + [key for j in range(N_DD) for key in needs[("dd", j)]]
    steps = [(j, needs[("gt", j)] + dt1) for j in TP_TILES]
    h_mark = {}
    run_order = L1_ORDER
    marks = {}
    for n, what in enumerate(run_order):
        if what == "own":
            tiles(1, steps, half_off, 0, NB, {**h_mark, **marks})
            marks, h_mark = {}, {}
        elif what in GROUPS:
            chunks = GROUPS[what]
            tiles(1, [(j, keys + got_h(1, *chunks)) for j, keys in steps], half_off, NB + chunks[0], len(chunks), {**h_mark, **marks})
            marks, h_mark = {(0, "pre"): [("p ready", 1, i) for i in chunks[:-1]], (0, "post"): [("p ready", 1, chunks[-1])]}, {}
        else:
            tiles(1, [(j, needs[("gd", j)] + dd1) for j in range(N_DP)],
                  lambda t: lax.rem(t, 2) * HALF + lax.div(t, 2) * (HALF - TF), 0, NB, {**h_mark, **marks})
            marks, h_mark = {}, {}

    for i in range(NB - 1):
        plan.need([("p", 1, i)])
        plan.retire(keys=[("p", 1, i)])
        run(plan.take())
        load([(f_r.at[rows_of(i), :], x.at[rows_of(i + NB), :])])
        x[rows_of(i), :] += x[rows_of(i + NB), :]
        plan.spend(T_ADD)
    plan.service()
    done = pltpu.make_async_copy(x.at[pl.ds(0, TOK), :], out, ld.at[0])
    done.start()
    plan.need(plan.all)
    plan.retire(everything=True)
    run(plan.take())
    done.wait()


def finish(x_in, r_in, out, xv, rv, sem):
    n = TOK // FB
    first = (NB - 1) * MB // FB
    rows = [pl.ds(i * FB, FB) for i in range(n)]
    order = list(range(first, n)) + list(range(first))
    got = {i: pltpu.make_async_copy(x_in.at[rows[i], :], xv.at[rows[i], :], sem.at[0, i]) for i in range(n)}
    ret = {i: pltpu.make_async_copy(r_in.at[rows[i], :], rv.at[pl.ds((i - first) * FB, FB), :], sem.at[1, i]) for i in range(first, n)}
    put = {i: pltpu.make_async_copy(xv.at[rows[i], :], out.at[rows[i], :], sem.at[2, i]) for i in range(n)}
    for i in order:
        if i in ret:
            ret[i].start()
        got[i].start()
    for i in range(first, n):
        ret[i].wait()
        got[i].wait()
        xv[rows[i], :] += rv[pl.ds((i - first) * FB, FB), :]
    for i in range(first):
        got[i].wait()
        put[i].start()
    for i in range(first, n):
        put[i].start()
    for i in range(n):
        put[i].wait()


def solution(mesh):
    tok_spec = P(("rep", "fsdp"), None)
    seg_spec = P(("rep", "fsdp"))
    mat_spec = P(None, "fsdp", None)
    gain_spec = P(None, None)
    bf, f32 = jnp.bfloat16, jnp.float32

    def per_device(tokens, seg_ids, w_q, w_k, w_v, w_o, w_gate, w_up, w_down, g_attn, g_mlp):
        half = HEAD // 2
        inv = np.float32(ROPE_BASE) ** (-np.arange(half, dtype=np.float32) / np.float32(half))
        freq = jnp.asarray(np.concatenate([inv, inv]).reshape(1, HEAD), f32)
        any_s = pl.BlockSpec(memory_space=pl.ANY)
        vm = pl.BlockSpec(memory_space=pltpu.VMEM)
        full = [(LAYERS, D, D), (LAYERS, D, KV), (LAYERS, D, KV), (LAYERS, D, D), (LAYERS, D, FF), (LAYERS, D, FF), (LAYERS, FF, D)]
        res = pl.pallas_call(
            kernel,
            out_shape=[jax.ShapeDtypeStruct((TOK, D), f32)] * 2 + [jax.ShapeDtypeStruct(s, bf) for s in full] + [jax.ShapeDtypeStruct((TOK, D), f32)],
            in_specs=[any_s, vm, vm, vm, vm] + [any_s] * 7,
            out_specs=[any_s] * 10,
            scratch_shapes=[
                pltpu.VMEM((2 * TOK, D), f32), pltpu.VMEM((2 * TOK, D), bf), pltpu.VMEM((TOK, D), bf),
                pltpu.VMEM((TOK, KV), bf), pltpu.VMEM((TOK, KV), bf), pltpu.VMEM((TOK, D), bf),
                pltpu.VMEM((TOK, HEAD), f32), pltpu.VMEM((TOK, HEAD), f32), pltpu.VMEM((TOK, TOK), f32),
                pltpu.VMEM((D, D), bf), pltpu.VMEM((D, KV), bf), pltpu.VMEM((D, KV), bf), pltpu.VMEM((D, D), bf),
                pltpu.VMEM((D, TF), bf), pltpu.VMEM((D, TF), bf), pltpu.VMEM((TF, D), bf),
                pltpu.VMEM((ROWS, D), bf), pltpu.VMEM((ROWS, KV), bf), pltpu.VMEM((ROWS, KV), bf), pltpu.VMEM((ROWS, D), bf),
                pltpu.VMEM((4, ROWS, TF), bf), pltpu.VMEM((4, ROWS, TF), bf), pltpu.VMEM((4, DR, D), bf),
                pltpu.SemaphoreType.DMA((N_SEM,)), pltpu.SemaphoreType.DMA((N_SEM,)), pltpu.SemaphoreType.DMA((4,)),
            ],
            compiler_params=pltpu.CompilerParams(collective_id=0, has_side_effects=True, vmem_limit_bytes=66 * 1000 * 1000),
        )(tokens, seg_ids.reshape(1, TOK), freq, g_attn, g_mlp, w_q, w_k, w_v, w_o, w_gate, w_up, w_down)
        return pl.pallas_call(
            finish,
            out_shape=jax.ShapeDtypeStruct((TOK, D), f32),
            in_specs=[any_s, any_s],
            out_specs=any_s,
            scratch_shapes=[pltpu.VMEM((TOK, D), f32), pltpu.VMEM((MB, D), f32), pltpu.SemaphoreType.DMA((3, TOK // FB))],
            compiler_params=pltpu.CompilerParams(vmem_limit_bytes=66 * 1000 * 1000),
        )(res[0], res[1])

    return jax.shard_map(per_device, mesh=mesh, in_specs=(tok_spec, seg_spec, mat_spec, mat_spec, mat_spec, mat_spec, mat_spec, mat_spec, mat_spec, gain_spec, gain_spec), out_specs=tok_spec, check_vma=False)
```

```python
import jax
import jax.numpy as jnp
import numpy as np
from jax import lax
from jax.experimental import pallas as pl
from jax.experimental.pallas import tpu as pltpu
from jax.sharding import PartitionSpec as P

HEAD = 128
HEADS = 12
KV_HEADS = 2
EPS = 1e-5
ROPE_BASE = 10000.0
MESH = pl.DeviceIdType.MESH

N_DEV = 8
TOK = 1024
D = 1536
KV = KV_HEADS * HEAD
FF = 8960
HALF = FF // 2
ROWS = D // N_DEV
FROWS = FF // N_DEV
TF = 640
N_G0 = HALF // TF
TP_TILES = (1, 2, 3, 4, 5)
N_DP = 4
DR = 160
N_DT = 5
N_DD = 2
N_DN = FROWS // DR
LAYERS = 2
MB = 256
NB = TOK // MB
SCALE = HEAD ** -0.5

RATE = {"X": 46600.0, "Y": 46600.0, "D": 500000.0, "L": 800000.0}
LAT = {"X": 2.5, "Y": 2.5, "D": 1.5, "L": 1.0}
HORIZON = 20.0
T_TABLES, T_WIDEN, T_NORM, T_QKV, T_HEAD, T_PROJ, T_TILE, T_ADD = 3.0, 1.6, 0.4, 1.8, 2.0, 1.1, 7.0, 1.7
OWN_FIRST = 3
P_AFTER = {3: [("h ready", 1, 1)]}
L1_ORDER = (("own", 0, 2), "lo", "hi", ("own", 2, 5), "dp")
GROUPS = {"c0": (0,), "c1": (1,), "lo": (0, 1), "hi": (2, 3), "c123": (1, 2, 3)}
TOKEN_ORDER = [(c, l, i) for c, l in (("h", 0), ("p", 0), ("h", 1), ("p", 1)) for i in range(NB)]
N_SEM = 226
T_LOAD = 2.4
FB = 128


class Transfer:
    def __init__(self, key, link, size, n_sem, start, wait, done, deps):
        self.key, self.link, self.size, self.n_sem = key, link, size, n_sem
        self.start, self.wait, self.done, self.deps = start, wait, done, set(deps)
        self.sems = []


class Planner:
    def __init__(self):
        self.now = 0.0
        self.free = dict.fromkeys("XYDL", 0.0)
        self.all, self.queue, self.users, self.mates = {}, {"X": [], "Y": []}, {}, {}
        self.pool = list(range(N_SEM))
        self.issued, self.arrived, self.flying, self.sent, self.ops = set(), set(), [], [], []

    def add(self, tr):
        self.all[tr.key] = tr
        for dep in tr.deps:
            self.users.setdefault(dep, []).append(tr.key)

    def issue(self, key):
        tr = self.all[key]
        self.issued.add(key)
        tr.sems, self.pool = self.pool[:tr.n_sem], self.pool[tr.n_sem:]
        self.ops.append(tr.start)
        self.free[tr.link] = max(self.free[tr.link], self.now) + tr.size / RATE[tr.link]
        self.flying.append((self.free[tr.link] + LAT[tr.link], key))
        for mate in self.mates.get(key, ()):
            if mate not in self.issued and self.all[mate].deps <= self.arrived:
                self.issue(mate)

    def mark(self, key):
        self.arrived.add(key)
        for user in self.users.get(key, ()):
            tr = self.all[user]
            if tr.link in "DL" and user not in self.issued and tr.deps <= self.arrived:
                self.issue(user)

    def receive(self, item):
        self.flying.remove(item)
        tr = self.all[item[1]]
        self.ops.append(tr.wait)
        if tr.done is not None:
            self.sent.append((item[0] + 2.0, item[1]))
        else:
            self.pool += tr.sems
        self.mark(item[1])

    def fill(self):
        for link in "XY":
            while self.free[link] - self.now < HORIZON:
                ready = [k for k in self.queue[link] if self.all[k].deps <= self.arrived]
                if not ready:
                    break
                self.queue[link].remove(ready[0])
                self.issue(ready[0])

    def retire(self, keys=None, everything=False):
        for item in list(self.sent):
            if everything or (keys is not None and item[1] in keys) or (keys is None and item[0] <= self.now):
                self.sent.remove(item)
                self.ops.append(self.all[item[1]].done)
                self.pool += self.all[item[1]].sems

    def service(self):
        while True:
            due = sorted(i for i in self.flying if i[0] <= self.now)
            if not due:
                break
            self.receive(due[0])
            self.fill()
        self.fill()
        self.retire()

    def need(self, keys):
        keys = set(keys)
        while not keys <= self.arrived:
            self.fill()
            item = min(self.flying)
            self.now = max(self.now, item[0])
            self.receive(item)
        self.service()

    def spend(self, us):
        self.now += us

    def take(self):
        ops, self.ops = self.ops, []
        return ops


def run(ops):
    for op in ops:
        op()


def run_at(index, table):
    for k, ops in (table.items() if isinstance(table, dict) else enumerate(table)):
        if ops:
            pl.when(index == k)(lambda ops=ops: run(ops))


def kernel(tok, seg_r, freq, g_attn, g_mlp, w_q, w_k, w_v, w_o, w_g, w_u, w_d,
           out, f_r, f_q, f_k, f_v, f_o, f_g, f_u, f_d, f_p,
           x, h, q, k, v, o, cos_t, sin_t, mask, vq, vk, vv, vo, vg, vu, vd,
           b_q, b_k, b_v, b_o, b_g, b_u, b_d,
           send, recv, ld, tl):
    me = lax.axis_index("fsdp")
    core = lax.rem(me, 2)
    xc = lax.rem(me // 2, 2)
    yc = me // 4
    xn = me + 2 - 4 * xc
    yn = me + 4 - 8 * yc
    cn = me + 1 - 2 * core
    dg = xn + 4 - 8 * yc

    barrier = pltpu.get_barrier_semaphore()
    for nb in (xn, yn, cn):
        pl.semaphore_signal(barrier, inc=1, device_id={"fsdp": nb}, device_id_type=MESH)
    pl.semaphore_wait(barrier, 3)

    plan = Planner()

    def al(i, n):
        return i if isinstance(i, int) else pl.multiple_of(i, n)

    def view(ref, l, r0, nr, c0, nc):
        return ref.at[l, pl.ds(al(r0, 16), nr), pl.ds(al(c0, 128), nc)]

    def remote(key, link, pairs, dev, deps):
        sizes = [n for n, _ in pairs]

        def each():
            for i, (_, make) in zip(plan.all[key].sems, pairs):
                src, dst = make()
                yield pltpu.make_async_remote_copy(src_ref=src, dst_ref=dst, send_sem=send.at[i], recv_sem=recv.at[i],
                                                   device_id={"fsdp": dev}, device_id_type=MESH)

        plan.add(Transfer(key, link, sum(sizes), len(pairs), lambda: [c.start() for c in each()], lambda: [c.wait_recv() for c in each()],
                          lambda: [c.wait_send() for c in each()], deps))

    def local(key, pairs, deps):
        sizes = [n for n, _ in pairs]

        def each():
            for i, (_, make) in zip(plan.all[key].sems, pairs):
                src, dst = make()
                yield pltpu.make_async_copy(src, dst, send.at[i])

        plan.add(Transfer(key, "L", sum(sizes), len(pairs), lambda: [c.start() for c in each()], lambda: [c.wait() for c in each()], None, deps))

    def block(src, dst, l, col, other_col, nc, stage):
        def at(dev, other=False):
            return view(dst, l, dev * ROWS, ROWS, other_col if other else col, nc)

        def part(dev, p):
            return view(dst, l, dev * ROWS + (ROWS // 2) * p, ROWS // 2, col, nc)
        return (2 * ROWS * nc, lambda other=False: view(src, l, 0, ROWS, other_col if other else col, nc), at, stage)

    def down_block(l, j, stage):
        return (2 * DR * D, lambda other=False: view(w_d, l, j * DR, DR, 0, D), lambda dev, other=False: view(f_d, l, dev * FROWS + j * DR, DR, 0, D), stage)

    def shared_block(row_of):
        at = lambda dev, other=False: view(f_d, 1, row_of(dev), DR, 0, D)
        return (2 * DR * D, lambda other=False: at(me), at, None)

    def place(dev):
        return dev // 4, lax.rem(dev // 2, 2), lax.rem(dev, 2)

    def tp_row(j):
        def row(dev):
            yy, xx, cc = place(dev)
            return yy * HALF + xx * (2 * FROWS) + TF * (1 - xx) + (N_DT * DR) * cc + j * DR
        return row

    def dp_row(j):
        def row(dev):
            yy, xx, cc = place(dev)
            return yy * HALF + xx * (2 * FROWS) + (2 * FROWS - TF) * xx + (N_DD * DR) * cc + j * DR
        return row

    def add_round(rd, mats, parts, deps=(), before=None):
        K = lambda t: (rd, t)

        def own(other=False):
            return [(m[0], lambda m=m: (m[1](other), m[2](me, other))) for m in mats]

        def held(dev):
            return [(m[0], lambda m=m: (m[2](dev), m[2](dev))) for m in mats]

        for t in parts:
            if t == "X":
                remote(K(t), "X", own(), xn, deps)
            elif t == "Y":
                remote(K(t), "Y", own(other=True), yn, deps)
            elif t == "D":
                remote(K(t), "D", own(), cn, [])
            elif t == "XR":
                remote(K(t), "X", held(yn), xn, [K("Y")])
            elif t == "DX":
                remote(K(t), "D", held(xn), cn, [K("X")])
            elif t == "DY":
                remote(K(t), "D", held(yn), cn, [K("Y")])
            elif t == "DR":
                remote(K(t), "D", held(dg), cn, [K("XR")])
            elif t == "bin":
                local(K(t), [(m[0], lambda m=m: (m[1](), m[3])) for m in mats], [before] if before else [])
            else:
                local(K(t), [(m[0], lambda m=m: (m[3], m[2](me))) for m in mats], [K("bin")])
        if "D" in parts and "X" in parts:
            plan.mates[K("X")] = [K("D"), K("bin")]
        needs[rd] = [K(t) for t in parts]

    needs = {}
    FULL = ("X", "Y", "D", "XR", "DX", "DY", "DR", "bin", "bout")
    for l in (0, 1):
        add_round(("qkv", l), [block(w_q, f_q, l, 0, 0, D, b_q), block(w_k, f_k, l, 0, 0, KV, b_k), block(w_v, f_v, l, 0, 0, KV, b_v)], FULL,
                  before=(("qkv", 0), "bout") if l else None)
        add_round(("o", l), [block(w_o, f_o, l, 0, 0, D, b_o)], FULL, before=(("o", 0), "bout") if l else None)
    dn_seq = [("dn", l, j) for l in (0, 1) for j in range(N_DN)]
    for n, rd in enumerate(dn_seq):
        add_round(rd, [down_block(rd[1], rd[2], b_d.at[n % 4])], ("X", "D", "DX", "bin", "bout") if rd[1] == 0 else ("D", "bin", "bout"),
                  before=(dn_seq[n - 4], "bout") if n >= 4 else None)
    dn1 = [key for j in range(N_DN) for key in needs[("dn", 1, j)]]
    for j in range(N_DT):
        add_round(("dt", j), [shared_block(tp_row(j))], ("X", "DX"), deps=dn1)
    for j in range(N_DD):
        add_round(("dd", j), [shared_block(dp_row(j))], ("X", "Y", "XR", "DX", "DY", "DR"), deps=dn1)
    gu_seq = [("gu", j) for j in range(N_G0)] + [("gt", j) for j in TP_TILES] + [("gd", j) for j in range(N_DP)]
    for n, rd in enumerate(gu_seq):
        kind, j = rd
        l = 0 if kind == "gu" else 1
        if kind == "gd":
            col = (j % 2) * HALF + (j // 2) * (HALF - TF)
            other = col
        else:
            col, other = yc * HALF + j * TF, (1 - yc) * HALF + j * TF
        add_round(rd, [block(w_g, f_g, l, col, other, TF, b_g.at[n % 4]), block(w_u, f_u, l, col, other, TF, b_u.at[n % 4])], FULL,
                  before=(gu_seq[n - 4], "bout") if n >= 4 else None)
    for j in range(N_DN):
        plan.mates[(("gu", j), "X")] += [(("dn", 1, j), "D"), (("dn", 1, j), "bin")]
    for i in range(NB):
        mine, theirs = pl.ds(i * MB, MB), pl.ds(TOK + i * MB, MB)
        for l, land in ((0, f_p), (1, f_r)):
            remote(("h", l, i), "Y", [(2 * MB * D, lambda mine=mine, theirs=theirs: (h.at[mine, :], h.at[theirs, :]))], yn, [("h ready", l, i)])
            remote(("p", l, i), "Y", [(4 * MB * D, lambda mine=mine, theirs=theirs, land=land: (x.at[theirs, :], land.at[mine, :]))], yn, [("p ready", l, i)] + (P_AFTER.get(i, []) if l == 0 else []))

    def seq(rds, *ts):
        return [(rd, t) for rd in rds for t in ts]

    attn = lambda l: [("qkv", l), ("o", l)]
    gus, gts, gds = [("gu", j) for j in range(N_G0)], [("gt", j) for j in TP_TILES], [("gd", j) for j in range(N_DP)]
    dts, dds = [("dt", j) for j in range(N_DT)], [("dd", j) for j in range(N_DD)]
    plan.queue["X"] = (seq(attn(0), "X") + seq(attn(0), "XR") + seq(dn_seq[:N_DN], "X") + seq(gus, "X", "XR")
                       + seq(attn(1), "X") + seq(attn(1), "XR") + seq(dts, "X") + seq(gts, "X", "XR") + seq(dds, "X", "XR") + seq(gds, "X", "XR"))
    plan.queue["Y"] = TOKEN_ORDER + seq(attn(0), "Y") + seq(gus, "Y") + seq(attn(1), "Y") + seq(gts, "Y") + seq(dds, "Y") + seq(gds, "Y")

    def rows_of(i):
        return pl.ds(i * MB if isinstance(i, int) else pl.multiple_of(i * MB, MB), MB)

    def load(pairs):
        cps = [pltpu.make_async_copy(s, d, ld.at[i]) for i, (s, d) in enumerate(pairs)]
        for c in cps:
            c.start()
        for c in cps:
            c.wait()

    plan.service()
    run(plan.take())
    tok_in = pltpu.make_async_copy(tok, o, ld.at[0])
    tok_in.start()

    def tables(i, c):
        rows = rows_of(i)
        rr = lax.broadcasted_iota(jnp.int32, (MB, TOK), 0) + i * MB
        cc = lax.broadcasted_iota(jnp.int32, (MB, TOK), 1)
        seg = jnp.broadcast_to(seg_r[...], (MB, TOK)).astype(jnp.float32)
        seg_c = jnp.sum(jnp.where(cc == rr, seg, 0.0), axis=1, keepdims=True)
        ok = jnp.where((seg == seg_c) & (cc <= rr), 1.0, 0.0)
        mask[rows, :] = ok
        pos = jnp.sum(ok, axis=1, keepdims=True) - 1.0
        ang = pos * freq[...]
        lane = lax.broadcasted_iota(jnp.int32, (MB, HEAD), 1)
        cos_t[rows, :] = jnp.cos(ang)
        sn = jnp.sin(ang)
        sin_t[rows, :] = jnp.where(lane < HEAD // 2, -sn, sn)
        return c

    lax.fori_loop(0, NB, tables, 0)
    plan.spend(T_TABLES)
    plan.service()
    run(plan.take())
    tok_in.wait()

    def widen(i, c):
        rows = rows_of(i)
        x[rows, :] = o[rows, :].astype(jnp.float32)
        x[rows_of(i + NB), :] = jnp.zeros((MB, D), jnp.float32)
        return c

    lax.fori_loop(0, NB, widen, 0)
    plan.spend(T_WIDEN)

    def norm_row(gain_ref, l, i):
        rows = rows_of(i)
        xv = x[rows, :]
        inv = lax.rsqrt(jnp.mean(xv * xv, axis=-1, keepdims=True) + EPS)
        h[rows, :] = (xv * inv * gain_ref[l:l + 1, :].astype(jnp.float32)).astype(jnp.bfloat16)

    def rope(val, rows):
        f = val.astype(jnp.bfloat16).astype(jnp.float32)
        return (f * cos_t[rows, :] + pltpu.roll(f, HEAD // 2, 1) * sin_t[rows, :]).astype(jnp.bfloat16)

    def qkv_row(i):
        rows = rows_of(i)
        hv = h[rows, :]
        for g in range(HEADS // 4):
            val = jnp.dot(hv, vq[:, g * 512:(g + 1) * 512], preferred_element_type=jnp.float32)
            for e in range(4):
                q[rows, g * 512 + e * HEAD:g * 512 + (e + 1) * HEAD] = rope(val[:, e * HEAD:(e + 1) * HEAD], rows)
        val = jnp.dot(hv, vk[...], preferred_element_type=jnp.float32)
        for e in range(KV_HEADS):
            k[rows, e * HEAD:(e + 1) * HEAD] = rope(val[:, e * HEAD:(e + 1) * HEAD], rows)
        v[rows, :] = jnp.dot(hv, vv[...], preferred_element_type=jnp.float32).astype(jnp.bfloat16)

    def one_head(hd, blocks):
        qc = pl.ds(pl.multiple_of(hd * HEAD, HEAD), HEAD)
        kc = pl.ds(pl.multiple_of((hd // (HEADS // KV_HEADS)) * HEAD, HEAD), HEAD)
        for i in blocks:
            n = (i + 1) * MB
            s = lax.dot_general(q[i * MB:n, qc], k[0:n, kc], (((1,), (1,)), ((), ())), preferred_element_type=jnp.float32) * SCALE
            s = jnp.where(mask[i * MB:n, 0:n] > 0.5, s, -1e30)
            e = jnp.exp(s - jnp.max(s, axis=1, keepdims=True))
            p = (e / jnp.sum(e, axis=1, keepdims=True)).astype(jnp.bfloat16)
            o[i * MB:n, qc] = jnp.dot(p, v[0:n, kc], preferred_element_type=jnp.float32).astype(jnp.bfloat16)

    def mlp_row(i, slot, c):
        rows = rows_of(i)
        hv = h[rows, :]
        gt = jnp.dot(hv, vg[slot], preferred_element_type=jnp.float32)
        up = jnp.dot(hv, vu[slot], preferred_element_type=jnp.float32)
        a = (gt * jax.nn.sigmoid(gt) * up).astype(jnp.bfloat16)
        x[rows, :] += jnp.dot(a, vd[slot], preferred_element_type=jnp.float32)
        return c

    def get_qkv(l):
        plan.need(needs[("qkv", l)])
        run(plan.take())
        load([(f_q.at[l], vq), (f_k.at[l], vk), (f_v.at[l], vv)])
        plan.spend(3.0)

    def get_o(l):
        plan.need(needs[("o", l)])
        run(plan.take())
        load([(f_o.at[l], vo)])
        plan.spend(2.0)

    def heads(blocks):
        table = []
        for i in range(HEADS):
            if i % 2 == 0 or len(blocks) == NB:
                plan.service()
            table.append(plan.take())
            plan.spend(T_HEAD * sum(b + 1 for b in blocks) / 10)

        def head_step(hd, c):
            run_at(hd, table)
            one_head(hd, blocks)
            return c

        lax.fori_loop(0, HEADS, head_step, 0)

    def proj_row(l, i):
        rows = rows_of(i)
        x[rows, :] += jnp.dot(o[rows, :], vo[...], preferred_element_type=jnp.float32)
        norm_row(g_mlp, l, i)

    def tiles(l, steps, offset, first, n_rows, marks=None):
        pre, post, ahead = {}, {}, {}
        early = False
        for n, (t, keys) in enumerate(steps):
            for key in (marks or {}).get((n, "pre"), ()):
                plan.mark(key)
            plan.need(keys)
            pre[t] = plan.take()
            if not early:
                pre[t].append(lambda t=t: [c.start() for c in tile_loads(l, offset(t), t % 2)])
                plan.spend(T_LOAD)
            for key in (marks or {}).get((n, "post"), ()):
                plan.mark(key)
            plan.service()
            post[t] = plan.take()
            early = n + 1 < len(steps) and set(steps[n + 1][1]) <= plan.arrived
            if early:
                post[t].append(lambda t=t: [c.start() for c in tile_loads(l, offset(t + 1), (t + 1) % 2)])
            plan.spend(T_TILE * n_rows / NB)

        def body(t, c):
            slot = lax.rem(t, 2)
            run_at(t, pre)
            for cp in tile_loads(l, offset(t), slot):
                cp.wait()
            run_at(t, post)
            lax.fori_loop(first, first + n_rows, lambda i, c: mlp_row(i, slot, c), 0)
            return c

        lax.fori_loop(steps[0][0], steps[-1][0] + 1, body, 0)

    def tile_loads(l, off, slot):
        cols = pl.ds(al(off, 128), TF)
        return [pltpu.make_async_copy(f_g.at[l, :, cols], vg.at[slot], tl.at[slot, 0]), pltpu.make_async_copy(f_u.at[l, :, cols], vu.at[slot], tl.at[slot, 1]),
                pltpu.make_async_copy(f_d.at[l, cols, :], vd.at[slot], tl.at[slot, 2])]

    get_qkv(0)
    table_q = []
    for i in range(NB):
        plan.service()
        table_q.append(plan.take())
        plan.spend(T_QKV + T_NORM)

    def qkv_step(i, c):
        run_at(i, table_q)
        norm_row(g_attn, 0, i)
        qkv_row(i)
        return c

    lax.fori_loop(0, NB, qkv_step, 0)
    heads(range(NB))
    get_o(0)
    table_o = []
    for i in range(NB):
        plan.service()
        if i >= 2:
            plan.mark(("h ready", 0, i - 2))
            plan.fill()
        table_o.append(plan.take())
        plan.spend(T_PROJ + T_NORM)

    def proj_step(i, c):
        run_at(i, table_o)
        proj_row(0, i)
        return c

    lax.fori_loop(0, NB, proj_step, 0)

    dn0 = [key for j in range(N_DN) for key in needs[("dn", 0, j)]]
    half_off = lambda t: yc * HALF + t * TF
    steps = [(j, needs[("gu", j)] + dn0) for j in range(N_G0)]
    got_h = lambda l, *chunks: [("h", l, i) for i in chunks]
    tiles(0, steps[:OWN_FIRST], half_off, 0, NB, {(0, "pre"): [("h ready", 0, NB - 2)], (0, "post"): [("h ready", 0, NB - 1)]})
    tiles(0, [(j, keys + got_h(0, *range(NB))) for j, keys in steps], half_off, NB, NB)
    tiles(0, steps[OWN_FIRST:], half_off, 0, NB, {(0, "post"): [("p ready", 0, i) for i in range(NB)]})

    get_qkv(1)
    for i in range(NB):
        plan.need([("p", 0, i)])
        plan.retire(keys=[("p", 0, i)])
        run(plan.take())
        load([(f_p.at[rows_of(i), :], x.at[rows_of(i + NB), :])])
        x[rows_of(i), :] += x[rows_of(i + NB), :]
        norm_row(g_attn, 1, i)
        qkv_row(i)
        plan.spend(T_QKV + T_NORM + T_ADD)
        heads([i])
        if i == 0:
            get_o(1)
        proj_row(1, i)
        x[rows_of(i + NB), :] = jnp.zeros((MB, D), jnp.float32)
        plan.spend(T_PROJ + T_NORM + 0.4)
        plan.mark(("h ready", 1, i))
        plan.service()
        run(plan.take())

    dt1 = dn1 + [key for j in range(N_DT) for key in needs[("dt", j)]]
    dd1 = dn1 + [key for j in range(N_DD) for key in needs[("dd", j)]]
    steps = [(j, needs[("gt", j)] + dt1) for j in TP_TILES]
    h_mark = {}
    run_order = L1_ORDER
    marks = {}
    for n, what in enumerate(run_order):
        if what[0] == "own":
            tiles(1, steps[what[1]:what[2]], half_off, 0, NB, {**h_mark, **marks})
            marks, h_mark = {}, {}
        elif what in GROUPS:
            chunks = GROUPS[what]
            tiles(1, [(j, keys + got_h(1, *chunks)) for j, keys in steps], half_off, NB + chunks[0], len(chunks), {**h_mark, **marks})
            marks, h_mark = {(0, "pre"): [("p ready", 1, i) for i in chunks[:-1]], (0, "post"): [("p ready", 1, chunks[-1])]}, {}
        else:
            tiles(1, [(j, needs[("gd", j)] + dd1) for j in range(N_DP)],
                  lambda t: (t % 2) * HALF + (t // 2) * (HALF - TF) if isinstance(t, int) else lax.rem(t, 2) * HALF + lax.div(t, 2) * (HALF - TF), 0, NB, {**h_mark, **marks})
            marks, h_mark = {}, {}

    for i in range(NB - 1):
        plan.need([("p", 1, i)])
        plan.retire(keys=[("p", 1, i)])
        run(plan.take())
        load([(f_r.at[rows_of(i), :], x.at[rows_of(i + NB), :])])
        x[rows_of(i), :] += x[rows_of(i + NB), :]
        plan.spend(T_ADD)
    plan.service()
    done = pltpu.make_async_copy(x.at[pl.ds(0, TOK), :], out, ld.at[0])
    done.start()
    plan.need(plan.all)
    plan.retire(everything=True)
    run(plan.take())
    done.wait()


def finish(x_in, r_in, out, xv, rv, sem):
    n = TOK // FB
    first = (NB - 1) * MB // FB
    rows = [pl.ds(i * FB, FB) for i in range(n)]
    order = list(range(first, n)) + list(range(first))
    got = {i: pltpu.make_async_copy(x_in.at[rows[i], :], xv.at[rows[i], :], sem.at[0, i]) for i in range(n)}
    ret = {i: pltpu.make_async_copy(r_in.at[rows[i], :], rv.at[pl.ds((i - first) * FB, FB), :], sem.at[1, i]) for i in range(first, n)}
    put = {i: pltpu.make_async_copy(xv.at[rows[i], :], out.at[rows[i], :], sem.at[2, i]) for i in range(n)}
    for i in order:
        if i in ret:
            ret[i].start()
        got[i].start()
    for i in range(first, n):
        ret[i].wait()
        got[i].wait()
        xv[rows[i], :] += rv[pl.ds((i - first) * FB, FB), :]
    for i in range(first):
        got[i].wait()
        put[i].start()
    for i in range(first, n):
        put[i].start()
    for i in range(n):
        put[i].wait()


def solution(mesh):
    tok_spec = P(("rep", "fsdp"), None)
    seg_spec = P(("rep", "fsdp"))
    mat_spec = P(None, "fsdp", None)
    gain_spec = P(None, None)
    bf, f32 = jnp.bfloat16, jnp.float32

    def per_device(tokens, seg_ids, w_q, w_k, w_v, w_o, w_gate, w_up, w_down, g_attn, g_mlp):
        half = HEAD // 2
        inv = np.float32(ROPE_BASE) ** (-np.arange(half, dtype=np.float32) / np.float32(half))
        freq = jnp.asarray(np.concatenate([inv, inv]).reshape(1, HEAD), f32)
        any_s = pl.BlockSpec(memory_space=pl.ANY)
        vm = pl.BlockSpec(memory_space=pltpu.VMEM)
        full = [(LAYERS, D, D), (LAYERS, D, KV), (LAYERS, D, KV), (LAYERS, D, D), (LAYERS, D, FF), (LAYERS, D, FF), (LAYERS, FF, D)]
        res = pl.pallas_call(
            kernel,
            out_shape=[jax.ShapeDtypeStruct((TOK, D), f32)] * 2 + [jax.ShapeDtypeStruct(s, bf) for s in full] + [jax.ShapeDtypeStruct((TOK, D), f32)],
            in_specs=[any_s, vm, vm, vm, vm] + [any_s] * 7,
            out_specs=[any_s] * 10,
            scratch_shapes=[
                pltpu.VMEM((2 * TOK, D), f32), pltpu.VMEM((2 * TOK, D), bf), pltpu.VMEM((TOK, D), bf),
                pltpu.VMEM((TOK, KV), bf), pltpu.VMEM((TOK, KV), bf), pltpu.VMEM((TOK, D), bf),
                pltpu.VMEM((TOK, HEAD), f32), pltpu.VMEM((TOK, HEAD), f32), pltpu.VMEM((TOK, TOK), f32),
                pltpu.VMEM((D, D), bf), pltpu.VMEM((D, KV), bf), pltpu.VMEM((D, KV), bf), pltpu.VMEM((D, D), bf),
                pltpu.VMEM((2, D, TF), bf), pltpu.VMEM((2, D, TF), bf), pltpu.VMEM((2, TF, D), bf),
                pltpu.VMEM((ROWS, D), bf), pltpu.VMEM((ROWS, KV), bf), pltpu.VMEM((ROWS, KV), bf), pltpu.VMEM((ROWS, D), bf),
                pltpu.VMEM((4, ROWS, TF), bf), pltpu.VMEM((4, ROWS, TF), bf), pltpu.VMEM((4, DR, D), bf),
                pltpu.SemaphoreType.DMA((N_SEM,)), pltpu.SemaphoreType.DMA((N_SEM,)), pltpu.SemaphoreType.DMA((4,)), pltpu.SemaphoreType.DMA((2, 3)),
            ],
            compiler_params=pltpu.CompilerParams(collective_id=0, has_side_effects=True, vmem_limit_bytes=66 * 1000 * 1000),
        )(tokens, seg_ids.reshape(1, TOK), freq, g_attn, g_mlp, w_q, w_k, w_v, w_o, w_gate, w_up, w_down)
        return pl.pallas_call(
            finish,
            out_shape=jax.ShapeDtypeStruct((TOK, D), f32),
            in_specs=[any_s, any_s],
            out_specs=any_s,
            scratch_shapes=[pltpu.VMEM((TOK, D), f32), pltpu.VMEM((MB, D), f32), pltpu.SemaphoreType.DMA((3, TOK // FB))],
            compiler_params=pltpu.CompilerParams(vmem_limit_bytes=66 * 1000 * 1000),
        )(res[0], res[1])

    return jax.shard_map(per_device, mesh=mesh, in_specs=(tok_spec, seg_spec, mat_spec, mat_spec, mat_spec, mat_spec, mat_spec, mat_spec, mat_spec, gain_spec, gain_spec), out_specs=tok_spec, check_vma=False)
```

```python
import jax
import jax.numpy as jnp
import numpy as np
from jax import lax
from jax.experimental import pallas as pl
from jax.experimental.pallas import tpu as pltpu
from jax.sharding import PartitionSpec as P

HEAD = 128
HEADS = 12
KV_HEADS = 2
EPS = 1e-5
ROPE_BASE = 10000.0
MESH = pl.DeviceIdType.MESH

N_DEV = 8
TOK = 1024
D = 1536
KV = KV_HEADS * HEAD
FF = 8960
HALF = FF // 2
ROWS = D // N_DEV
FROWS = FF // N_DEV
TF = 640
N_G0 = HALF // TF
TP_TILES = (1, 2, 3, 4, 5)
N_DP = 4
DR = 160
N_DT = 5
N_DD = 2
N_DN = FROWS // DR
LAYERS = 2
MB = 256
NB = TOK // MB
SCALE = HEAD ** -0.5

RATE = {"X": 46600.0, "Y": 46600.0, "D": 500000.0, "L": 800000.0}
LAT = {"X": 2.5, "Y": 2.5, "D": 1.5, "L": 1.0}
HORIZON = 18.0
T_TABLES, T_WIDEN, T_NORM, T_QKV, T_HEAD, T_PROJ, T_TILE, T_ADD = 3.0, 1.6, 0.4, 2.2, 2.3, 1.1, 7.6, 1.7
OWN_FIRST = 3
P_AFTER = {3: [("h ready", 1, 1)]}
L1_ORDER = (("own", 0, 1), "lo", "hi", ("own", 1, 5), "dp")
GROUPS = {"c0": (0,), "c1": (1,), "lo": (0, 1), "hi": (2, 3), "c123": (1, 2, 3)}
TOKEN_ORDER = [(c, l, i) for c, l in (("h", 0), ("p", 0), ("h", 1), ("p", 1)) for i in range(NB)]
N_SEM = 226
T_LOAD = 2.8
FB = 128


class Transfer:
    def __init__(self, key, link, size, n_sem, start, wait, done, deps):
        self.key, self.link, self.size, self.n_sem = key, link, size, n_sem
        self.start, self.wait, self.done, self.deps = start, wait, done, set(deps)
        self.sems = []


class Planner:
    def __init__(self):
        self.now = 0.0
        self.free = dict.fromkeys("XYDL", 0.0)
        self.all, self.queue, self.users, self.mates = {}, {"X": [], "Y": []}, {}, {}
        self.pool = list(range(N_SEM))
        self.issued, self.arrived, self.flying, self.sent, self.ops = set(), set(), [], [], []

    def add(self, tr):
        self.all[tr.key] = tr
        for dep in tr.deps:
            self.users.setdefault(dep, []).append(tr.key)

    def issue(self, key):
        tr = self.all[key]
        self.issued.add(key)
        tr.sems, self.pool = self.pool[:tr.n_sem], self.pool[tr.n_sem:]
        self.ops.append(tr.start)
        self.free[tr.link] = max(self.free[tr.link], self.now) + tr.size / RATE[tr.link]
        self.flying.append((self.free[tr.link] + LAT[tr.link], key))
        for mate in self.mates.get(key, ()):
            if mate not in self.issued and self.all[mate].deps <= self.arrived:
                self.issue(mate)

    def mark(self, key):
        self.arrived.add(key)
        for user in self.users.get(key, ()):
            tr = self.all[user]
            if tr.link in "DL" and user not in self.issued and tr.deps <= self.arrived:
                self.issue(user)

    def receive(self, item):
        self.flying.remove(item)
        tr = self.all[item[1]]
        self.ops.append(tr.wait)
        if tr.done is not None:
            self.sent.append((item[0] + 2.0, item[1]))
        else:
            self.pool += tr.sems
        self.mark(item[1])

    def fill(self):
        for link in "XY":
            while self.free[link] - self.now < HORIZON:
                ready = [k for k in self.queue[link] if self.all[k].deps <= self.arrived]
                if not ready:
                    break
                self.queue[link].remove(ready[0])
                self.issue(ready[0])

    def retire(self, keys=None, everything=False):
        for item in list(self.sent):
            if everything or (keys is not None and item[1] in keys) or (keys is None and item[0] <= self.now):
                self.sent.remove(item)
                self.ops.append(self.all[item[1]].done)
                self.pool += self.all[item[1]].sems

    def service(self):
        while True:
            due = sorted(i for i in self.flying if i[0] <= self.now)
            if not due:
                break
            self.receive(due[0])
            self.fill()
        self.fill()
        self.retire()

    def need(self, keys):
        keys = set(keys)
        while not keys <= self.arrived:
            self.fill()
            item = min(self.flying)
            self.now = max(self.now, item[0])
            self.receive(item)
        self.service()

    def spend(self, us):
        self.now += us

    def take(self):
        ops, self.ops = self.ops, []
        return ops


def run(ops):
    for op in ops:
        op()


def run_at(index, table):
    for k, ops in (table.items() if isinstance(table, dict) else enumerate(table)):
        if ops:
            pl.when(index == k)(lambda ops=ops: run(ops))


def kernel(tok, seg_r, freq, g_attn, g_mlp, w_q, w_k, w_v, w_o, w_g, w_u, w_d,
           out, f_r, f_q, f_k, f_v, f_o, f_g, f_u, f_d, f_p,
           x, h, q, k, v, o, cos_t, sin_t, mask, vq, vk, vv, vo, vg, vu, vd,
           b_q, b_k, b_v, b_o, b_g, b_u, b_d,
           send, recv, ld, tl):
    me = lax.axis_index("fsdp")
    core = lax.rem(me, 2)
    xc = lax.rem(me // 2, 2)
    yc = me // 4
    xn = me + 2 - 4 * xc
    yn = me + 4 - 8 * yc
    cn = me + 1 - 2 * core
    dg = xn + 4 - 8 * yc

    barrier = pltpu.get_barrier_semaphore()
    for nb in (xn, yn, cn):
        pl.semaphore_signal(barrier, inc=1, device_id={"fsdp": nb}, device_id_type=MESH)
    pl.semaphore_wait(barrier, 3)

    plan = Planner()

    def al(i, n):
        return i if isinstance(i, int) else pl.multiple_of(i, n)

    def view(ref, l, r0, nr, c0, nc):
        return ref.at[l, pl.ds(al(r0, 16), nr), pl.ds(al(c0, 128), nc)]

    def remote(key, link, pairs, dev, deps):
        sizes = [n for n, _ in pairs]

        def each():
            for i, (_, make) in zip(plan.all[key].sems, pairs):
                src, dst = make()
                yield pltpu.make_async_remote_copy(src_ref=src, dst_ref=dst, send_sem=send.at[i], recv_sem=recv.at[i],
                                                   device_id={"fsdp": dev}, device_id_type=MESH)

        plan.add(Transfer(key, link, sum(sizes), len(pairs), lambda: [c.start() for c in each()], lambda: [c.wait_recv() for c in each()],
                          lambda: [c.wait_send() for c in each()], deps))

    def local(key, pairs, deps):
        sizes = [n for n, _ in pairs]

        def each():
            for i, (_, make) in zip(plan.all[key].sems, pairs):
                src, dst = make()
                yield pltpu.make_async_copy(src, dst, send.at[i])

        plan.add(Transfer(key, "L", sum(sizes), len(pairs), lambda: [c.start() for c in each()], lambda: [c.wait() for c in each()], None, deps))

    def block(src, dst, l, col, other_col, nc, stage):
        def at(dev, other=False):
            return view(dst, l, dev * ROWS, ROWS, other_col if other else col, nc)

        def part(dev, p):
            return view(dst, l, dev * ROWS + (ROWS // 2) * p, ROWS // 2, col, nc)
        return (2 * ROWS * nc, lambda other=False: view(src, l, 0, ROWS, other_col if other else col, nc), at, stage)

    def down_block(l, j, stage):
        return (2 * DR * D, lambda other=False: view(w_d, l, j * DR, DR, 0, D), lambda dev, other=False: view(f_d, l, dev * FROWS + j * DR, DR, 0, D), stage)

    def shared_block(row_of):
        at = lambda dev, other=False: view(f_d, 1, row_of(dev), DR, 0, D)
        return (2 * DR * D, lambda other=False: at(me), at, None)

    def place(dev):
        return dev // 4, lax.rem(dev // 2, 2), lax.rem(dev, 2)

    def tp_row(j):
        def row(dev):
            yy, xx, cc = place(dev)
            return yy * HALF + xx * (2 * FROWS) + TF * (1 - xx) + (N_DT * DR) * cc + j * DR
        return row

    def dp_row(j):
        def row(dev):
            yy, xx, cc = place(dev)
            return yy * HALF + xx * (2 * FROWS) + (2 * FROWS - TF) * xx + (N_DD * DR) * cc + j * DR
        return row

    def add_round(rd, mats, parts, deps=(), before=None):
        K = lambda t: (rd, t)

        def own(other=False):
            return [(m[0], lambda m=m: (m[1](other), m[2](me, other))) for m in mats]

        def held(dev):
            return [(m[0], lambda m=m: (m[2](dev), m[2](dev))) for m in mats]

        for t in parts:
            if t == "X":
                remote(K(t), "X", own(), xn, deps)
            elif t == "Y":
                remote(K(t), "Y", own(other=True), yn, deps)
            elif t == "D":
                remote(K(t), "D", own(), cn, [])
            elif t == "XR":
                remote(K(t), "X", held(yn), xn, [K("Y")])
            elif t == "DX":
                remote(K(t), "D", held(xn), cn, [K("X")])
            elif t == "DY":
                remote(K(t), "D", held(yn), cn, [K("Y")])
            elif t == "DR":
                remote(K(t), "D", held(dg), cn, [K("XR")])
            elif t == "bin":
                local(K(t), [(m[0], lambda m=m: (m[1](), m[3])) for m in mats], [before] if before else [])
            else:
                local(K(t), [(m[0], lambda m=m: (m[3], m[2](me))) for m in mats], [K("bin")])
        if "D" in parts and "X" in parts:
            plan.mates[K("X")] = [K("D"), K("bin")]
        needs[rd] = [K(t) for t in parts]

    needs = {}
    FULL = ("X", "Y", "D", "XR", "DX", "DY", "DR", "bin", "bout")
    for l in (0, 1):
        add_round(("qkv", l), [block(w_q, f_q, l, 0, 0, D, b_q), block(w_k, f_k, l, 0, 0, KV, b_k), block(w_v, f_v, l, 0, 0, KV, b_v)], FULL,
                  before=(("qkv", 0), "bout") if l else None)
        add_round(("o", l), [block(w_o, f_o, l, 0, 0, D, b_o)], FULL, before=(("o", 0), "bout") if l else None)
    dn_seq = [("dn", l, j) for l in (0, 1) for j in range(N_DN)]
    for n, rd in enumerate(dn_seq):
        add_round(rd, [down_block(rd[1], rd[2], b_d.at[n % 4])], ("X", "D", "DX", "bin", "bout") if rd[1] == 0 else ("D", "bin", "bout"),
                  before=(dn_seq[n - 4], "bout") if n >= 4 else None)
    dn1 = [key for j in range(N_DN) for key in needs[("dn", 1, j)]]
    for j in range(N_DT):
        add_round(("dt", j), [shared_block(tp_row(j))], ("X", "DX"), deps=dn1)
    for j in range(N_DD):
        add_round(("dd", j), [shared_block(dp_row(j))], ("X", "Y", "XR", "DX", "DY", "DR"), deps=dn1)
    gu_seq = [("gu", j) for j in range(N_G0)] + [("gt", j) for j in TP_TILES] + [("gd", j) for j in range(N_DP)]
    for n, rd in enumerate(gu_seq):
        kind, j = rd
        l = 0 if kind == "gu" else 1
        if kind == "gd":
            col = (j % 2) * HALF + (j // 2) * (HALF - TF)
            other = col
        else:
            col, other = yc * HALF + j * TF, (1 - yc) * HALF + j * TF
        add_round(rd, [block(w_g, f_g, l, col, other, TF, b_g.at[n % 4]), block(w_u, f_u, l, col, other, TF, b_u.at[n % 4])], FULL,
                  before=(gu_seq[n - 4], "bout") if n >= 4 else None)
    for j in range(N_DN):
        plan.mates[(("gu", j), "X")] += [(("dn", 1, j), "D"), (("dn", 1, j), "bin")]
    for i in range(NB):
        mine, theirs = pl.ds(i * MB, MB), pl.ds(TOK + i * MB, MB)
        for l, land in ((0, f_p), (1, f_r)):
            remote(("h", l, i), "Y", [(2 * MB * D, lambda mine=mine, theirs=theirs: (h.at[mine, :], h.at[theirs, :]))], yn, [("h ready", l, i)])
            remote(("p", l, i), "Y", [(4 * MB * D, lambda mine=mine, theirs=theirs, land=land: (x.at[theirs, :], land.at[mine, :]))], yn, [("p ready", l, i)] + (P_AFTER.get(i, []) if l == 0 else []))

    def seq(rds, *ts):
        return [(rd, t) for rd in rds for t in ts]

    attn = lambda l: [("qkv", l), ("o", l)]
    gus, gts, gds = [("gu", j) for j in range(N_G0)], [("gt", j) for j in TP_TILES], [("gd", j) for j in range(N_DP)]
    dts, dds = [("dt", j) for j in range(N_DT)], [("dd", j) for j in range(N_DD)]
    plan.queue["X"] = (seq(attn(0), "X") + seq(attn(0), "XR") + seq(dn_seq[:N_DN], "X") + seq(gus, "X", "XR")
                       + seq(attn(1), "X") + seq(attn(1), "XR") + seq(dts, "X") + seq(gts, "X", "XR") + seq(dds, "X", "XR") + seq(gds, "X", "XR"))
    plan.queue["Y"] = TOKEN_ORDER + seq(attn(0), "Y") + seq(gus, "Y") + seq(attn(1), "Y") + seq(gts, "Y") + seq(dds, "Y") + seq(gds, "Y")

    def rows_of(i):
        return pl.ds(i * MB if isinstance(i, int) else pl.multiple_of(i * MB, MB), MB)

    def load(pairs):
        cps = [pltpu.make_async_copy(s, d, ld.at[i]) for i, (s, d) in enumerate(pairs)]
        for c in cps:
            c.start()
        for c in cps:
            c.wait()

    plan.service()
    run(plan.take())
    tok_in = pltpu.make_async_copy(tok, o, ld.at[0])
    tok_in.start()

    def tables(i, c):
        rows = rows_of(i)
        rr = lax.broadcasted_iota(jnp.int32, (MB, TOK), 0) + i * MB
        cc = lax.broadcasted_iota(jnp.int32, (MB, TOK), 1)
        seg = jnp.broadcast_to(seg_r[...], (MB, TOK)).astype(jnp.float32)
        seg_c = jnp.sum(jnp.where(cc == rr, seg, 0.0), axis=1, keepdims=True)
        ok = jnp.where((seg == seg_c) & (cc <= rr), 1.0, 0.0)
        mask[rows, :] = ok
        pos = jnp.sum(ok, axis=1, keepdims=True) - 1.0
        ang = pos * freq[...]
        lane = lax.broadcasted_iota(jnp.int32, (MB, HEAD), 1)
        cos_t[rows, :] = jnp.cos(ang)
        sn = jnp.sin(ang)
        sin_t[rows, :] = jnp.where(lane < HEAD // 2, -sn, sn)
        return c

    lax.fori_loop(0, NB, tables, 0)
    plan.spend(T_TABLES)
    plan.service()
    run(plan.take())
    tok_in.wait()

    def widen(i, c):
        rows = rows_of(i)
        x[rows, :] = o[rows, :].astype(jnp.float32)
        x[rows_of(i + NB), :] = jnp.zeros((MB, D), jnp.float32)
        return c

    lax.fori_loop(0, NB, widen, 0)
    plan.spend(T_WIDEN)

    def norm_row(gain_ref, l, i):
        rows = rows_of(i)
        xv = x[rows, :]
        inv = lax.rsqrt(jnp.mean(xv * xv, axis=-1, keepdims=True) + EPS)
        h[rows, :] = (xv * inv * gain_ref[l:l + 1, :].astype(jnp.float32)).astype(jnp.bfloat16)

    def rope(val, rows):
        f = val.astype(jnp.bfloat16).astype(jnp.float32)
        return (f * cos_t[rows, :] + pltpu.roll(f, HEAD // 2, 1) * sin_t[rows, :]).astype(jnp.bfloat16)

    def qkv_row(i):
        rows = rows_of(i)
        hv = h[rows, :]
        for g in range(HEADS // 4):
            val = jnp.dot(hv, vq[:, g * 512:(g + 1) * 512], preferred_element_type=jnp.float32)
            for e in range(4):
                q[rows, g * 512 + e * HEAD:g * 512 + (e + 1) * HEAD] = rope(val[:, e * HEAD:(e + 1) * HEAD], rows)
        val = jnp.dot(hv, vk[...], preferred_element_type=jnp.float32)
        for e in range(KV_HEADS):
            k[rows, e * HEAD:(e + 1) * HEAD] = rope(val[:, e * HEAD:(e + 1) * HEAD], rows)
        v[rows, :] = jnp.dot(hv, vv[...], preferred_element_type=jnp.float32).astype(jnp.bfloat16)

    def one_head(hd, blocks):
        qc = pl.ds(pl.multiple_of(hd * HEAD, HEAD), HEAD)
        kc = pl.ds(pl.multiple_of((hd // (HEADS // KV_HEADS)) * HEAD, HEAD), HEAD)
        for i in blocks:
            n = (i + 1) * MB
            s = lax.dot_general(q[i * MB:n, qc], k[0:n, kc], (((1,), (1,)), ((), ())), preferred_element_type=jnp.float32) * SCALE
            s = jnp.where(mask[i * MB:n, 0:n] > 0.5, s, -1e30)
            e = jnp.exp(s - jnp.max(s, axis=1, keepdims=True))
            p = (e / jnp.sum(e, axis=1, keepdims=True)).astype(jnp.bfloat16)
            o[i * MB:n, qc] = jnp.dot(p, v[0:n, kc], preferred_element_type=jnp.float32).astype(jnp.bfloat16)

    def mlp_row(i, slot, c):
        rows = rows_of(i)
        hv = h[rows, :]
        gt = jnp.dot(hv, vg[slot], preferred_element_type=jnp.float32)
        up = jnp.dot(hv, vu[slot], preferred_element_type=jnp.float32)
        a = (gt * jax.nn.sigmoid(gt) * up).astype(jnp.bfloat16)
        x[rows, :] += jnp.dot(a, vd[slot], preferred_element_type=jnp.float32)
        return c

    def get_qkv(l):
        plan.need(needs[("qkv", l)])
        run(plan.take())
        load([(f_q.at[l], vq), (f_k.at[l], vk), (f_v.at[l], vv)])
        plan.spend(3.0)

    def get_o(l):
        plan.need(needs[("o", l)])
        run(plan.take())
        load([(f_o.at[l], vo)])
        plan.spend(2.0)

    def heads(blocks):
        table = []
        for i in range(HEADS):
            if i % 2 == 0 or len(blocks) == NB:
                plan.service()
            table.append(plan.take())
            plan.spend(T_HEAD * sum(b + 1 for b in blocks) / 10)

        def head_step(hd, c):
            run_at(hd, table)
            one_head(hd, blocks)
            return c

        lax.fori_loop(0, HEADS, head_step, 0)

    def proj_row(l, i):
        rows = rows_of(i)
        x[rows, :] += jnp.dot(o[rows, :], vo[...], preferred_element_type=jnp.float32)
        norm_row(g_mlp, l, i)

    def tiles(l, steps, offset, first, n_rows, marks=None):
        pre, post, ahead = {}, {}, {}
        early = False
        for n, (t, keys) in enumerate(steps):
            for key in (marks or {}).get((n, "pre"), ()):
                plan.mark(key)
            plan.need(keys)
            pre[t] = plan.take()
            if not early:
                pre[t].append(lambda t=t: [c.start() for c in tile_loads(l, offset(t), t % 2)])
                plan.spend(T_LOAD)
            for key in (marks or {}).get((n, "post"), ()):
                plan.mark(key)
            plan.service()
            post[t] = plan.take()
            early = n + 1 < len(steps) and set(steps[n + 1][1]) <= plan.arrived
            if early:
                post[t].append(lambda t=t: [c.start() for c in tile_loads(l, offset(t + 1), (t + 1) % 2)])
            plan.spend(T_TILE * n_rows / NB)

        def body(t, c):
            slot = lax.rem(t, 2)
            run_at(t, pre)
            for cp in tile_loads(l, offset(t), slot):
                cp.wait()
            run_at(t, post)
            lax.fori_loop(first, first + n_rows, lambda i, c: mlp_row(i, slot, c), 0)
            return c

        lax.fori_loop(steps[0][0], steps[-1][0] + 1, body, 0)

    def tile_loads(l, off, slot):
        cols = pl.ds(al(off, 128), TF)
        return [pltpu.make_async_copy(f_g.at[l, :, cols], vg.at[slot], tl.at[slot, 0]), pltpu.make_async_copy(f_u.at[l, :, cols], vu.at[slot], tl.at[slot, 1]),
                pltpu.make_async_copy(f_d.at[l, cols, :], vd.at[slot], tl.at[slot, 2])]

    get_qkv(0)
    table_q = []
    for i in range(NB):
        plan.service()
        table_q.append(plan.take())
        plan.spend(T_QKV + T_NORM)

    def qkv_step(i, c):
        run_at(i, table_q)
        norm_row(g_attn, 0, i)
        qkv_row(i)
        return c

    lax.fori_loop(0, NB, qkv_step, 0)
    heads(range(NB))
    get_o(0)
    table_o = []
    for i in range(NB):
        plan.service()
        if i >= 2:
            plan.mark(("h ready", 0, i - 2))
            plan.fill()
        table_o.append(plan.take())
        plan.spend(T_PROJ + T_NORM)

    def proj_step(i, c):
        run_at(i, table_o)
        proj_row(0, i)
        return c

    lax.fori_loop(0, NB, proj_step, 0)

    dn0 = [key for j in range(N_DN) for key in needs[("dn", 0, j)]]
    half_off = lambda t: yc * HALF + t * TF
    steps = [(j, needs[("gu", j)] + dn0) for j in range(N_G0)]
    got_h = lambda l, *chunks: [("h", l, i) for i in chunks]
    tiles(0, steps[:OWN_FIRST], half_off, 0, NB, {(0, "pre"): [("h ready", 0, NB - 2)], (0, "post"): [("h ready", 0, NB - 1)]})
    tiles(0, [(j, keys + got_h(0, *range(NB))) for j, keys in steps], half_off, NB, NB)
    tiles(0, steps[OWN_FIRST:], half_off, 0, NB, {(0, "post"): [("p ready", 0, i) for i in range(NB)]})

    get_qkv(1)
    for i in range(NB):
        plan.need([("p", 0, i)])
        plan.retire(keys=[("p", 0, i)])
        run(plan.take())
        load([(f_p.at[rows_of(i), :], x.at[rows_of(i + NB), :])])
        x[rows_of(i), :] += x[rows_of(i + NB), :]
        norm_row(g_attn, 1, i)
        qkv_row(i)
        plan.spend(T_QKV + T_NORM + T_ADD)
        heads([i])
        if i == 0:
            get_o(1)
        proj_row(1, i)
        x[rows_of(i + NB), :] = jnp.zeros((MB, D), jnp.float32)
        plan.spend(T_PROJ + T_NORM + 0.4)
        plan.mark(("h ready", 1, i))
        plan.service()
        run(plan.take())

    dt1 = dn1 + [key for j in range(N_DT) for key in needs[("dt", j)]]
    dd1 = dn1 + [key for j in range(N_DD) for key in needs[("dd", j)]]
    steps = [(j, needs[("gt", j)] + dt1) for j in TP_TILES]
    h_mark = {}
    run_order = L1_ORDER
    marks = {}
    for n, what in enumerate(run_order):
        if what[0] == "own":
            tiles(1, steps[what[1]:what[2]], half_off, 0, NB, {**h_mark, **marks})
            marks, h_mark = {}, {}
        elif what in GROUPS:
            chunks = GROUPS[what]
            tiles(1, [(j, keys + got_h(1, *chunks)) for j, keys in steps], half_off, NB + chunks[0], len(chunks), {**h_mark, **marks})
            marks, h_mark = {(0, "pre"): [("p ready", 1, i) for i in chunks[:-1]], (0, "post"): [("p ready", 1, chunks[-1])]}, {}
        else:
            tiles(1, [(j, needs[("gd", j)] + dd1) for j in range(N_DP)],
                  lambda t: (t % 2) * HALF + (t // 2) * (HALF - TF) if isinstance(t, int) else lax.rem(t, 2) * HALF + lax.div(t, 2) * (HALF - TF), 0, NB, {**h_mark, **marks})
            marks, h_mark = {}, {}

    for i in range(NB - 1):
        plan.need([("p", 1, i)])
        plan.retire(keys=[("p", 1, i)])
        run(plan.take())
        load([(f_r.at[rows_of(i), :], x.at[rows_of(i + NB), :])])
        x[rows_of(i), :] += x[rows_of(i + NB), :]
        plan.spend(T_ADD)
    plan.service()
    done = pltpu.make_async_copy(x.at[pl.ds(0, TOK), :], out, ld.at[0])
    done.start()
    plan.need(plan.all)
    plan.retire(everything=True)
    run(plan.take())
    done.wait()


def finish(x_in, r_in, out, xv, rv, sem):
    n = TOK // FB
    first = (NB - 1) * MB // FB
    rows = [pl.ds(i * FB, FB) for i in range(n)]
    order = list(range(first, n)) + list(range(first))
    got = {i: pltpu.make_async_copy(x_in.at[rows[i], :], xv.at[rows[i], :], sem.at[0, i]) for i in range(n)}
    ret = {i: pltpu.make_async_copy(r_in.at[rows[i], :], rv.at[pl.ds((i - first) * FB, FB), :], sem.at[1, i]) for i in range(first, n)}
    put = {i: pltpu.make_async_copy(xv.at[rows[i], :], out.at[rows[i], :], sem.at[2, i]) for i in range(n)}
    for i in order:
        if i in ret:
            ret[i].start()
        got[i].start()
    for i in range(first, n):
        ret[i].wait()
        got[i].wait()
        xv[rows[i], :] += rv[pl.ds((i - first) * FB, FB), :]
    for i in range(first):
        got[i].wait()
        put[i].start()
    for i in range(first, n):
        put[i].start()
    for i in range(n):
        put[i].wait()


def solution(mesh):
    tok_spec = P(("rep", "fsdp"), None)
    seg_spec = P(("rep", "fsdp"))
    mat_spec = P(None, "fsdp", None)
    gain_spec = P(None, None)
    bf, f32 = jnp.bfloat16, jnp.float32

    def per_device(tokens, seg_ids, w_q, w_k, w_v, w_o, w_gate, w_up, w_down, g_attn, g_mlp):
        half = HEAD // 2
        inv = np.float32(ROPE_BASE) ** (-np.arange(half, dtype=np.float32) / np.float32(half))
        freq = jnp.asarray(np.concatenate([inv, inv]).reshape(1, HEAD), f32)
        any_s = pl.BlockSpec(memory_space=pl.ANY)
        vm = pl.BlockSpec(memory_space=pltpu.VMEM)
        full = [(LAYERS, D, D), (LAYERS, D, KV), (LAYERS, D, KV), (LAYERS, D, D), (LAYERS, D, FF), (LAYERS, D, FF), (LAYERS, FF, D)]
        res = pl.pallas_call(
            kernel,
            out_shape=[jax.ShapeDtypeStruct((TOK, D), f32)] * 2 + [jax.ShapeDtypeStruct(s, bf) for s in full] + [jax.ShapeDtypeStruct((TOK, D), f32)],
            in_specs=[any_s, vm, vm, vm, vm] + [any_s] * 7,
            out_specs=[any_s] * 10,
            scratch_shapes=[
                pltpu.VMEM((2 * TOK, D), f32), pltpu.VMEM((2 * TOK, D), bf), pltpu.VMEM((TOK, D), bf),
                pltpu.VMEM((TOK, KV), bf), pltpu.VMEM((TOK, KV), bf), pltpu.VMEM((TOK, D), bf),
                pltpu.VMEM((TOK, HEAD), f32), pltpu.VMEM((TOK, HEAD), f32), pltpu.VMEM((TOK, TOK), f32),
                pltpu.VMEM((D, D), bf), pltpu.VMEM((D, KV), bf), pltpu.VMEM((D, KV), bf), pltpu.VMEM((D, D), bf),
                pltpu.VMEM((2, D, TF), bf), pltpu.VMEM((2, D, TF), bf), pltpu.VMEM((2, TF, D), bf),
                pltpu.VMEM((ROWS, D), bf), pltpu.VMEM((ROWS, KV), bf), pltpu.VMEM((ROWS, KV), bf), pltpu.VMEM((ROWS, D), bf),
                pltpu.VMEM((4, ROWS, TF), bf), pltpu.VMEM((4, ROWS, TF), bf), pltpu.VMEM((4, DR, D), bf),
                pltpu.SemaphoreType.DMA((N_SEM,)), pltpu.SemaphoreType.DMA((N_SEM,)), pltpu.SemaphoreType.DMA((4,)), pltpu.SemaphoreType.DMA((2, 3)),
            ],
            compiler_params=pltpu.CompilerParams(collective_id=0, has_side_effects=True, vmem_limit_bytes=66 * 1000 * 1000),
        )(tokens, seg_ids.reshape(1, TOK), freq, g_attn, g_mlp, w_q, w_k, w_v, w_o, w_gate, w_up, w_down)
        return pl.pallas_call(
            finish,
            out_shape=jax.ShapeDtypeStruct((TOK, D), f32),
            in_specs=[any_s, any_s],
            out_specs=any_s,
            scratch_shapes=[pltpu.VMEM((TOK, D), f32), pltpu.VMEM((MB, D), f32), pltpu.SemaphoreType.DMA((3, TOK // FB))],
            compiler_params=pltpu.CompilerParams(vmem_limit_bytes=66 * 1000 * 1000),
        )(res[0], res[1])

    return jax.shard_map(per_device, mesh=mesh, in_specs=(tok_spec, seg_spec, mat_spec, mat_spec, mat_spec, mat_spec, mat_spec, mat_spec, mat_spec, gain_spec, gain_spec), out_specs=tok_spec, check_vma=False)
```

```python
import jax
import jax.numpy as jnp
import numpy as np
from jax import lax
from jax.experimental import pallas as pl
from jax.experimental.pallas import tpu as pltpu
from jax.sharding import PartitionSpec as P

HEAD = 128
HEADS = 12
KV_HEADS = 2
EPS = 1e-5
ROPE_BASE = 10000.0
MESH = pl.DeviceIdType.MESH

N_DEV = 8
TOK = 1024
D = 1536
KV = KV_HEADS * HEAD
FF = 8960
HALF = FF // 2
ROWS = D // N_DEV
FROWS = FF // N_DEV
TF = 640
N_G0 = HALF // TF
TP_TILES = (1, 2, 3, 4, 5)
N_DP = 4
DR = 160
N_DT = 5
N_DD = 2
N_DN = FROWS // DR
LAYERS = 2
MB = 256
NB = TOK // MB
SCALE = HEAD ** -0.5

RATE = {"X": 46600.0, "Y": 46600.0, "D": 500000.0, "L": 800000.0}
LAT = {"X": 2.5, "Y": 2.5, "D": 1.5, "L": 1.0}
HORIZON = 20.0
T_TABLES, T_WIDEN, T_NORM, T_QKV, T_HEAD, T_PROJ, T_TILE, T_ADD = 3.0, 1.6, 0.4, 1.8, 2.0, 1.1, 7.0, 1.7
OWN_FIRST = 3
P_AFTER = {3: [("h ready", 1, 1)]}
L1_ORDER = (("own", 0, 2), "lo", "hi", ("own", 2, 5), "dp")
GROUPS = {"c0": (0,), "c1": (1,), "lo": (0, 1), "hi": (2, 3), "c123": (1, 2, 3)}
TOKEN_ORDER = [(c, l, i) for c, l in (("h", 0), ("p", 0), ("h", 1), ("p", 1)) for i in range(NB)]
N_SEM = 226
T_LOAD = 2.4
FB = 64


class Transfer:
    def __init__(self, key, link, size, n_sem, start, wait, done, deps):
        self.key, self.link, self.size, self.n_sem = key, link, size, n_sem
        self.start, self.wait, self.done, self.deps = start, wait, done, set(deps)
        self.sems = []


class Planner:
    def __init__(self):
        self.now = 0.0
        self.free = dict.fromkeys("XYDL", 0.0)
        self.all, self.queue, self.users, self.mates = {}, {"X": [], "Y": []}, {}, {}
        self.pool = list(range(N_SEM))
        self.issued, self.arrived, self.flying, self.sent, self.ops = set(), set(), [], [], []

    def add(self, tr):
        self.all[tr.key] = tr
        for dep in tr.deps:
            self.users.setdefault(dep, []).append(tr.key)

    def issue(self, key):
        tr = self.all[key]
        self.issued.add(key)
        tr.sems, self.pool = self.pool[:tr.n_sem], self.pool[tr.n_sem:]
        self.ops.append(tr.start)
        self.free[tr.link] = max(self.free[tr.link], self.now) + tr.size / RATE[tr.link]
        self.flying.append((self.free[tr.link] + LAT[tr.link], key))
        for mate in self.mates.get(key, ()):
            if mate not in self.issued and self.all[mate].deps <= self.arrived:
                self.issue(mate)

    def mark(self, key):
        self.arrived.add(key)
        for user in self.users.get(key, ()):
            tr = self.all[user]
            if tr.link in "DL" and user not in self.issued and tr.deps <= self.arrived:
                self.issue(user)

    def receive(self, item):
        self.flying.remove(item)
        tr = self.all[item[1]]
        self.ops.append(tr.wait)
        if tr.done is not None:
            self.sent.append((item[0] + 2.0, item[1]))
        else:
            self.pool += tr.sems
        self.mark(item[1])

    def fill(self):
        for link in "XY":
            while self.free[link] - self.now < HORIZON:
                ready = [k for k in self.queue[link] if self.all[k].deps <= self.arrived]
                if not ready:
                    break
                self.queue[link].remove(ready[0])
                self.issue(ready[0])

    def retire(self, keys=None, everything=False):
        for item in list(self.sent):
            if everything or (keys is not None and item[1] in keys) or (keys is None and item[0] <= self.now):
                self.sent.remove(item)
                self.ops.append(self.all[item[1]].done)
                self.pool += self.all[item[1]].sems

    def service(self):
        while True:
            due = sorted(i for i in self.flying if i[0] <= self.now)
            if not due:
                break
            self.receive(due[0])
            self.fill()
        self.fill()
        self.retire()

    def need(self, keys):
        keys = set(keys)
        while not keys <= self.arrived:
            self.fill()
            item = min(self.flying)
            self.now = max(self.now, item[0])
            self.receive(item)
        self.service()

    def spend(self, us):
        self.now += us

    def take(self):
        ops, self.ops = self.ops, []
        return ops


def run(ops):
    for op in ops:
        op()


def run_at(index, table):
    for k, ops in (table.items() if isinstance(table, dict) else enumerate(table)):
        if ops:
            pl.when(index == k)(lambda ops=ops: run(ops))


def kernel(tok, seg_r, freq, g_attn, g_mlp, w_q, w_k, w_v, w_o, w_g, w_u, w_d,
           out, f_r, f_q, f_k, f_v, f_o, f_g, f_u, f_d, f_p,
           x, h, q, k, v, o, cos_t, sin_t, mask, vq, vk, vv, vo, vg, vu, vd,
           b_q, b_k, b_v, b_o, b_g, b_u, b_d,
           send, recv, ld, tl):
    me = lax.axis_index("fsdp")
    core = lax.rem(me, 2)
    xc = lax.rem(me // 2, 2)
    yc = me // 4
    xn = me + 2 - 4 * xc
    yn = me + 4 - 8 * yc
    cn = me + 1 - 2 * core
    dg = xn + 4 - 8 * yc

    barrier = pltpu.get_barrier_semaphore()
    for nb in (xn, yn, cn):
        pl.semaphore_signal(barrier, inc=1, device_id={"fsdp": nb}, device_id_type=MESH)
    pl.semaphore_wait(barrier, 3)

    plan = Planner()

    def al(i, n):
        return i if isinstance(i, int) else pl.multiple_of(i, n)

    def view(ref, l, r0, nr, c0, nc):
        return ref.at[l, pl.ds(al(r0, 16), nr), pl.ds(al(c0, 128), nc)]

    def remote(key, link, pairs, dev, deps):
        sizes = [n for n, _ in pairs]

        def each():
            for i, (_, make) in zip(plan.all[key].sems, pairs):
                src, dst = make()
                yield pltpu.make_async_remote_copy(src_ref=src, dst_ref=dst, send_sem=send.at[i], recv_sem=recv.at[i],
                                                   device_id={"fsdp": dev}, device_id_type=MESH)

        plan.add(Transfer(key, link, sum(sizes), len(pairs), lambda: [c.start() for c in each()], lambda: [c.wait_recv() for c in each()],
                          lambda: [c.wait_send() for c in each()], deps))

    def local(key, pairs, deps):
        sizes = [n for n, _ in pairs]

        def each():
            for i, (_, make) in zip(plan.all[key].sems, pairs):
                src, dst = make()
                yield pltpu.make_async_copy(src, dst, send.at[i])

        plan.add(Transfer(key, "L", sum(sizes), len(pairs), lambda: [c.start() for c in each()], lambda: [c.wait() for c in each()], None, deps))

    def block(src, dst, l, col, other_col, nc, stage):
        def at(dev, other=False):
            return view(dst, l, dev * ROWS, ROWS, other_col if other else col, nc)

        def part(dev, p):
            return view(dst, l, dev * ROWS + (ROWS // 2) * p, ROWS // 2, col, nc)
        return (2 * ROWS * nc, lambda other=False: view(src, l, 0, ROWS, other_col if other else col, nc), at, stage)

    def down_block(l, j, stage):
        return (2 * DR * D, lambda other=False: view(w_d, l, j * DR, DR, 0, D), lambda dev, other=False: view(f_d, l, dev * FROWS + j * DR, DR, 0, D), stage)

    def shared_block(row_of):
        at = lambda dev, other=False: view(f_d, 1, row_of(dev), DR, 0, D)
        return (2 * DR * D, lambda other=False: at(me), at, None)

    def place(dev):
        return dev // 4, lax.rem(dev // 2, 2), lax.rem(dev, 2)

    def tp_row(j):
        def row(dev):
            yy, xx, cc = place(dev)
            return yy * HALF + xx * (2 * FROWS) + TF * (1 - xx) + (N_DT * DR) * cc + j * DR
        return row

    def dp_row(j):
        def row(dev):
            yy, xx, cc = place(dev)
            return yy * HALF + xx * (2 * FROWS) + (2 * FROWS - TF) * xx + (N_DD * DR) * cc + j * DR
        return row

    def add_round(rd, mats, parts, deps=(), before=None):
        K = lambda t: (rd, t)

        def own(other=False):
            return [(m[0], lambda m=m: (m[1](other), m[2](me, other))) for m in mats]

        def held(dev):
            return [(m[0], lambda m=m: (m[2](dev), m[2](dev))) for m in mats]

        for t in parts:
            if t == "X":
                remote(K(t), "X", own(), xn, deps)
            elif t == "Y":
                remote(K(t), "Y", own(other=True), yn, deps)
            elif t == "D":
                remote(K(t), "D", own(), cn, [])
            elif t == "XR":
                remote(K(t), "X", held(yn), xn, [K("Y")])
            elif t == "DX":
                remote(K(t), "D", held(xn), cn, [K("X")])
            elif t == "DY":
                remote(K(t), "D", held(yn), cn, [K("Y")])
            elif t == "DR":
                remote(K(t), "D", held(dg), cn, [K("XR")])
            elif t == "bin":
                local(K(t), [(m[0], lambda m=m: (m[1](), m[3])) for m in mats], [before] if before else [])
            else:
                local(K(t), [(m[0], lambda m=m: (m[3], m[2](me))) for m in mats], [K("bin")])
        if "D" in parts and "X" in parts:
            plan.mates[K("X")] = [K("D"), K("bin")]
        needs[rd] = [K(t) for t in parts]

    needs = {}
    FULL = ("X", "Y", "D", "XR", "DX", "DY", "DR", "bin", "bout")
    for l in (0, 1):
        add_round(("qkv", l), [block(w_q, f_q, l, 0, 0, D, b_q), block(w_k, f_k, l, 0, 0, KV, b_k), block(w_v, f_v, l, 0, 0, KV, b_v)], FULL,
                  before=(("qkv", 0), "bout") if l else None)
        add_round(("o", l), [block(w_o, f_o, l, 0, 0, D, b_o)], FULL, before=(("o", 0), "bout") if l else None)
    dn_seq = [("dn", l, j) for l in (0, 1) for j in range(N_DN)]
    for n, rd in enumerate(dn_seq):
        add_round(rd, [down_block(rd[1], rd[2], b_d.at[n % 4])], ("X", "D", "DX", "bin", "bout") if rd[1] == 0 else ("D", "bin", "bout"),
                  before=(dn_seq[n - 4], "bout") if n >= 4 else None)
    dn1 = [key for j in range(N_DN) for key in needs[("dn", 1, j)]]
    for j in range(N_DT):
        add_round(("dt", j), [shared_block(tp_row(j))], ("X", "DX"), deps=dn1)
    for j in range(N_DD):
        add_round(("dd", j), [shared_block(dp_row(j))], ("X", "Y", "XR", "DX", "DY", "DR"), deps=dn1)
    gu_seq = [("gu", j) for j in range(N_G0)] + [("gt", j) for j in TP_TILES] + [("gd", j) for j in range(N_DP)]
    for n, rd in enumerate(gu_seq):
        kind, j = rd
        l = 0 if kind == "gu" else 1
        if kind == "gd":
            col = (j % 2) * HALF + (j // 2) * (HALF - TF)
            other = col
        else:
            col, other = yc * HALF + j * TF, (1 - yc) * HALF + j * TF
        add_round(rd, [block(w_g, f_g, l, col, other, TF, b_g.at[n % 4]), block(w_u, f_u, l, col, other, TF, b_u.at[n % 4])], FULL,
                  before=(gu_seq[n - 4], "bout") if n >= 4 else None)
    for j in range(N_DN):
        plan.mates[(("gu", j), "X")] += [(("dn", 1, j), "D"), (("dn", 1, j), "bin")]
    for i in range(NB):
        mine, theirs = pl.ds(i * MB, MB), pl.ds(TOK + i * MB, MB)
        for l, land in ((0, f_p), (1, f_r)):
            remote(("h", l, i), "Y", [(2 * MB * D, lambda mine=mine, theirs=theirs: (h.at[mine, :], h.at[theirs, :]))], yn, [("h ready", l, i)])
            remote(("p", l, i), "Y", [(4 * MB * D, lambda mine=mine, theirs=theirs, land=land: (x.at[theirs, :], land.at[mine, :]))], yn, [("p ready", l, i)] + (P_AFTER.get(i, []) if l == 0 else []))

    def seq(rds, *ts):
        return [(rd, t) for rd in rds for t in ts]

    attn = lambda l: [("qkv", l), ("o", l)]
    gus, gts, gds = [("gu", j) for j in range(N_G0)], [("gt", j) for j in TP_TILES], [("gd", j) for j in range(N_DP)]
    dts, dds = [("dt", j) for j in range(N_DT)], [("dd", j) for j in range(N_DD)]
    plan.queue["X"] = (seq(attn(0), "X") + seq(attn(0), "XR") + seq(dn_seq[:N_DN], "X") + seq(gus, "X", "XR")
                       + seq(attn(1), "X") + seq(attn(1), "XR") + seq(dts, "X") + seq(gts, "X", "XR") + seq(dds, "X", "XR") + seq(gds, "X", "XR"))
    plan.queue["Y"] = TOKEN_ORDER + seq(attn(0), "Y") + seq(gus, "Y") + seq(attn(1), "Y") + seq(gts, "Y") + seq(dds, "Y") + seq(gds, "Y")

    def rows_of(i):
        return pl.ds(i * MB if isinstance(i, int) else pl.multiple_of(i * MB, MB), MB)

    def load(pairs):
        cps = [pltpu.make_async_copy(s, d, ld.at[i]) for i, (s, d) in enumerate(pairs)]
        for c in cps:
            c.start()
        for c in cps:
            c.wait()

    plan.service()
    run(plan.take())
    tok_in = pltpu.make_async_copy(tok, o, ld.at[0])
    tok_in.start()

    def tables(i, c):
        rows = rows_of(i)
        rr = lax.broadcasted_iota(jnp.int32, (MB, TOK), 0) + i * MB
        cc = lax.broadcasted_iota(jnp.int32, (MB, TOK), 1)
        seg = jnp.broadcast_to(seg_r[...], (MB, TOK)).astype(jnp.float32)
        seg_c = jnp.sum(jnp.where(cc == rr, seg, 0.0), axis=1, keepdims=True)
        ok = jnp.where((seg == seg_c) & (cc <= rr), 1.0, 0.0)
        mask[rows, :] = ok
        pos = jnp.sum(ok, axis=1, keepdims=True) - 1.0
        ang = pos * freq[...]
        lane = lax.broadcasted_iota(jnp.int32, (MB, HEAD), 1)
        cos_t[rows, :] = jnp.cos(ang)
        sn = jnp.sin(ang)
        sin_t[rows, :] = jnp.where(lane < HEAD // 2, -sn, sn)
        return c

    lax.fori_loop(0, NB, tables, 0)
    plan.spend(T_TABLES)
    plan.service()
    run(plan.take())
    tok_in.wait()

    def widen(i, c):
        rows = rows_of(i)
        x[rows, :] = o[rows, :].astype(jnp.float32)
        x[rows_of(i + NB), :] = jnp.zeros((MB, D), jnp.float32)
        return c

    lax.fori_loop(0, NB, widen, 0)
    plan.spend(T_WIDEN)

    def norm_row(gain_ref, l, i):
        rows = rows_of(i)
        xv = x[rows, :]
        inv = lax.rsqrt(jnp.mean(xv * xv, axis=-1, keepdims=True) + EPS)
        h[rows, :] = (xv * inv * gain_ref[l:l + 1, :].astype(jnp.float32)).astype(jnp.bfloat16)

    def rope(val, rows):
        f = val.astype(jnp.bfloat16).astype(jnp.float32)
        return (f * cos_t[rows, :] + pltpu.roll(f, HEAD // 2, 1) * sin_t[rows, :]).astype(jnp.bfloat16)

    def qkv_row(i):
        rows = rows_of(i)
        hv = h[rows, :]
        for g in range(HEADS // 4):
            val = jnp.dot(hv, vq[:, g * 512:(g + 1) * 512], preferred_element_type=jnp.float32)
            for e in range(4):
                q[rows, g * 512 + e * HEAD:g * 512 + (e + 1) * HEAD] = rope(val[:, e * HEAD:(e + 1) * HEAD], rows)
        val = jnp.dot(hv, vk[...], preferred_element_type=jnp.float32)
        for e in range(KV_HEADS):
            k[rows, e * HEAD:(e + 1) * HEAD] = rope(val[:, e * HEAD:(e + 1) * HEAD], rows)
        v[rows, :] = jnp.dot(hv, vv[...], preferred_element_type=jnp.float32).astype(jnp.bfloat16)

    def one_head(hd, blocks):
        qc = pl.ds(pl.multiple_of(hd * HEAD, HEAD), HEAD)
        kc = pl.ds(pl.multiple_of((hd // (HEADS // KV_HEADS)) * HEAD, HEAD), HEAD)
        for i in blocks:
            n = (i + 1) * MB
            s = lax.dot_general(q[i * MB:n, qc], k[0:n, kc], (((1,), (1,)), ((), ())), preferred_element_type=jnp.float32) * SCALE
            s = jnp.where(mask[i * MB:n, 0:n] > 0.5, s, -1e30)
            e = jnp.exp(s - jnp.max(s, axis=1, keepdims=True))
            p = (e / jnp.sum(e, axis=1, keepdims=True)).astype(jnp.bfloat16)
            o[i * MB:n, qc] = jnp.dot(p, v[0:n, kc], preferred_element_type=jnp.float32).astype(jnp.bfloat16)

    def mlp_row(i, slot, c):
        rows = rows_of(i)
        hv = h[rows, :]
        gt = jnp.dot(hv, vg[slot], preferred_element_type=jnp.float32)
        up = jnp.dot(hv, vu[slot], preferred_element_type=jnp.float32)
        a = (gt * jax.nn.sigmoid(gt) * up).astype(jnp.bfloat16)
        x[rows, :] += jnp.dot(a, vd[slot], preferred_element_type=jnp.float32)
        return c

    def get_qkv(l):
        plan.need(needs[("qkv", l)])
        run(plan.take())
        load([(f_q.at[l], vq), (f_k.at[l], vk), (f_v.at[l], vv)])
        plan.spend(3.0)

    def get_o(l):
        plan.need(needs[("o", l)])
        run(plan.take())
        load([(f_o.at[l], vo)])
        plan.spend(2.0)

    def heads(blocks):
        table = []
        for i in range(HEADS):
            if i % 2 == 0 or len(blocks) == NB:
                plan.service()
            table.append(plan.take())
            plan.spend(T_HEAD * sum(b + 1 for b in blocks) / 10)

        def head_step(hd, c):
            run_at(hd, table)
            one_head(hd, blocks)
            return c

        lax.fori_loop(0, HEADS, head_step, 0)

    def proj_row(l, i):
        rows = rows_of(i)
        x[rows, :] += jnp.dot(o[rows, :], vo[...], preferred_element_type=jnp.float32)
        norm_row(g_mlp, l, i)

    def tiles(l, steps, offset, first, n_rows, marks=None):
        pre, post, ahead = {}, {}, {}
        early = False
        for n, (t, keys) in enumerate(steps):
            for key in (marks or {}).get((n, "pre"), ()):
                plan.mark(key)
            plan.need(keys)
            pre[t] = plan.take()
            if not early:
                pre[t].append(lambda t=t: [c.start() for c in tile_loads(l, offset(t), t % 2)])
                plan.spend(T_LOAD)
            for key in (marks or {}).get((n, "post"), ()):
                plan.mark(key)
            plan.service()
            post[t] = plan.take()
            early = n + 1 < len(steps) and set(steps[n + 1][1]) <= plan.arrived
            if early:
                post[t].append(lambda t=t: [c.start() for c in tile_loads(l, offset(t + 1), (t + 1) % 2)])
            plan.spend(T_TILE * n_rows / NB)

        def body(t, c):
            slot = lax.rem(t, 2)
            run_at(t, pre)
            for cp in tile_loads(l, offset(t), slot):
                cp.wait()
            run_at(t, post)
            lax.fori_loop(first, first + n_rows, lambda i, c: mlp_row(i, slot, c), 0)
            return c

        lax.fori_loop(steps[0][0], steps[-1][0] + 1, body, 0)

    def tile_loads(l, off, slot):
        cols = pl.ds(al(off, 128), TF)
        return [pltpu.make_async_copy(f_g.at[l, :, cols], vg.at[slot], tl.at[slot, 0]), pltpu.make_async_copy(f_u.at[l, :, cols], vu.at[slot], tl.at[slot, 1]),
                pltpu.make_async_copy(f_d.at[l, cols, :], vd.at[slot], tl.at[slot, 2])]

    get_qkv(0)
    table_q = []
    for i in range(NB):
        plan.service()
        table_q.append(plan.take())
        plan.spend(T_QKV + T_NORM)

    def qkv_step(i, c):
        run_at(i, table_q)
        norm_row(g_attn, 0, i)
        qkv_row(i)
        return c

    lax.fori_loop(0, NB, qkv_step, 0)
    heads(range(NB))
    get_o(0)
    table_o = []
    for i in range(NB):
        plan.service()
        if i >= 2:
            plan.mark(("h ready", 0, i - 2))
            plan.fill()
        table_o.append(plan.take())
        plan.spend(T_PROJ + T_NORM)

    def proj_step(i, c):
        run_at(i, table_o)
        proj_row(0, i)
        return c

    lax.fori_loop(0, NB, proj_step, 0)

    dn0 = [key for j in range(N_DN) for key in needs[("dn", 0, j)]]
    half_off = lambda t: yc * HALF + t * TF
    steps = [(j, needs[("gu", j)] + dn0) for j in range(N_G0)]
    got_h = lambda l, *chunks: [("h", l, i) for i in chunks]
    tiles(0, steps[:OWN_FIRST], half_off, 0, NB, {(0, "pre"): [("h ready", 0, NB - 2)], (0, "post"): [("h ready", 0, NB - 1)]})
    tiles(0, [(j, keys + got_h(0, *range(NB))) for j, keys in steps], half_off, NB, NB)
    tiles(0, steps[OWN_FIRST:], half_off, 0, NB, {(0, "post"): [("p ready", 0, i) for i in range(NB)]})

    get_qkv(1)
    for i in range(NB):
        plan.need([("p", 0, i)])
        plan.retire(keys=[("p", 0, i)])
        run(plan.take())
        load([(f_p.at[rows_of(i), :], x.at[rows_of(i + NB), :])])
        x[rows_of(i), :] += x[rows_of(i + NB), :]
        norm_row(g_attn, 1, i)
        qkv_row(i)
        plan.spend(T_QKV + T_NORM + T_ADD)
        heads([i])
        if i == 0:
            get_o(1)
        proj_row(1, i)
        x[rows_of(i + NB), :] = jnp.zeros((MB, D), jnp.float32)
        plan.spend(T_PROJ + T_NORM + 0.4)
        plan.mark(("h ready", 1, i))
        plan.service()
        run(plan.take())

    dt1 = dn1 + [key for j in range(N_DT) for key in needs[("dt", j)]]
    dd1 = dn1 + [key for j in range(N_DD) for key in needs[("dd", j)]]
    steps = [(j, needs[("gt", j)] + dt1) for j in TP_TILES]
    h_mark = {}
    run_order = L1_ORDER
    marks = {}
    for n, what in enumerate(run_order):
        if what[0] == "own":
            tiles(1, steps[what[1]:what[2]], half_off, 0, NB, {**h_mark, **marks})
            marks, h_mark = {}, {}
        elif what in GROUPS:
            chunks = GROUPS[what]
            tiles(1, [(j, keys + got_h(1, *chunks)) for j, keys in steps], half_off, NB + chunks[0], len(chunks), {**h_mark, **marks})
            marks, h_mark = {(0, "pre"): [("p ready", 1, i) for i in chunks[:-1]], (0, "post"): [("p ready", 1, chunks[-1])]}, {}
        else:
            tiles(1, [(j, needs[("gd", j)] + dd1) for j in range(N_DP)],
                  lambda t: (t % 2) * HALF + (t // 2) * (HALF - TF) if isinstance(t, int) else lax.rem(t, 2) * HALF + lax.div(t, 2) * (HALF - TF), 0, NB, {**h_mark, **marks})
            marks, h_mark = {}, {}

    for i in range(NB - 1):
        plan.need([("p", 1, i)])
        plan.retire(keys=[("p", 1, i)])
        run(plan.take())
        load([(f_r.at[rows_of(i), :], x.at[rows_of(i + NB), :])])
        x[rows_of(i), :] += x[rows_of(i + NB), :]
        plan.spend(T_ADD)
    plan.service()
    done = pltpu.make_async_copy(x.at[pl.ds(0, TOK), :], out, ld.at[0])
    done.start()
    plan.need(plan.all)
    plan.retire(everything=True)
    run(plan.take())
    done.wait()


def finish(x_in, r_in, out, xv, rv, sem):
    n = TOK // FB
    first = (NB - 1) * MB // FB
    rows = [pl.ds(i * FB, FB) for i in range(n)]
    order = list(range(first, n)) + list(range(first))
    got = {i: pltpu.make_async_copy(x_in.at[rows[i], :], xv.at[rows[i], :], sem.at[0, i]) for i in range(n)}
    ret = {i: pltpu.make_async_copy(r_in.at[rows[i], :], rv.at[pl.ds((i - first) * FB, FB), :], sem.at[1, i]) for i in range(first, n)}
    put = {i: pltpu.make_async_copy(xv.at[rows[i], :], out.at[rows[i], :], sem.at[2, i]) for i in range(n)}
    for i in order:
        if i in ret:
            ret[i].start()
        got[i].start()
    for i in range(first, n):
        ret[i].wait()
        got[i].wait()
        xv[rows[i], :] += rv[pl.ds((i - first) * FB, FB), :]
    for i in range(first):
        got[i].wait()
        put[i].start()
    for i in range(first, n):
        put[i].start()
    for i in range(n):
        put[i].wait()


def solution(mesh):
    tok_spec = P(("rep", "fsdp"), None)
    seg_spec = P(("rep", "fsdp"))
    mat_spec = P(None, "fsdp", None)
    gain_spec = P(None, None)
    bf, f32 = jnp.bfloat16, jnp.float32

    def per_device(tokens, seg_ids, w_q, w_k, w_v, w_o, w_gate, w_up, w_down, g_attn, g_mlp):
        half = HEAD // 2
        inv = np.float32(ROPE_BASE) ** (-np.arange(half, dtype=np.float32) / np.float32(half))
        freq = jnp.asarray(np.concatenate([inv, inv]).reshape(1, HEAD), f32)
        any_s = pl.BlockSpec(memory_space=pl.ANY)
        vm = pl.BlockSpec(memory_space=pltpu.VMEM)
        full = [(LAYERS, D, D), (LAYERS, D, KV), (LAYERS, D, KV), (LAYERS, D, D), (LAYERS, D, FF), (LAYERS, D, FF), (LAYERS, FF, D)]
        res = pl.pallas_call(
            kernel,
            out_shape=[jax.ShapeDtypeStruct((TOK, D), f32)] * 2 + [jax.ShapeDtypeStruct(s, bf) for s in full] + [jax.ShapeDtypeStruct((TOK, D), f32)],
            in_specs=[any_s, vm, vm, vm, vm] + [any_s] * 7,
            out_specs=[any_s] * 10,
            scratch_shapes=[
                pltpu.VMEM((2 * TOK, D), f32), pltpu.VMEM((2 * TOK, D), bf), pltpu.VMEM((TOK, D), bf),
                pltpu.VMEM((TOK, KV), bf), pltpu.VMEM((TOK, KV), bf), pltpu.VMEM((TOK, D), bf),
                pltpu.VMEM((TOK, HEAD), f32), pltpu.VMEM((TOK, HEAD), f32), pltpu.VMEM((TOK, TOK), f32),
                pltpu.VMEM((D, D), bf), pltpu.VMEM((D, KV), bf), pltpu.VMEM((D, KV), bf), pltpu.VMEM((D, D), bf),
                pltpu.VMEM((2, D, TF), bf), pltpu.VMEM((2, D, TF), bf), pltpu.VMEM((2, TF, D), bf),
                pltpu.VMEM((ROWS, D), bf), pltpu.VMEM((ROWS, KV), bf), pltpu.VMEM((ROWS, KV), bf), pltpu.VMEM((ROWS, D), bf),
                pltpu.VMEM((4, ROWS, TF), bf), pltpu.VMEM((4, ROWS, TF), bf), pltpu.VMEM((4, DR, D), bf),
                pltpu.SemaphoreType.DMA((N_SEM,)), pltpu.SemaphoreType.DMA((N_SEM,)), pltpu.SemaphoreType.DMA((4,)), pltpu.SemaphoreType.DMA((2, 3)),
            ],
            compiler_params=pltpu.CompilerParams(collective_id=0, has_side_effects=True, vmem_limit_bytes=66 * 1000 * 1000),
        )(tokens, seg_ids.reshape(1, TOK), freq, g_attn, g_mlp, w_q, w_k, w_v, w_o, w_gate, w_up, w_down)
        return pl.pallas_call(
            finish,
            out_shape=jax.ShapeDtypeStruct((TOK, D), f32),
            in_specs=[any_s, any_s],
            out_specs=any_s,
            scratch_shapes=[pltpu.VMEM((TOK, D), f32), pltpu.VMEM((MB, D), f32), pltpu.SemaphoreType.DMA((3, TOK // FB))],
            compiler_params=pltpu.CompilerParams(vmem_limit_bytes=66 * 1000 * 1000),
        )(res[0], res[1])

    return jax.shard_map(per_device, mesh=mesh, in_specs=(tok_spec, seg_spec, mat_spec, mat_spec, mat_spec, mat_spec, mat_spec, mat_spec, mat_spec, gain_spec, gain_spec), out_specs=tok_spec, check_vma=False)
```
